128 devices in a mesh: dp: 1, col: 16 (over z, y), row: 8 (over x, core).
Axes of the slice: x: 4, y: 4, z: 4, core: 2. Of those that a mesh axis runs over, the one named last changes fastest.
Arguments:
- hidden: bfloat16 [4096, 4096], P('dp', 'row')
- norm_gain: float32 [4096], P('row')
- w_head: bfloat16 [4096, 32000], P('row', 'col')
Outputs:
- output 1: float32 [4096, 32000], P('dp', ('col', 'row'))
- output 2: float32 [4096], P('dp')
All inputs are finite; a program needn't handle non-finite values.
Results may differ from the reference program's by a relative error of at most 0.001.
Values sent between devices are 32-bit elements.
A program may use at most 1 GiB of HBM per device.

```python
import jax
import jax.numpy as jnp
from jax import lax

BATCH = 4096
HIDDEN = 4096
VOCAB = 32000
EPS = 1e-5


def setup_inputs(seed: int = 0, part: int = 0) -> dict:
    key = jax.random.key(seed)
    part_key = jax.random.fold_in(key, part)
    key_tok, key_feat = jax.random.split(part_key, 2)
    key_gain, key_weight = jax.random.split(key, 2)
    position = jnp.arange(HIDDEN, dtype=jnp.float32) / HIDDEN
    feat_scale = (0.4 + 1.2 * position) * jax.random.uniform(key_feat, (HIDDEN,), jnp.float32, 0.8, 1.2)
    hidden = jax.random.normal(key_tok, (BATCH, HIDDEN), jnp.float32) * feat_scale
    gain = 2.4 / (0.4 + 1.2 * position) * jax.random.uniform(key_gain, (HIDDEN,), jnp.float32, 0.7, 1.3)
    weight = jax.random.normal(key_weight, (HIDDEN, VOCAB), jnp.float32) * HIDDEN ** -0.5
    return {"hidden": hidden.astype(jnp.bfloat16), "norm_gain": gain, "w_head": weight.astype(jnp.bfloat16)}


def reference(hidden, norm_gain, w_head):
    wide_hidden = hidden.astype(jnp.float32)
    mean_sq = jnp.mean(wide_hidden * wide_hidden, axis=-1, keepdims=True)
    normed = (wide_hidden * lax.rsqrt(mean_sq + EPS) * norm_gain).astype(jnp.bfloat16)
    logits = jnp.dot(normed, w_head, preferred_element_type=jnp.float32)
    log_norm = jax.nn.logsumexp(logits, axis=-1)
    return logits - log_norm[:, None], log_norm
```

```python
import jax
import jax.numpy as jnp
from jax import lax
from jax.sharding import PartitionSpec as P

EPS = 1e-5


def solution(mesh):
    row_count = mesh.shape["row"]

    def local_head(hidden, norm_gain, w_head):
        wide_hidden = hidden.astype(jnp.float32)
        local_sq = jnp.sum(wide_hidden * wide_hidden, axis=-1)
        total_sq = lax.psum(local_sq, "row")[:, None]
        mean_sq = total_sq / (hidden.shape[1] * row_count)
        normed = (wide_hidden * lax.rsqrt(mean_sq + EPS) * norm_gain).astype(jnp.bfloat16)
        words = w_head.shape[1] // row_count
        pad = -words % 128
        blocks = jnp.pad(w_head.reshape(w_head.shape[0], row_count, words), ((0, 0), (0, 0), (0, pad)))
        share = jnp.einsum("sk,kbw->bsw", normed, blocks, preferred_element_type=jnp.float32)
        logits = lax.psum_scatter(share, "row", scatter_dimension=0, tiled=False)[:, :words]
        local_max = jnp.max(logits, axis=-1)
        global_max = lax.pmax(local_max, ("col", "row"))
        local_mass = jnp.sum(jnp.exp(logits - global_max[:, None]), axis=-1)
        total_mass = lax.psum(local_mass, ("col", "row"))
        log_norm = global_max + jnp.log(total_mass)
        return logits - log_norm[:, None], log_norm

    return jax.shard_map(
        local_head,
        mesh=mesh,
        in_specs=(P("dp", "row"), P("row"), P("row", "col")),
        out_specs=(P("dp", ("col", "row")), P("dp")),
        check_vma=False,
    )
```

```python
import functools

import jax
import jax.numpy as jnp
from jax import lax
from jax.experimental import pallas as pl
from jax.experimental.pallas import tpu as pltpu
from jax.sharding import PartitionSpec as P

EPS = 1e-5
MESH = pl.DeviceIdType.MESH
F32 = jnp.float32
BF16 = jnp.bfloat16
LOW = -3.0e38

SEQ, FEAT, WORDS, PAD = 4096, 512, 250, 256
HALF = SEQ // 2
BLOCK, PIECE = 128, 32


def kernel(h_hbm, g_ref, w_hbm, z_hbm, lse_ref,
           h, w, wst, wl, wbf, xst, xl, xbf, zs, zp, zr, ssq, rinv, st1, st2, st3,
           in_sem, ssq_send, ssq_recv, wp_send, wp_recv, wb_send, wb_recv, wr_send, wr_recv,
           xp_send, xp_recv, xb_send, xf_send, x_recv, z_send, z_recv, zp_send, zp_recv,
           out_sem, st_send, st1_recv, st2_recv, st3_recv):
    col, row = lax.axis_index("col"), lax.axis_index("row")
    z, y = lax.div(col, 4), lax.rem(col, 4)
    x, c = lax.div(row, 2), lax.rem(row, 2)
    mate = 1 - c
    near = x + 1 - 2 * lax.rem(x, 2)
    far = 3 - x

    def at_row(r):
        return (0, col, r)

    def at_col(yy, zz):
        return (0, zz * 4 + yy, row)

    partner = at_row(x * 2 + mate)
    near_same = at_row(near * 2 + c)

    def remote(src, dst, send, recv, dev):
        return pltpu.make_async_remote_copy(
            src_ref=src, dst_ref=dst, send_sem=send, recv_sem=recv, device_id=dev, device_id_type=MESH)

    def drain_send(ref, sem):
        remote(ref, ref, sem, sem, partner).wait_send()

    def drain_recv(ref, sem):
        remote(ref, ref, sem, sem, partner).wait_recv()

    for k in range(4):
        rows = pl.ds(k * 1024, 1024)
        pltpu.make_async_copy(h_hbm.at[rows, :], h.at[rows, :], in_sem.at[k]).start()
    w_in = pltpu.make_async_copy(w_hbm, w, in_sem.at[4])
    w_in.start()

    barrier = pltpu.get_barrier_semaphore()
    peers = [at_row(lax.rem(row + d, 8)) for d in range(1, 8)]
    peers += [at_col(lax.rem(y + d, 4), z) for d in range(1, 4)]
    peers += [at_col(y, lax.rem(z + d, 4)) for d in range(1, 4)]
    for dev in peers:
        pl.semaphore_signal(barrier, inc=1, device_id=dev, device_id_type=MESH)

    w_in.wait()

    def prep(t, _):
        rows = pl.ds(pl.multiple_of(t * 64, 64), 64)
        wide = w[rows, :].astype(F32)
        for b in range(8):
            part = wide[:, b * WORDS:(b + 1) * WORDS]
            wst[b, rows, :] = jnp.concatenate([part, jnp.zeros((64, PAD - WORDS), F32)], axis=1)
        return 0

    lax.fori_loop(0, FEAT // 64, prep, 0)
    pl.semaphore_wait(barrier, len(peers))

    def kind_block(chip, n):
        return ((3 - chip) * 2 + n) if n < 2 else (chip * 2 + n - 2)

    def send_near(n, k0, size):
        rows = pl.ds(k0, size)
        remote(wst.at[kind_block(near, n), rows, :], wl.at[1, n, rows, :], wb_send, wb_recv.at[n], near_same).start()

    send_near(0, 0, 256)

    for k in range(4):
        rows = pl.ds(k * 1024, 1024)
        pltpu.make_async_copy(h_hbm.at[rows, :], h.at[rows, :], in_sem.at[k]).wait()

        def squares(t, _, k=k):
            b = k * 8 + t
            hb = h[pl.ds(pl.multiple_of(b * BLOCK, BLOCK), BLOCK), :].astype(F32)
            sq = hb * hb
            part = (sq[:, 0:128] + sq[:, 128:256]) + (sq[:, 256:384] + sq[:, 384:512])
            ssq[row, pl.ds(b, 1), :] = jnp.sum(part.T, axis=0, keepdims=True)
            return 0

        lax.fori_loop(0, 8, squares, 0)
    for d in range(1, 8):
        remote(ssq.at[row], ssq.at[row], ssq_send, ssq_recv.at[row], at_row(lax.rem(row + d, 8))).start()

    send_near(0, 256, 256)
    for n in range(4):
        remote(wst.at[kind_block(x, n)], wl.at[0, n], wp_send, wp_recv.at[n], partner).start()

    for d in range(1, 8):
        r = lax.rem(row + d, 8)
        drain_recv(ssq.at[r], ssq_recv.at[r])
    total = ssq[0]
    for r in range(1, 8):
        total = total + ssq[r]
    rinv[...] = lax.rsqrt(total / (FEAT * 8) + EPS)

    def flow(f):
        t, s = lax.div(f, 2), 1 - 2 * lax.rem(f, 2)
        return y * (1 - t) + z * t, z * (1 - t) + y * t, s

    def first(f, i):
        c1, _, s = flow(f)
        return lax.rem(c1 - s * i + 4, 4)

    def second(f, j):
        _, c2, s = flow(f)
        return lax.rem(c2 - s * j + 4, 4)

    def norm_block(nb):
        rows = pl.ds(pl.multiple_of(nb * BLOCK, BLOCK), BLOCK)
        scale = jnp.broadcast_to(rinv[pl.ds(nb, 1), :], (BLOCK, BLOCK)).T
        for q in range(4):
            lanes = slice(q * 128, (q + 1) * 128)
            value = h[rows, lanes].astype(F32) * scale * g_ref[:, lanes]
            xst[rows, lanes] = value.astype(BF16).astype(F32)

    def send_mate(n):
        i, f = lax.div(n, 4), lax.rem(n, 4)
        blk = f * 4 + first(f, i)
        src = pl.ds(pl.multiple_of(mate * HALF + blk * BLOCK, BLOCK), BLOCK)
        dst = pl.ds(pl.multiple_of(blk * BLOCK, BLOCK), BLOCK)
        remote(xst.at[src, :], xl.at[0, dst, :], xp_send, xp_recv.at[blk], partner).start()

    def norm_step(n, _):
        i, f = lax.div(n, 4), lax.rem(n, 4)
        blk = f * 4 + first(f, i)
        norm_block(blk)
        norm_block(16 + blk)
        send_mate(n)

        @pl.when(i == 0)
        def _():
            piece = blk * BLOCK + second(f, 0) * PIECE
            dst = pl.ds(pl.multiple_of(piece, PIECE), PIECE)
            for core in range(2):
                src = pl.ds(pl.multiple_of(core * HALF + piece, PIECE), PIECE)
                slot = 1 + (core + c) - 2 * core * c
                remote(xst.at[src, :], xl.at[slot, dst, :], xb_send, x_recv.at[f, 0],
                       at_row(near * 2 + core)).start()
        return 0

    lax.fori_loop(0, 4, norm_step, 0)
    for n in range(1, 4):
        send_near(n, 0, FEAT)
    lax.fori_loop(4, 16, norm_step, 0)

    def relay_weights(n):
        drain_recv(wl.at[1, n], wb_recv.at[n])
        remote(wl.at[1, n], wl.at[2, n], wr_send, wr_recv.at[n], partner).start()

    def take_weights(n):
        drain_recv(wl.at[0, n], wp_recv.at[n])
        drain_recv(wl.at[2, n], wr_recv.at[n])
        wbf[n, 0:512, :] = wst[kind_block(x, n)].astype(BF16)
        for k in range(3):
            wbf[n, (k + 1) * 512:(k + 2) * 512, :] = wl[k, n].astype(BF16)

    ups = (at_col(lax.rem(y + 1, 4), z), at_col(lax.rem(y + 3, 4), z),
           at_col(y, lax.rem(z + 1, 4)), at_col(y, lax.rem(z + 3, 4)))
    along_first = (ups[0], ups[1], ups[2], ups[3])
    along_second = (ups[2], ups[3], ups[0], ups[1])

    def serve(i, j):
        for f in range(4):
            base = f * 512 + first(f, i) * BLOCK + second(f, j) * PIECE
            ref = xl.at[pl.ds(1, 2), pl.ds(pl.multiple_of(base, PIECE), PIECE), :]
            step = i * 4 + j
            drain_recv(ref, x_recv.at[f, step])

            @pl.when(j < 3)
            def _():
                remote(ref, ref, xf_send.at[f], x_recv.at[f, step + 1], along_second[f]).start()

            @pl.when((j == 0) & (i < 3))
            def _():
                remote(ref, ref, xf_send.at[f], x_recv.at[f, step + 4], along_first[f]).start()

    relay_weights(0)
    lax.fori_loop(0, 4, lambda j, _: (serve(0, j), 0)[1], 0)
    take_weights(0)

    def rows_of(n):
        i, f = lax.div(n, 4), lax.rem(n, 4)
        blk = f * 4 + first(f, i)
        return blk, pl.multiple_of(blk * BLOCK, BLOCK)

    def gather_block(blk, base):
        rows = pl.ds(base, BLOCK)
        drain_recv(xl.at[0, rows, :], xp_recv.at[blk])
        xbf[rows, 0:512] = xst[pl.ds(pl.multiple_of(c * HALF + base, BLOCK), BLOCK), :].astype(BF16)
        for k in range(3):
            xbf[rows, (k + 1) * 512:(k + 2) * 512] = xl[k, rows, :].astype(BF16)

    def far_block(n, blk, base):
        rows = pl.ds(base, BLOCK)
        zs[n, rows, :] = jnp.dot(xbf[rows, :], wbf[n], preferred_element_type=F32)
        remote(zs.at[n, rows, :], zr.at[c, rows, :], z_send.at[n], z_recv.at[c, blk], at_row(far * 2 + n)).start()

    def step_a(n, _):
        serve(1, n)
        blk, base = rows_of(n)
        gather_block(blk, base)
        far_block(0, blk, base)
        return 0

    lax.fori_loop(0, 4, step_a, 0)
    relay_weights(1)
    take_weights(1)

    def step_ab(n, _):
        @pl.when(n < 12)
        def _():
            serve(lax.div(n, 4) + 1, lax.rem(n, 4))

        blk, base = rows_of(n)
        gather_block(blk, base)
        far_block(0, blk, base)
        far_block(1, blk, base)
        return 0

    lax.fori_loop(4, 8, step_ab, 0)
    relay_weights(2)
    lax.fori_loop(8, 12, step_ab, 0)
    relay_weights(3)
    lax.fori_loop(12, 16, step_ab, 0)

    def step_b(n, _):
        blk, base = rows_of(n)
        far_block(1, blk, base)
        return 0

    lax.fori_loop(0, 4, step_b, 0)
    take_weights(2)
    take_weights(3)

    def step_own(n, _):
        blk, base = rows_of(n)
        rows = pl.ds(base, BLOCK)
        xl[0, rows, 256:512] = jnp.dot(xbf[rows, :], wbf[2 + mate], preferred_element_type=F32)
        remote(xl.at[0, rows, pl.ds(256, 256)], zp.at[rows, :], zp_send, zp_recv.at[blk], partner).start()
        xl[0, rows, 0:256] = jnp.dot(xbf[rows, :], wbf[2 + c], preferred_element_type=F32)
        return 0

    lax.fori_loop(0, 16, step_own, 0)

    def finish(half, blk, base, mine):
        rows = pl.ds(base, BLOCK)
        drain_recv(zr.at[half, rows, :], z_recv.at[half, blk])
        value = zr[half, rows, :] + mine
        zr[half, rows, :] = value
        pltpu.make_async_copy(
            zr.at[half, rows, :],
            z_hbm.at[pl.ds(pl.multiple_of(half * HALF + base, BLOCK), BLOCK), :], out_sem.at[half]).start()
        lane = lax.broadcasted_iota(jnp.int32, (BLOCK, 128), 1)
        left, right = value[:, 0:128], jnp.where(lane < WORDS - 128, value[:, 128:256], LOW)
        top = jnp.max(jnp.maximum(left, right).T, axis=0, keepdims=True)
        shift = jnp.broadcast_to(top, (BLOCK, BLOCK)).T
        mass = jnp.exp(left - shift) + jnp.exp(right - shift)
        nb = half * 16 + blk
        st1[row, 0, pl.ds(nb, 1), :] = top
        st1[row, 1, pl.ds(nb, 1), :] = jnp.sum(mass.T, axis=0, keepdims=True)

    def step_out(n, _):
        blk, base = rows_of(n)
        rows = pl.ds(base, BLOCK)
        finish(c, blk, base, xl[0, rows, 0:256])
        drain_recv(zp.at[rows, :], zp_recv.at[blk])
        finish(mate, blk, base, zp[rows, :])
        return 0

    lax.fori_loop(0, 16, step_out, 0)

    def combine(st, count):
        top = st[0, 0]
        for k in range(1, count):
            top = jnp.maximum(top, st[k, 0])
        mass = st[0, 1] * jnp.exp(st[0, 0] - top)
        for k in range(1, count):
            mass = mass + st[k, 1] * jnp.exp(st[k, 0] - top)
        return top, mass

    def exchange(st, me, count, send, recv, dev):
        for d in range(1, count):
            remote(st.at[me], st.at[me], send, recv.at[me], dev(lax.rem(me + d, count))).start()
        for d in range(1, count):
            other = lax.rem(me + d, count)
            drain_recv(st.at[other], recv.at[other])

    exchange(st1, row, 8, st_send.at[0], st1_recv, at_row)
    top, mass = combine(st1, 8)
    st2[z, 0], st2[z, 1] = top, mass
    exchange(st2, z, 4, st_send.at[1], st2_recv, lambda k: at_col(y, k))
    top, mass = combine(st2, 4)
    st3[y, 0], st3[y, 1] = top, mass
    exchange(st3, y, 4, st_send.at[2], st3_recv, lambda k: at_col(k, z))
    top, mass = combine(st3, 4)
    lse_ref[...] = top + jnp.log(mass)

    drain_send(ssq.at[pl.ds(0, 7)], ssq_send)
    drain_send(wl.at[0], wp_send)
    drain_send(wl.at[0], wb_send)
    drain_send(wl.at[0], wr_send)
    drain_send(xl.at[0], xp_send)
    drain_send(xl.at[0, pl.ds(0, 256), :], xb_send)
    for f in range(4):
        drain_send(xl.at[pl.ds(1, 2), pl.ds(0, 15 * PIECE), :], xf_send.at[f])
    for n in range(2):
        drain_send(zs.at[n], z_send.at[n])
    drain_send(zp, zp_send)
    drain_send(st1.at[pl.ds(0, 7)], st_send.at[0])
    drain_send(st2.at[pl.ds(0, 3)], st_send.at[1])
    drain_send(st3.at[pl.ds(0, 3)], st_send.at[2])
    for half in range(2):
        pltpu.make_async_copy(zr.at[half], z_hbm.at[pl.ds(half * HALF, HALF), :], out_sem.at[half]).wait()


def solution(mesh):
    dma = pltpu.SemaphoreType.DMA

    def local_head(hidden, norm_gain, w_head):
        logits, log_norm = pl.pallas_call(
            kernel,
            out_shape=(jax.ShapeDtypeStruct((SEQ, PAD), F32), jax.ShapeDtypeStruct((32, 128), F32)),
            in_specs=[pl.BlockSpec(memory_space=pl.ANY), pl.BlockSpec(memory_space=pltpu.VMEM),
                      pl.BlockSpec(memory_space=pl.ANY)],
            out_specs=(pl.BlockSpec(memory_space=pl.ANY), pl.BlockSpec(memory_space=pltpu.VMEM)),
            scratch_shapes=[
                pltpu.VMEM((SEQ, FEAT), BF16),
                pltpu.VMEM((FEAT, 8 * WORDS), BF16),
                pltpu.VMEM((8, FEAT, PAD), F32),
                pltpu.VMEM((3, 4, FEAT, PAD), F32),
                pltpu.VMEM((4, 4 * FEAT, PAD), BF16),
                pltpu.VMEM((SEQ, FEAT), F32),
                pltpu.VMEM((3, HALF, FEAT), F32),
                pltpu.VMEM((HALF, 4 * FEAT), BF16),
                pltpu.VMEM((2, HALF, PAD), F32),
                pltpu.VMEM((HALF, PAD), F32),
                pltpu.VMEM((2, HALF, PAD), F32),
                pltpu.VMEM((8, 32, 128), F32),
                pltpu.VMEM((32, 128), F32),
                pltpu.VMEM((8, 2, 32, 128), F32),
                pltpu.VMEM((4, 2, 32, 128), F32),
                pltpu.VMEM((4, 2, 32, 128), F32),
                dma((5,)),
                dma, dma((8,)),
                dma, dma((4,)),
                dma, dma((4,)),
                dma, dma((4,)),
                dma, dma((16,)),
                dma, dma((4,)), dma((4, 16)),
                dma((2,)), dma((2, 16)),
                dma, dma((16,)),
                dma((2,)),
                dma((3,)), dma((8,)), dma((4,)), dma((4,)),
            ],
            compiler_params=pltpu.CompilerParams(
                collective_id=0, has_side_effects=True, vmem_limit_bytes=67_043_328),
        )(hidden, norm_gain.reshape(1, FEAT), w_head)
        log_norm = log_norm.reshape(SEQ)
        return logits[:, :WORDS] - log_norm[:, None], log_norm

    return jax.shard_map(
        local_head,
        mesh=mesh,
        in_specs=(P("dp", "row"), P("row"), P("row", "col")),
        out_specs=(P("dp", ("col", "row")), P("dp")),
        check_vma=False,
    )
```

```python
import functools

import jax
import jax.numpy as jnp
from jax import lax
from jax.experimental import pallas as pl
from jax.experimental.pallas import tpu as pltpu
from jax.sharding import PartitionSpec as P

EPS = 1e-5
MESH = pl.DeviceIdType.MESH
F32 = jnp.float32
BF16 = jnp.bfloat16
LOW = -3.0e38

SEQ, FEAT, WORDS, PAD = 4096, 512, 250, 256
HALF = SEQ // 2
BLOCK, PIECE = 128, 32
AHEAD = 7


def kernel(h_hbm, g_ref, w_hbm, z_hbm, lse_ref,
           h, hp16, hp, w, wst, wl, wbf, xst, xl, xbf, zs, zp, zr, gl, ssq, rcol, st1, st2, st3,
           in_sem, ssq_send, ssq_recv, g_send, g_recv, wp_send, wp_recv, wb_send, wb_recv, wr_send, wr_recv,
           xp_send, xp_recv, xb_send, xf_send, x_recv, z_send, z_recv, zp_send, zp_recv,
           out_sem, st_send, st1_recv, st2_recv, st3_recv):
    col, row = lax.axis_index("col"), lax.axis_index("row")
    z, y = lax.div(col, 4), lax.rem(col, 4)
    x, c = lax.div(row, 2), lax.rem(row, 2)
    mate = 1 - c
    near = x + 1 - 2 * lax.rem(x, 2)
    far = 3 - x

    def at_row(r):
        return (0, col, r)

    def at_col(yy, zz):
        return (0, zz * 4 + yy, row)

    partner = at_row(x * 2 + mate)
    near_same = at_row(near * 2 + c)
    near_other = at_row(near * 2 + mate)

    def remote(src, dst, send, recv, dev):
        return pltpu.make_async_remote_copy(
            src_ref=src, dst_ref=dst, send_sem=send, recv_sem=recv, device_id=dev, device_id_type=MESH)

    def drain_send(ref, sem):
        remote(ref, ref, sem, sem, partner).wait_send()

    def drain_recv(ref, sem):
        remote(ref, ref, sem, sem, partner).wait_recv()

    firsts, seconds = (y, y, z, z), (z, z, y, y)
    signs = (1, -1, 1, -1)

    def first(f, i):
        return lax.rem(firsts[f] - signs[f] * i + 4, 4)

    def second(f, j):
        return lax.rem(seconds[f] - signs[f] * j + 4, 4)

    def piece_base(f, i, j):
        return f * 512 + first(f, i) * BLOCK + second(f, j) * PIECE

    def piece_rows(f, i, j, offset=0):
        return pl.ds(pl.multiple_of(offset + piece_base(f, i, j), PIECE), PIECE)

    own_pieces = [(f, core) for f in range(4) for core in range(2)]

    def load_piece(f, core):
        return pltpu.make_async_copy(
            h_hbm.at[piece_rows(f, 0, 0, core * HALF), :], hp16.at[f * 2 + core], in_sem.at[5 + f * 2 + core])

    def load_h(k):
        rows = pl.ds(k * 1024, 1024)
        return pltpu.make_async_copy(h_hbm.at[rows, :], h.at[rows, :], in_sem.at[k])

    for f, core in own_pieces:
        load_piece(f, core).start()
    w_in = pltpu.make_async_copy(w_hbm, w, in_sem.at[4])
    w_in.start()
    for k in range(4):
        load_h(k).start()

    barrier = pltpu.get_barrier_semaphore()
    peers = [at_row(lax.rem(row + d, 8)) for d in range(1, 8)]
    peers += [at_col(lax.rem(y + d, 4), z) for d in range(1, 4)]
    peers += [at_col(y, lax.rem(z + d, 4)) for d in range(1, 4)]
    for dev in peers:
        pl.semaphore_signal(barrier, inc=1, device_id=dev, device_id_type=MESH)

    for f, core in own_pieces:
        load_piece(f, core).wait()
        hp[f * 2 + core] = hp16[f * 2 + core].astype(F32)
    with jax.named_scope("bar"):
        pl.semaphore_wait(barrier, len(peers))

    for f, core in own_pieces:
        slot = 1 + (core + c) - 2 * core * c
        remote(hp.at[f * 2 + core], xl.at[slot, piece_rows(f, 0, 0), :], xb_send, x_recv.at[f, 0],
               at_row(near * 2 + core)).start()
    for slot, dev in enumerate((partner, near_same, near_other)):
        remote(g_ref, gl.at[slot], g_send, g_recv.at[slot], dev).start()

    w_in.wait()

    def prep(b, rows):
        start = rows // 16 * 16
        for q in range(4):
            lanes = slice(q * 128, (q + 1) * 128)
            wide = w[start:min(start + 272, 8 * WORDS), lanes].astype(F32)
            part = wide[rows - start:rows - start + WORDS, :]
            wst[b, :, lanes] = jnp.concatenate([part, jnp.zeros((PAD - WORDS, 128), F32)], axis=0)

    with jax.named_scope("prep"):
        for b in range(8):
            prep(b, b * WORDS)

    def kind_block(chip, n):
        return ((3 - chip) * 2 + n) if n < 2 else (chip * 2 + n - 2)

    def send_near(n):
        remote(wst.at[kind_block(near, n)], wl.at[1, n], wb_send, wb_recv.at[n], near_same).start()

    send_near(0)
    for n in range(4):
        remote(wst.at[kind_block(x, n)], wl.at[0, n], wp_send, wp_recv.at[n], partner).start()

    for k in range(4):
        load_h(k).wait()

        def squares(t, _, k=k):
            b = k * 8 + t
            hb = h[pl.ds(pl.multiple_of(b * BLOCK, BLOCK), BLOCK), :].astype(F32)
            sq = hb * hb
            part = (sq[:, 0:128] + sq[:, 128:256]) + (sq[:, 256:384] + sq[:, 384:512])
            ssq[row, pl.ds(b, 1), :] = jnp.sum(part.T, axis=0, keepdims=True)
            return 0

        with jax.named_scope("squares"):
            lax.fori_loop(0, 8, squares, 0)
    for d in range(1, 8):
        remote(ssq.at[row], ssq.at[row], ssq_send, ssq_recv.at[row], at_row(lax.rem(row + d, 8))).start()
    for n in range(1, 4):
        send_near(n)

    for f in range(4):
        rows = pl.ds(f * 512, 512)
        xst[rows, :] = h[pl.ds(pl.multiple_of(mate * HALF + f * 512, 512), 512), :].astype(F32)
        remote(xst.at[rows, :], xl.at[0, rows, :], xp_send, xp_recv.at[f], partner).start()

    def relay_weights(n):
        with jax.named_scope("wrelay"):
            drain_recv(wl.at[1, n], wb_recv.at[n])
        remote(wl.at[1, n], wl.at[2, n], wr_send, wr_recv.at[n], partner).start()

    def take_weights(n):
        with jax.named_scope("wtake"):
            drain_recv(wl.at[0, n], wp_recv.at[n])
            drain_recv(wl.at[2, n], wr_recv.at[n])
        wbf[n, :, 0:512] = wst[kind_block(x, n)].astype(BF16)
        for k in range(3):
            wbf[n, :, (k + 1) * 512:(k + 2) * 512] = wl[k, n].astype(BF16)

    ups = (at_col(lax.rem(y + 1, 4), z), at_col(lax.rem(y + 3, 4), z),
           at_col(y, lax.rem(z + 1, 4)), at_col(y, lax.rem(z + 3, 4)))
    along_first = (ups[0], ups[1], ups[2], ups[3])
    along_second = (ups[2], ups[3], ups[0], ups[1])

    def serve(i, j):
        with jax.named_scope("serve"):
            for f in range(4):
                ref = xl.at[pl.ds(1, 2), piece_rows(f, i, j), :]
                step = i * 4 + j
                drain_recv(ref, x_recv.at[f, step])
                if j == 0 and i < 3:
                    remote(ref, ref, xf_send.at[f], x_recv.at[f, step + 4], along_first[f]).start()
                if j < 3:
                    remote(ref, ref, xf_send.at[f], x_recv.at[f, step + 1], along_second[f]).start()

    def scales():
        with jax.named_scope("wssq"):
            for d in range(1, 8):
                r = lax.rem(row + d, 8)
                drain_recv(ssq.at[r], ssq_recv.at[r])
            for slot in range(3):
                drain_recv(gl.at[slot], g_recv.at[slot])
        mine = pl.ds(pl.multiple_of(c * 16, 16), 16)
        total = ssq[0, mine, :]
        for r in range(1, 8):
            total = total + ssq[r, mine, :]
        inv = lax.rsqrt(total / (FEAT * 8) + EPS)
        for b in range(16):
            rcol[b * BLOCK:(b + 1) * BLOCK, :] = jnp.broadcast_to(inv[b:b + 1, :], (BLOCK, BLOCK)).T

    def normalise(f, i, j):
        rows = piece_rows(f, i, j)
        scale = rcol[rows, :]
        for k in range(4):
            for q in range(4):
                lanes = slice(q * 128, (q + 1) * 128)
                if k == 0:
                    raw, gain = h[piece_rows(f, i, j, c * HALF), lanes].astype(F32), g_ref[:, lanes]
                else:
                    raw, gain = xl[k - 1, rows, lanes], gl[k - 1, :, lanes]
                xbf[rows, k * 512 + q * 128:k * 512 + (q + 1) * 128] = (raw * scale * gain).astype(BF16)

    def share(left, n):
        return lax.dot_general(left, wbf[n], (((1,), (1,)), ((), ())), preferred_element_type=F32)

    def far_group(i, j):
        with jax.named_scope("group"):
            for f in range(4):
                normalise(f, i, j)
            left = jnp.concatenate([xbf[piece_rows(f, i, j), :] for f in range(4)], axis=0)
            value = share(left, 0)
            for f in range(4):
                rows = piece_rows(f, i, j)
                zs[0, rows, :] = value[f * PIECE:(f + 1) * PIECE, :]
                remote(zs.at[0, rows, :], zr.at[c, rows, :], z_send.at[0], z_recv.at[c, f * 4 + first(f, i)],
                       at_row(far * 2)).start()

    order = sorted(((i, j) for i in range(4) for j in range(4)), key=lambda t: (t[0] + t[1], -t[0]))
    ahead = AHEAD
    for i, j in order[:ahead - 2]:
        serve(i, j)
    scales()
    serve(*order[ahead - 2])
    relay_weights(0)
    serve(*order[ahead - 1])
    for f in range(4):
        drain_recv(xl.at[0, pl.ds(f * 512, 512), :], xp_recv.at[f])
    with jax.named_scope("take"):
        take_weights(0)
    for k, (i, j) in enumerate(order):
        far_group(i, j)
        if k > 0 and k + ahead - 1 < 16:
            serve(*order[k + ahead - 1])
        if k == 6:
            relay_weights(1)
        if k == 10:
            relay_weights(2)
    with jax.named_scope("take"):
        take_weights(1)

    def block_rows(blk):
        return pl.ds(pl.multiple_of(blk * BLOCK, BLOCK), BLOCK)

    def step_far(blk, _):
        with jax.named_scope("far"):
            rows = block_rows(blk)
            zs[1, rows, :] = share(xbf[rows, :], 1)
            remote(zs.at[1, rows, :], zr.at[c, rows, :], z_send.at[1], z_recv.at[c, blk], at_row(far * 2 + 1)).start()
        return 0

    lax.fori_loop(0, 16, step_far, 0)
    relay_weights(3)
    take_weights(2)
    take_weights(3)

    def step_own(blk, _):
        with jax.named_scope("own"):
            rows = block_rows(blk)
            xl[0, rows, 256:512] = share(xbf[rows, :], 2 + mate)
            remote(xl.at[0, rows, pl.ds(256, 256)], zp.at[rows, :], zp_send, zp_recv.at[blk], partner).start()
            xl[0, rows, 0:256] = share(xbf[rows, :], 2 + c)
        return 0

    lax.fori_loop(0, 16, step_own, 0)

    def finish(p, half, q, mine):
        blk = p * 4 + q
        rows = block_rows(blk)
        with jax.named_scope("wz"):
            drain_recv(zr.at[half, rows, :], z_recv.at[half, blk])
        value = zr[half, rows, :] + mine
        zr[half, rows, :] = value
        pltpu.make_async_copy(
            zr.at[half, rows, :],
            z_hbm.at[pl.ds(pl.multiple_of(half * HALF + blk * BLOCK, BLOCK), BLOCK), :], out_sem.at[half]).start()
        lane = lax.broadcasted_iota(jnp.int32, (BLOCK, 128), 1)
        left, right = value[:, 0:128], jnp.where(lane < WORDS - 128, value[:, 128:256], LOW)
        top = jnp.max(jnp.maximum(left, right).T, axis=0, keepdims=True)
        shift = jnp.broadcast_to(top, (BLOCK, BLOCK)).T
        mass = jnp.exp(left - shift) + jnp.exp(right - shift)
        st1[p, row, 0, pl.ds(half * 4 + q, 1), :] = top
        st1[p, row, 1, pl.ds(half * 4 + q, 1), :] = jnp.sum(mass.T, axis=0, keepdims=True)

    def combine(st, p, count):
        top = st[p, 0, 0]
        for k in range(1, count):
            top = jnp.maximum(top, st[p, k, 0])
        mass = st[p, 0, 1] * jnp.exp(st[p, 0, 0] - top)
        for k in range(1, count):
            mass = mass + st[p, k, 1] * jnp.exp(st[p, k, 0] - top)
        return top, mass

    def exchange(st, p, me, count, send, recv, dev):
        with jax.named_scope("exch"):
            for d in range(1, count):
                remote(st.at[p, me], st.at[p, me], send, recv.at[p, me], dev(lax.rem(me + d, count))).start()
            for d in range(1, count):
                other = lax.rem(me + d, count)
                drain_recv(st.at[p, other], recv.at[p, other])

    for p in range(4):
        def step_out(q, _, p=p):
            rows = block_rows(p * 4 + q)
            finish(p, c, q, xl[0, rows, 0:256])
            drain_recv(zp.at[rows, :], zp_recv.at[p * 4 + q])
            finish(p, mate, q, zp[rows, :])
            return 0

        with jax.named_scope("finish"):
            lax.fori_loop(0, 4, step_out, 0)
        exchange(st1, p, row, 8, st_send.at[0], st1_recv, at_row)
        top, mass = combine(st1, p, 8)
        st2[p, z, 0], st2[p, z, 1] = top, mass
        exchange(st2, p, z, 4, st_send.at[1], st2_recv, lambda k: at_col(y, k))
        top, mass = combine(st2, p, 4)
        st3[p, y, 0], st3[p, y, 1] = top, mass
        exchange(st3, p, y, 4, st_send.at[2], st3_recv, lambda k: at_col(k, z))
        top, mass = combine(st3, p, 4)
        lse = top + jnp.log(mass)
        for half in range(2):
            lse_ref[half * 16 + p * 4:half * 16 + p * 4 + 4, :] = lse[half * 4:half * 4 + 4, :]

    drain_send(ssq.at[pl.ds(0, 7)], ssq_send)
    drain_send(gl, g_send)
    drain_send(wl.at[0], wp_send)
    drain_send(wl.at[0], wb_send)
    drain_send(wl.at[0], wr_send)
    drain_send(xl.at[0], xp_send)
    drain_send(xl.at[0, pl.ds(0, 256), :], xb_send)
    for f in range(4):
        drain_send(xl.at[pl.ds(1, 2), pl.ds(0, 15 * PIECE), :], xf_send.at[f])
    for n in range(2):
        drain_send(zs.at[n], z_send.at[n])
    drain_send(zp, zp_send)
    drain_send(st1.at[:, pl.ds(0, 7)], st_send.at[0])
    drain_send(st2.at[:, pl.ds(0, 3)], st_send.at[1])
    drain_send(st3.at[:, pl.ds(0, 3)], st_send.at[2])
    for half in range(2):
        pltpu.make_async_copy(zr.at[half], z_hbm.at[pl.ds(half * HALF, HALF), :], out_sem.at[half]).wait()


def solution(mesh):
    dma = pltpu.SemaphoreType.DMA

    def local_head(hidden, norm_gain, w_head):
        logits, log_norm = pl.pallas_call(
            kernel,
            out_shape=(jax.ShapeDtypeStruct((SEQ, PAD), F32), jax.ShapeDtypeStruct((32, 128), F32)),
            in_specs=[pl.BlockSpec(memory_space=pl.ANY), pl.BlockSpec(memory_space=pltpu.VMEM),
                      pl.BlockSpec(memory_space=pl.ANY)],
            out_specs=(pl.BlockSpec(memory_space=pl.ANY), pl.BlockSpec(memory_space=pltpu.VMEM)),
            scratch_shapes=[
                pltpu.VMEM((SEQ, FEAT), BF16),
                pltpu.VMEM((8, PIECE, FEAT), BF16),
                pltpu.VMEM((8, PIECE, FEAT), F32),
                pltpu.VMEM((8 * WORDS, FEAT), BF16),
                pltpu.VMEM((8, PAD, FEAT), F32),
                pltpu.VMEM((3, 4, PAD, FEAT), F32),
                pltpu.VMEM((4, PAD, 4 * FEAT), BF16),
                pltpu.VMEM((HALF, FEAT), F32),
                pltpu.VMEM((3, HALF, FEAT), F32),
                pltpu.VMEM((HALF, 4 * FEAT), BF16),
                pltpu.VMEM((2, HALF, PAD), F32),
                pltpu.VMEM((HALF, PAD), F32),
                pltpu.VMEM((2, HALF, PAD), F32),
                pltpu.VMEM((3, 1, FEAT), F32),
                pltpu.VMEM((8, 32, 128), F32),
                pltpu.VMEM((HALF, 128), F32),
                pltpu.VMEM((4, 8, 2, 8, 128), F32),
                pltpu.VMEM((4, 4, 2, 8, 128), F32),
                pltpu.VMEM((4, 4, 2, 8, 128), F32),
                dma((13,)),
                dma, dma((8,)),
                dma, dma((3,)),
                dma, dma((4,)),
                dma, dma((4,)),
                dma, dma((4,)),
                dma, dma((4,)),
                dma, dma((4,)), dma((4, 16)),
                dma((2,)), dma((2, 16)),
                dma, dma((16,)),
                dma((2,)),
                dma((3,)), dma((4, 8)), dma((4, 4)), dma((4, 4)),
            ],
            compiler_params=pltpu.CompilerParams(
                collective_id=0, has_side_effects=True, vmem_limit_bytes=67_043_328),
        )(hidden, norm_gain.reshape(1, FEAT), w_head.T)
        log_norm = log_norm.reshape(SEQ)
        return logits[:, :WORDS] - log_norm[:, None], log_norm

    return jax.shard_map(
        local_head,
        mesh=mesh,
        in_specs=(P("dp", "row"), P("row"), P("row", "col")),
        out_specs=(P("dp", ("col", "row")), P("dp")),
        check_vma=False,
    )
```

```python
import functools

import jax
import jax.numpy as jnp
from jax import lax
from jax.experimental import pallas as pl
from jax.experimental.pallas import tpu as pltpu
from jax.sharding import PartitionSpec as P

EPS = 1e-5
MESH = pl.DeviceIdType.MESH
F32 = jnp.float32
BF16 = jnp.bfloat16
LOW = -3.0e38

SEQ, FEAT, WORDS, PAD = 4096, 512, 250, 256
HALF = SEQ // 2
BLOCK, PIECE = 128, 32


def kernel(h_hbm, g_ref, w_hbm, z_hbm, lse_ref,
           h, hp16, hp, w, wst, wl, wbf, xst, xl, xbf, zs, zp, zr, gl, ssq, rcol, st, st1, st2, st3,
           in_sem, ssq_send, ssq_recv, g_send, g_recv, wp_send, wp_recv, wb_send, wb_recv, wr_send, wr_recv,
           xp_send, xp_recv, xb_send, xf_send, x_recv, z_send, z_recv, zp_send, zp_recv,
           out_sem, st_send, st1_recv, st2_recv, st3_recv):
    col, row = lax.axis_index("col"), lax.axis_index("row")
    z, y = lax.div(col, 4), lax.rem(col, 4)
    x, c = lax.div(row, 2), lax.rem(row, 2)
    mate = 1 - c
    near = x + 1 - 2 * lax.rem(x, 2)
    far = 3 - x

    def at_row(r):
        return (0, col, r)

    def at_col(yy, zz):
        return (0, zz * 4 + yy, row)

    partner = at_row(x * 2 + mate)
    near_same = at_row(near * 2 + c)
    near_other = at_row(near * 2 + mate)

    def remote(src, dst, send, recv, dev):
        return pltpu.make_async_remote_copy(
            src_ref=src, dst_ref=dst, send_sem=send, recv_sem=recv, device_id=dev, device_id_type=MESH)

    def drain_send(ref, sem):
        remote(ref, ref, sem, sem, partner).wait_send()

    def drain_recv(ref, sem):
        remote(ref, ref, sem, sem, partner).wait_recv()

    firsts, seconds = (y, y, z, z), (z, z, y, y)
    signs = (1, -1, 1, -1)

    def first(f, i):
        return lax.rem(firsts[f] - signs[f] * i + 4, 4)

    def second(f, j):
        return lax.rem(seconds[f] - signs[f] * j + 4, 4)

    def piece_base(f, i, j):
        return f * 512 + first(f, i) * BLOCK + second(f, j) * PIECE

    def piece_rows(f, i, j, offset=0):
        return pl.ds(pl.multiple_of(offset + piece_base(f, i, j), PIECE), PIECE)

    own_pieces = [(f, core) for f in range(4) for core in range(2)]

    def load_piece(f, core):
        return pltpu.make_async_copy(
            h_hbm.at[piece_rows(f, 0, 0, core * HALF), :], hp16.at[f * 2 + core], in_sem.at[5 + f * 2 + core])

    def load_h(k):
        rows = pl.ds(k * 1024, 1024)
        return pltpu.make_async_copy(h_hbm.at[rows, :], h.at[rows, :], in_sem.at[k])

    for f, core in own_pieces:
        load_piece(f, core).start()
    w_in = pltpu.make_async_copy(w_hbm, w, in_sem.at[4])
    w_in.start()
    for k in range(4):
        load_h(k).start()

    barrier = pltpu.get_barrier_semaphore()
    peers = [at_row(lax.rem(row + d, 8)) for d in range(1, 8)]
    peers += [at_col(lax.rem(y + d, 4), z) for d in range(1, 4)]
    peers += [at_col(y, lax.rem(z + d, 4)) for d in range(1, 4)]
    for dev in peers:
        pl.semaphore_signal(barrier, inc=1, device_id=dev, device_id_type=MESH)

    for f, core in own_pieces:
        load_piece(f, core).wait()
        hp[f * 2 + core] = hp16[f * 2 + core].astype(F32)
    with jax.named_scope("bar"):
        pl.semaphore_wait(barrier, len(peers))

    for f, core in own_pieces:
        slot = 1 + (core + c) - 2 * core * c
        remote(hp.at[f * 2 + core], xl.at[slot, piece_rows(f, 0, 0), :], xb_send, x_recv.at[f, 0],
               at_row(near * 2 + core)).start()
    for slot, dev in enumerate((partner, near_same, near_other)):
        remote(g_ref, gl.at[slot], g_send, g_recv.at[slot], dev).start()

    w_in.wait()

    def prep(b, rows):
        start = rows // 16 * 16
        for q in range(4):
            lanes = slice(q * 128, (q + 1) * 128)
            wide = w[start:min(start + 272, 8 * WORDS), lanes].astype(F32)
            part = wide[rows - start:rows - start + WORDS, :]
            wst[b, :, lanes] = jnp.concatenate([part, jnp.zeros((PAD - WORDS, 128), F32)], axis=0)

    with jax.named_scope("prep"):
        for b in range(8):
            prep(b, b * WORDS)

    def kind_block(chip, n):
        return ((3 - chip) * 2 + n) if n < 2 else (chip * 2 + n - 2)

    parts = ((0, 0, 128), (0, 128, 128), (1, 0, PAD), (2, 0, PAD), (3, 0, PAD))

    def send_near(p):
        n, w0, size = parts[p]
        rows = pl.ds(w0, size)
        remote(wst.at[kind_block(near, n), rows, :], wl.at[1, n, rows, :], wb_send, wb_recv.at[p], near_same).start()

    for n in range(4):
        remote(wst.at[kind_block(x, n)], wl.at[0, n], wp_send, wp_recv.at[n], partner).start()

    for k in range(4):
        load_h(k).wait()

        def squares(t, _, k=k):
            b = k * 8 + t
            hb = h[pl.ds(pl.multiple_of(b * BLOCK, BLOCK), BLOCK), :].astype(F32)
            sq = hb * hb
            part = (sq[:, 0:128] + sq[:, 128:256]) + (sq[:, 256:384] + sq[:, 384:512])
            ssq[row, pl.ds(b, 1), :] = jnp.sum(part.T, axis=0, keepdims=True)
            return 0

        with jax.named_scope("squares"):
            lax.fori_loop(0, 8, squares, 0)
    for d in range(1, 8):
        remote(ssq.at[row], ssq.at[row], ssq_send, ssq_recv.at[row], at_row(lax.rem(row + d, 8))).start()

    for f in range(4):
        rows = pl.ds(f * 512, 512)
        xst[rows, :] = h[pl.ds(pl.multiple_of(mate * HALF + f * 512, 512), 512), :].astype(F32)
        remote(xst.at[rows, :], xl.at[0, rows, :], xp_send, xp_recv.at[f], partner).start()

    def relay_weights(p):
        n, w0, size = parts[p]
        rows = pl.ds(w0, size)
        with jax.named_scope("wrelay"):
            drain_recv(wl.at[1, n, rows, :], wb_recv.at[p])
        remote(wl.at[1, n, rows, :], wl.at[2, n, rows, :], wr_send, wr_recv.at[p], partner).start()
        if 1 <= p < 4:
            send_near(p + 1)

    def take_weights(p):
        n, w0, size = parts[p]
        rows = pl.ds(w0, size)
        with jax.named_scope("wtake"):
            if w0 == 0:
                drain_recv(wl.at[0, n], wp_recv.at[n])
            drain_recv(wl.at[2, n, rows, :], wr_recv.at[p])
        wbf[n, rows, 0:512] = wst[kind_block(x, n), rows, :].astype(BF16)
        for k in range(3):
            wbf[n, rows, (k + 1) * 512:(k + 2) * 512] = wl[k, n, rows, :].astype(BF16)

    ups = (at_col(lax.rem(y + 1, 4), z), at_col(lax.rem(y + 3, 4), z),
           at_col(y, lax.rem(z + 1, 4)), at_col(y, lax.rem(z + 3, 4)))
    along_first = (ups[0], ups[1], ups[2], ups[3])
    along_second = (ups[2], ups[3], ups[0], ups[1])

    def serve(i, j, flows=(0, 1, 2, 3)):
        with jax.named_scope("serve"):
            for f in flows:
                ref = xl.at[pl.ds(1, 2), piece_rows(f, i, j), :]
                step = i * 4 + j
                drain_recv(ref, x_recv.at[f, step])
                if j == 0 and i < 3:
                    remote(ref, ref, xf_send.at[f], x_recv.at[f, step + 4], along_first[f]).start()
                if j < 3:
                    remote(ref, ref, xf_send.at[f], x_recv.at[f, step + 1], along_second[f]).start()

    def scales():
        with jax.named_scope("wssq"):
            for d in range(1, 8):
                r = lax.rem(row + d, 8)
                drain_recv(ssq.at[r], ssq_recv.at[r])
            for slot in range(3):
                drain_recv(gl.at[slot], g_recv.at[slot])
        mine = pl.ds(pl.multiple_of(c * 16, 16), 16)
        total = ssq[0, mine, :]
        for r in range(1, 8):
            total = total + ssq[r, mine, :]
        inv = lax.rsqrt(total / (FEAT * 8) + EPS)
        for b in range(16):
            rcol[b * BLOCK:(b + 1) * BLOCK, :] = jnp.broadcast_to(inv[b:b + 1, :], (BLOCK, BLOCK)).T

    def normalise(f, i, j):
        rows = piece_rows(f, i, j)
        scale = rcol[rows, :]
        for k in range(4):
            for q in range(4):
                lanes = slice(q * 128, (q + 1) * 128)
                if k == 0:
                    raw, gain = h[piece_rows(f, i, j, c * HALF), lanes].astype(F32), g_ref[:, lanes]
                else:
                    raw, gain = xl[k - 1, rows, lanes], gl[k - 1, :, lanes]
                xbf[rows, k * 512 + q * 128:k * 512 + (q + 1) * 128] = (raw * scale * gain).astype(BF16)

    def share(left, n, rows=slice(0, PAD)):
        return lax.dot_general(left, wbf[n, rows, :], (((1,), (1,)), ((), ())), preferred_element_type=F32)

    def far_group(i, j, words):
        with jax.named_scope("group"):
            left = jnp.concatenate([xbf[piece_rows(f, i, j), :] for f in range(4)], axis=0)
            value = share(left, 0, words)
            lanes = pl.ds(words.start, words.stop - words.start)
            for f in range(4):
                rows = piece_rows(f, i, j)
                zs[0, rows, words] = value[f * PIECE:(f + 1) * PIECE, :]
                remote(zs.at[0, rows, lanes], zr.at[c, rows, lanes], z_send.at[0],
                       z_recv.at[c, f * 4 + first(f, i)], at_row(far * 2)).start()

    def normalise_group(i, j):
        with jax.named_scope("norm"):
            for f in range(4):
                normalise(f, i, j)

    order = sorted(((i, j) for i in range(4) for j in range(4)), key=lambda t: (t[0] + t[1], -t[0]))
    low, high, full = slice(0, 128), slice(128, PAD), slice(0, PAD)
    serve(0, 0, (0, 1, 2))
    drain_send(xl.at[0, pl.ds(0, 256), :], xb_send)
    send_near(0)
    send_near(1)
    serve(0, 0, (3,))
    serve(*order[1])
    scales()
    for f in range(4):
        drain_recv(xl.at[0, pl.ds(f * 512, 512), :], xp_recv.at[f])
    serve(*order[2])
    relay_weights(0)
    normalise_group(*order[0])
    normalise_group(*order[1])
    take_weights(0)
    far_group(*order[0], low)
    far_group(*order[1], low)
    for k in (2, 3):
        normalise_group(*order[k])
        far_group(*order[k], low)
        serve(*order[k + 1])
        if k == 2:
            relay_weights(1)
    take_weights(1)
    for k in range(4):
        far_group(*order[k], high)
    for k in range(4, 16):
        normalise_group(*order[k])
        far_group(*order[k], full)
        if k < 15:
            serve(*order[k + 1])
        if k == 8:
            relay_weights(2)
        if k == 12:
            relay_weights(3)
    take_weights(2)

    def block_rows(blk):
        return pl.ds(pl.multiple_of(blk * BLOCK, BLOCK), BLOCK)

    def step_far(blk, _):
        with jax.named_scope("far"):
            rows = block_rows(blk)
            zs[1, rows, :] = share(xbf[rows, :], 1)
            remote(zs.at[1, rows, :], zr.at[c, rows, :], z_send.at[1], z_recv.at[c, blk], at_row(far * 2 + 1)).start()
        return 0

    lax.fori_loop(0, 16, step_far, 0)
    relay_weights(4)
    take_weights(3)
    take_weights(4)

    def step_own(blk, _):
        with jax.named_scope("own"):
            rows = block_rows(blk)
            xl[0, rows, 256:512] = share(xbf[rows, :], 2 + mate)
            remote(xl.at[0, rows, pl.ds(256, 256)], zp.at[rows, :], zp_send, zp_recv.at[blk], partner).start()
            xl[0, rows, 0:256] = share(xbf[rows, :], 2 + c)
        return 0

    lax.fori_loop(0, 16, step_own, 0)

    def finish(half, blk, mine):
        rows = block_rows(blk)
        with jax.named_scope("wz"):
            drain_recv(zr.at[half, rows, :], z_recv.at[half, blk])
        value = zr[half, rows, :] + mine
        zr[half, rows, :] = value
        pltpu.make_async_copy(
            zr.at[half, rows, :],
            z_hbm.at[pl.ds(pl.multiple_of(half * HALF + blk * BLOCK, BLOCK), BLOCK), :], out_sem.at[half]).start()
        lane = lax.broadcasted_iota(jnp.int32, (BLOCK, 128), 1)
        left, right = value[:, 0:128], jnp.where(lane < WORDS - 128, value[:, 128:256], LOW)
        top = jnp.max(jnp.maximum(left, right).T, axis=0, keepdims=True)
        shift = jnp.broadcast_to(top, (BLOCK, BLOCK)).T
        mass = jnp.exp(left - shift) + jnp.exp(right - shift)
        st[0, pl.ds(half * 16 + blk, 1), :] = top
        st[1, pl.ds(half * 16 + blk, 1), :] = jnp.sum(mass.T, axis=0, keepdims=True)

    def step_out(blk, _):
        rows = block_rows(blk)
        finish(c, blk, xl[0, rows, 0:256])
        drain_recv(zp.at[rows, :], zp_recv.at[blk])
        finish(mate, blk, zp[rows, :])
        return 0

    with jax.named_scope("finish"):
        lax.fori_loop(0, 16, step_out, 0)

    def exchange(buf, me, count, send, recv, dev):
        with jax.named_scope("exch"):
            for d in range(1, count):
                remote(buf.at[me], buf.at[me], send, recv.at[me], dev(lax.rem(me + d, count))).start()
            for d in range(1, count):
                other = lax.rem(me + d, count)
                drain_recv(buf.at[other], recv.at[other])
        top = buf[0]
        for k in range(1, count):
            top = jnp.maximum(top, buf[k])
        mass = jnp.exp(buf[0] - top)
        for k in range(1, count):
            mass = mass + jnp.exp(buf[k] - top)
        return top + jnp.log(mass)

    st1[row] = st[0] + jnp.log(st[1])
    st2[z] = exchange(st1, row, 8, st_send.at[0], st1_recv, at_row)
    st3[y] = exchange(st2, z, 4, st_send.at[1], st2_recv, lambda k: at_col(y, k))
    lse_ref[...] = exchange(st3, y, 4, st_send.at[2], st3_recv, lambda k: at_col(k, z))

    drain_send(ssq.at[pl.ds(0, 7)], ssq_send)
    drain_send(gl, g_send)
    drain_send(wl.at[0], wp_send)
    drain_send(wl.at[0], wb_send)
    drain_send(wl.at[0], wr_send)
    drain_send(xl.at[0], xp_send)
    for f in range(4):
        drain_send(xl.at[pl.ds(1, 2), pl.ds(0, 15 * PIECE), :], xf_send.at[f])
    for n in range(2):
        drain_send(zs.at[n], z_send.at[n])
    drain_send(zp, zp_send)
    drain_send(st1.at[pl.ds(0, 7)], st_send.at[0])
    drain_send(st2.at[pl.ds(0, 3)], st_send.at[1])
    drain_send(st3.at[pl.ds(0, 3)], st_send.at[2])
    for half in range(2):
        pltpu.make_async_copy(zr.at[half], z_hbm.at[pl.ds(half * HALF, HALF), :], out_sem.at[half]).wait()


def solution(mesh):
    dma = pltpu.SemaphoreType.DMA

    def local_head(hidden, norm_gain, w_head):
        logits, log_norm = pl.pallas_call(
            kernel,
            out_shape=(jax.ShapeDtypeStruct((SEQ, PAD), F32), jax.ShapeDtypeStruct((32, 128), F32)),
            in_specs=[pl.BlockSpec(memory_space=pl.ANY), pl.BlockSpec(memory_space=pltpu.VMEM),
                      pl.BlockSpec(memory_space=pl.ANY)],
            out_specs=(pl.BlockSpec(memory_space=pl.ANY), pl.BlockSpec(memory_space=pltpu.VMEM)),
            scratch_shapes=[
                pltpu.VMEM((SEQ, FEAT), BF16),
                pltpu.VMEM((8, PIECE, FEAT), BF16),
                pltpu.VMEM((8, PIECE, FEAT), F32),
                pltpu.VMEM((8 * WORDS, FEAT), BF16),
                pltpu.VMEM((8, PAD, FEAT), F32),
                pltpu.VMEM((3, 4, PAD, FEAT), F32),
                pltpu.VMEM((4, PAD, 4 * FEAT), BF16),
                pltpu.VMEM((HALF, FEAT), F32),
                pltpu.VMEM((3, HALF, FEAT), F32),
                pltpu.VMEM((HALF, 4 * FEAT), BF16),
                pltpu.VMEM((2, HALF, PAD), F32),
                pltpu.VMEM((HALF, PAD), F32),
                pltpu.VMEM((2, HALF, PAD), F32),
                pltpu.VMEM((3, 1, FEAT), F32),
                pltpu.VMEM((8, 32, 128), F32),
                pltpu.VMEM((HALF, 128), F32),
                pltpu.VMEM((2, 32, 128), F32),
                pltpu.VMEM((8, 32, 128), F32),
                pltpu.VMEM((4, 32, 128), F32),
                pltpu.VMEM((4, 32, 128), F32),
                dma((13,)),
                dma, dma((8,)),
                dma, dma((3,)),
                dma, dma((4,)),
                dma, dma((5,)),
                dma, dma((5,)),
                dma, dma((4,)),
                dma, dma((4,)), dma((4, 16)),
                dma((2,)), dma((2, 16)),
                dma, dma((16,)),
                dma((2,)),
                dma((3,)), dma((8,)), dma((4,)), dma((4,)),
            ],
            compiler_params=pltpu.CompilerParams(
                collective_id=0, has_side_effects=True, vmem_limit_bytes=67_043_328),
        )(hidden, norm_gain.reshape(1, FEAT), w_head.T)
        log_norm = log_norm.reshape(SEQ)
        return logits[:, :WORDS] - log_norm[:, None], log_norm

    return jax.shard_map(
        local_head,
        mesh=mesh,
        in_specs=(P("dp", "row"), P("row"), P("row", "col")),
        out_specs=(P("dp", ("col", "row")), P("dp")),
        check_vma=False,
    )
```

```python
import functools

import jax
import jax.numpy as jnp
from jax import lax
from jax.experimental import pallas as pl
from jax.experimental.pallas import tpu as pltpu
from jax.sharding import PartitionSpec as P

EPS = 1e-5
MESH = pl.DeviceIdType.MESH
F32 = jnp.float32
BF16 = jnp.bfloat16
LOW = -3.0e38

SEQ, FEAT, WORDS, PAD = 4096, 512, 250, 256
HALF = SEQ // 2
BLOCK, PIECE, WAVE = 128, 32, 16


def kernel(h_hbm, g_ref, w_hbm, z_hbm, lse_ref,
           h, hp16, hp, w, wst, wl, wbf, xst, xl, xbf, zs, zp, zr, gl, ssq, rcol, st, st1, st2, st3,
           in_sem, ssq_send, ssq_recv, g_send, g_recv, wp_send, wp_recv, wb_send, wb_recv, wr_send, wr_recv,
           xp_send, xp_recv, xb_send, xf_send, x_recv, z_send, z_recv, zp_send, zp_recv,
           out_sem, st_send, st1_recv, st2_recv, st3_recv):
    col, row = lax.axis_index("col"), lax.axis_index("row")
    z, y = lax.div(col, 4), lax.rem(col, 4)
    x, c = lax.div(row, 2), lax.rem(row, 2)
    mate = 1 - c
    near = x + 1 - 2 * lax.rem(x, 2)
    far = 3 - x

    def at_row(r):
        return (0, col, r)

    def at_col(yy, zz):
        return (0, zz * 4 + yy, row)

    partner = at_row(x * 2 + mate)
    near_same = at_row(near * 2 + c)
    near_other = at_row(near * 2 + mate)

    def remote(src, dst, send, recv, dev):
        return pltpu.make_async_remote_copy(
            src_ref=src, dst_ref=dst, send_sem=send, recv_sem=recv, device_id=dev, device_id_type=MESH)

    def drain_send(ref, sem):
        remote(ref, ref, sem, sem, partner).wait_send()

    def drain_recv(ref, sem):
        remote(ref, ref, sem, sem, partner).wait_recv()

    firsts, seconds = (y, y, z, z), (z, z, y, y)
    signs = (1, -1, 1, -1)

    def first(f, i):
        return lax.rem(firsts[f] - signs[f] * i + 4, 4)

    def second(f, j):
        return lax.rem(seconds[f] - signs[f] * j + 4, 4)

    def piece_base(f, i, j):
        return f * 512 + first(f, i) * BLOCK + second(f, j) * PIECE

    def piece_rows(f, i, j, offset=0):
        return pl.ds(pl.multiple_of(offset + piece_base(f, i, j), PIECE), PIECE)

    def wave_rows(f, t, offset=0):
        v, i, j = t
        return pl.ds(pl.multiple_of(offset + v * WAVE + piece_base(f, i, j), WAVE), WAVE)

    own_pieces = [(f, core) for f in range(4) for core in range(2)]

    def load_piece(f, core):
        return pltpu.make_async_copy(
            h_hbm.at[piece_rows(f, 0, 0, core * HALF), :], hp16.at[f * 2 + core], in_sem.at[5 + f * 2 + core])

    def load_h(k):
        rows = pl.ds(k * 1024, 1024)
        return pltpu.make_async_copy(h_hbm.at[rows, :], h.at[rows, :], in_sem.at[k])

    for f, core in own_pieces:
        load_piece(f, core).start()
    w_in = pltpu.make_async_copy(w_hbm, w, in_sem.at[4])
    w_in.start()
    for k in range(4):
        load_h(k).start()

    barrier = pltpu.get_barrier_semaphore()
    peers = [at_row(lax.rem(row + d, 8)) for d in range(1, 8)]
    peers += [at_col(lax.rem(y + d, 4), z) for d in range(1, 4)]
    peers += [at_col(y, lax.rem(z + d, 4)) for d in range(1, 4)]
    for dev in peers:
        pl.semaphore_signal(barrier, inc=1, device_id=dev, device_id_type=MESH)

    for f, core in own_pieces:
        load_piece(f, core).wait()
        hp[f * 2 + core] = hp16[f * 2 + core].astype(F32)
    with jax.named_scope("bar"):
        pl.semaphore_wait(barrier, len(peers))

    def send_pieces(v):
        for f, core in own_pieces:
            slot = 1 + (core + c) - 2 * core * c
            remote(hp.at[f * 2 + core, pl.ds(v * WAVE, WAVE), :], xl.at[slot, wave_rows(f, (v, 0, 0)), :],
                   xb_send.at[v], x_recv.at[f, v * 16], at_row(near * 2 + core)).start()

    send_pieces(0)
    for slot, dev in enumerate((partner, near_same, near_other)):
        remote(g_ref, gl.at[slot], g_send, g_recv.at[slot], dev).start()

    w_in.wait()

    def prep(b, rows):
        start = rows // 16 * 16
        for q in range(4):
            lanes = slice(q * 128, (q + 1) * 128)
            wide = w[start:min(start + 272, 8 * WORDS), lanes].astype(F32)
            part = wide[rows - start:rows - start + WORDS, :]
            wst[b, :, lanes] = jnp.concatenate([part, jnp.zeros((PAD - WORDS, 128), F32)], axis=0)

    with jax.named_scope("prep"):
        for b in range(8):
            prep(b, b * WORDS)

    def kind_block(chip, n):
        return ((3 - chip) * 2 + n) if n < 2 else (chip * 2 + n - 2)

    parts = ((0, 0, 128), (0, 128, 128), (1, 0, PAD), (2, 0, PAD), (3, 0, PAD))

    def send_near(p):
        n, w0, size = parts[p]
        rows = pl.ds(w0, size)
        remote(wst.at[kind_block(near, n), rows, :], wl.at[1, n, rows, :], wb_send, wb_recv.at[p], near_same).start()

    for n in range(4):
        remote(wst.at[kind_block(x, n)], wl.at[0, n], wp_send, wp_recv.at[n], partner).start()

    for k in range(4):
        load_h(k).wait()

        def squares(t, _, k=k):
            b = k * 8 + t
            hb = h[pl.ds(pl.multiple_of(b * BLOCK, BLOCK), BLOCK), :].astype(F32)
            sq = hb * hb
            part = (sq[:, 0:128] + sq[:, 128:256]) + (sq[:, 256:384] + sq[:, 384:512])
            ssq[row, pl.ds(b, 1), :] = jnp.sum(part.T, axis=0, keepdims=True)
            return 0

        with jax.named_scope("squares"):
            lax.fori_loop(0, 8, squares, 0)
    for d in range(1, 8):
        remote(ssq.at[row], ssq.at[row], ssq_send, ssq_recv.at[row], at_row(lax.rem(row + d, 8))).start()

    for f in range(4):
        rows = pl.ds(f * 512, 512)
        xst[rows, :] = h[pl.ds(pl.multiple_of(mate * HALF + f * 512, 512), 512), :].astype(F32)
        remote(xst.at[rows, :], xl.at[0, rows, :], xp_send, xp_recv.at[f], partner).start()

    def relay_weights(p):
        n, w0, size = parts[p]
        rows = pl.ds(w0, size)
        with jax.named_scope("wrelay"):
            drain_recv(wl.at[1, n, rows, :], wb_recv.at[p])
        remote(wl.at[1, n, rows, :], wl.at[2, n, rows, :], wr_send, wr_recv.at[p], partner).start()

    def take_weights(p):
        n, w0, size = parts[p]
        rows = pl.ds(w0, size)
        with jax.named_scope("wtake"):
            if w0 == 0:
                drain_recv(wl.at[0, n], wp_recv.at[n])
            drain_recv(wl.at[2, n, rows, :], wr_recv.at[p])
        wbf[n, rows, 0:512] = wst[kind_block(x, n), rows, :].astype(BF16)
        for k in range(3):
            wbf[n, rows, (k + 1) * 512:(k + 2) * 512] = wl[k, n, rows, :].astype(BF16)

    ups = (at_col(lax.rem(y + 1, 4), z), at_col(lax.rem(y + 3, 4), z),
           at_col(y, lax.rem(z + 1, 4)), at_col(y, lax.rem(z + 3, 4)))
    along_first = (ups[0], ups[1], ups[2], ups[3])
    along_second = (ups[2], ups[3], ups[0], ups[1])

    def step_of(n):
        i = 3 - lax.rem(n, 4)
        reach = lax.div(n, 4) - i
        return reach, (lax.div(reach, 4), i, lax.rem(reach, 4))

    def each(lo, hi, body):
        def at(n, _):
            reach, t = step_of(n)

            @pl.when((reach >= 0) & (reach < 8))
            def _():
                body(t)
            return 0

        lax.fori_loop(lo, hi, at, 0)

    def serve(t, flows=(0, 1, 2, 3)):
        v, i, j = t
        with jax.named_scope("serve"):
            for f in flows:
                ref = xl.at[pl.ds(1, 2), wave_rows(f, t), :]
                step = v * 16 + i * 4 + j
                drain_recv(ref, x_recv.at[f, step])

                @pl.when((j == 0) & (i < 3))
                def _():
                    remote(ref, ref, xf_send.at[f], x_recv.at[f, step + 4], along_first[f]).start()

                @pl.when(j < 3)
                def _():
                    remote(ref, ref, xf_send.at[f], x_recv.at[f, step + 1], along_second[f]).start()

    def scales():
        with jax.named_scope("wssq"):
            for d in range(1, 8):
                r = lax.rem(row + d, 8)
                drain_recv(ssq.at[r], ssq_recv.at[r])
            for slot in range(3):
                drain_recv(gl.at[slot], g_recv.at[slot])
        mine = pl.ds(pl.multiple_of(c * 16, 16), 16)
        total = ssq[0, mine, :]
        for r in range(1, 8):
            total = total + ssq[r, mine, :]
        inv = lax.rsqrt(total / (FEAT * 8) + EPS)
        for b in range(16):
            rcol[b * BLOCK:(b + 1) * BLOCK, :] = jnp.broadcast_to(inv[b:b + 1, :], (BLOCK, BLOCK)).T

    def normalise(f, t):
        rows = wave_rows(f, t)
        scale = rcol[rows, :]
        for k in range(4):
            for q in range(4):
                lanes = slice(q * 128, (q + 1) * 128)
                if k == 0:
                    raw, gain = h[wave_rows(f, t, c * HALF), lanes].astype(F32), g_ref[:, lanes]
                else:
                    raw, gain = xl[k - 1, rows, lanes], gl[k - 1, :, lanes]
                xbf[rows, k * 512 + q * 128:k * 512 + (q + 1) * 128] = (raw * scale * gain).astype(BF16)

    def share(left, n, rows=slice(0, PAD)):
        return lax.dot_general(left, wbf[n, rows, :], (((1,), (1,)), ((), ())), preferred_element_type=F32)

    def far_group(t, words):
        with jax.named_scope("group"):
            left = jnp.concatenate([xbf[wave_rows(f, t), :] for f in range(4)], axis=0)
            value = share(left, 0, words)
            lanes = pl.ds(words.start, words.stop - words.start)
            for f in range(4):
                rows = wave_rows(f, t)
                zs[0, rows, words] = value[f * WAVE:(f + 1) * WAVE, :]
                remote(zs.at[0, rows, lanes], zr.at[c, rows, lanes], z_send.at[0],
                       z_recv.at[c, f * 4 + first(f, t[1])], at_row(far * 2)).start()

    def normalise_group(t):
        with jax.named_scope("norm"):
            for f in range(4):
                normalise(f, t)

    low, high, full = slice(0, 128), slice(128, PAD), slice(0, PAD)
    origin = tuple(jnp.int32(0) for _ in range(3))
    serve(origin, (0, 1))
    drain_send(xl.at[0, pl.ds(0, 128), :], xb_send.at[0])
    send_near(0)
    send_near(1)
    serve(origin, (2, 3))
    each(4, 8, serve)
    scales()
    for f in range(4):
        drain_recv(xl.at[0, pl.ds(f * 512, 512), :], xp_recv.at[f])
    relay_weights(0)
    each(0, 8, normalise_group)
    each(8, 10, serve)
    take_weights(0)
    each(0, 8, lambda t: far_group(t, low))

    def low_step(t):
        normalise_group(t)
        far_group(t, low)

    each(8, 10, low_step)
    each(10, 12, lambda t: (serve(t), low_step(t)))
    each(12, 14, lambda t: (serve(t), low_step(t)))
    relay_weights(1)
    send_pieces(1)
    each(14, 16, lambda t: (serve(t), low_step(t)))
    take_weights(1)
    each(0, 16, lambda t: far_group(t, high))

    def full_step(t):
        serve(t)
        normalise_group(t)
        far_group(t, full)

    each(16, 20, full_step)
    send_near(2)
    each(20, 32, full_step)
    relay_weights(2)
    send_near(3)
    each(32, 44, full_step)
    relay_weights(3)
    send_near(4)
    take_weights(2)

    def block_rows(blk):
        return pl.ds(pl.multiple_of(blk * BLOCK, BLOCK), BLOCK)

    def step_far(blk, _):
        with jax.named_scope("far"):
            rows = block_rows(blk)
            zs[1, rows, :] = share(xbf[rows, :], 1)
            remote(zs.at[1, rows, :], zr.at[c, rows, :], z_send.at[1], z_recv.at[c, blk], at_row(far * 2 + 1)).start()
        return 0

    lax.fori_loop(0, 16, step_far, 0)
    relay_weights(4)
    take_weights(3)
    take_weights(4)

    def step_own(blk, _):
        with jax.named_scope("own"):
            rows = block_rows(blk)
            xl[0, rows, 256:512] = share(xbf[rows, :], 2 + mate)
            remote(xl.at[0, rows, pl.ds(256, 256)], zp.at[rows, :], zp_send, zp_recv.at[blk], partner).start()
            xl[0, rows, 0:256] = share(xbf[rows, :], 2 + c)
        return 0

    lax.fori_loop(0, 16, step_own, 0)

    def finish(half, blk, mine):
        rows = block_rows(blk)
        with jax.named_scope("wz"):
            drain_recv(zr.at[half, rows, :], z_recv.at[half, blk])
        value = zr[half, rows, :] + mine
        zr[half, rows, :] = value
        pltpu.make_async_copy(
            zr.at[half, rows, :],
            z_hbm.at[pl.ds(pl.multiple_of(half * HALF + blk * BLOCK, BLOCK), BLOCK), :], out_sem.at[half]).start()
        lane = lax.broadcasted_iota(jnp.int32, (BLOCK, 128), 1)
        left, right = value[:, 0:128], jnp.where(lane < WORDS - 128, value[:, 128:256], LOW)
        top = jnp.max(jnp.maximum(left, right).T, axis=0, keepdims=True)
        shift = jnp.broadcast_to(top, (BLOCK, BLOCK)).T
        mass = jnp.exp(left - shift) + jnp.exp(right - shift)
        st[0, pl.ds(half * 16 + blk, 1), :] = top
        st[1, pl.ds(half * 16 + blk, 1), :] = jnp.sum(mass.T, axis=0, keepdims=True)

    def step_out(blk, _):
        rows = block_rows(blk)
        finish(c, blk, xl[0, rows, 0:256])
        drain_recv(zp.at[rows, :], zp_recv.at[blk])
        finish(mate, blk, zp[rows, :])
        return 0

    with jax.named_scope("finish"):
        lax.fori_loop(0, 16, step_out, 0)

    def exchange(buf, me, count, send, recv, dev):
        with jax.named_scope("exch"):
            for d in range(1, count):
                remote(buf.at[me], buf.at[me], send, recv.at[me], dev(lax.rem(me + d, count))).start()
            for d in range(1, count):
                other = lax.rem(me + d, count)
                drain_recv(buf.at[other], recv.at[other])
        top = buf[0]
        for k in range(1, count):
            top = jnp.maximum(top, buf[k])
        mass = jnp.exp(buf[0] - top)
        for k in range(1, count):
            mass = mass + jnp.exp(buf[k] - top)
        return top + jnp.log(mass)

    st1[row] = st[0] + jnp.log(st[1])
    st2[z] = exchange(st1, row, 8, st_send.at[0], st1_recv, at_row)
    st3[y] = exchange(st2, z, 4, st_send.at[1], st2_recv, lambda k: at_col(y, k))
    lse_ref[...] = exchange(st3, y, 4, st_send.at[2], st3_recv, lambda k: at_col(k, z))

    drain_send(ssq.at[pl.ds(0, 7)], ssq_send)
    drain_send(gl, g_send)
    drain_send(wl.at[0], wp_send)
    drain_send(wl.at[0], wb_send)
    drain_send(wl.at[0], wr_send)
    drain_send(xl.at[0], xp_send)
    drain_send(xl.at[0, pl.ds(0, 128), :], xb_send.at[1])
    for f in range(4):
        drain_send(xl.at[pl.ds(1, 2), pl.ds(0, 15 * PIECE), :], xf_send.at[f])
    for n in range(2):
        drain_send(zs.at[n], z_send.at[n])
    drain_send(zp, zp_send)
    drain_send(st1.at[pl.ds(0, 7)], st_send.at[0])
    drain_send(st2.at[pl.ds(0, 3)], st_send.at[1])
    drain_send(st3.at[pl.ds(0, 3)], st_send.at[2])
    for half in range(2):
        pltpu.make_async_copy(zr.at[half], z_hbm.at[pl.ds(half * HALF, HALF), :], out_sem.at[half]).wait()


def solution(mesh):
    dma = pltpu.SemaphoreType.DMA

    def local_head(hidden, norm_gain, w_head):
        logits, log_norm = pl.pallas_call(
            kernel,
            out_shape=(jax.ShapeDtypeStruct((SEQ, PAD), F32), jax.ShapeDtypeStruct((32, 128), F32)),
            in_specs=[pl.BlockSpec(memory_space=pl.ANY), pl.BlockSpec(memory_space=pltpu.VMEM),
                      pl.BlockSpec(memory_space=pl.ANY)],
            out_specs=(pl.BlockSpec(memory_space=pl.ANY), pl.BlockSpec(memory_space=pltpu.VMEM)),
            scratch_shapes=[
                pltpu.VMEM((SEQ, FEAT), BF16),
                pltpu.VMEM((8, PIECE, FEAT), BF16),
                pltpu.VMEM((8, PIECE, FEAT), F32),
                pltpu.VMEM((8 * WORDS, FEAT), BF16),
                pltpu.VMEM((8, PAD, FEAT), F32),
                pltpu.VMEM((3, 4, PAD, FEAT), F32),
                pltpu.VMEM((4, PAD, 4 * FEAT), BF16),
                pltpu.VMEM((HALF, FEAT), F32),
                pltpu.VMEM((3, HALF, FEAT), F32),
                pltpu.VMEM((HALF, 4 * FEAT), BF16),
                pltpu.VMEM((2, HALF, PAD), F32),
                pltpu.VMEM((HALF, PAD), F32),
                pltpu.VMEM((2, HALF, PAD), F32),
                pltpu.VMEM((3, 1, FEAT), F32),
                pltpu.VMEM((8, 32, 128), F32),
                pltpu.VMEM((HALF, 128), F32),
                pltpu.VMEM((2, 32, 128), F32),
                pltpu.VMEM((8, 32, 128), F32),
                pltpu.VMEM((4, 32, 128), F32),
                pltpu.VMEM((4, 32, 128), F32),
                dma((13,)),
                dma, dma((8,)),
                dma, dma((3,)),
                dma, dma((4,)),
                dma, dma((5,)),
                dma, dma((5,)),
                dma, dma((4,)),
                dma((2,)), dma((4,)), dma((4, 32)),
                dma((2,)), dma((2, 16)),
                dma, dma((16,)),
                dma((2,)),
                dma((3,)), dma((8,)), dma((4,)), dma((4,)),
            ],
            compiler_params=pltpu.CompilerParams(
                collective_id=0, has_side_effects=True, vmem_limit_bytes=67_043_328),
        )(hidden, norm_gain.reshape(1, FEAT), w_head.T)
        log_norm = log_norm.reshape(SEQ)
        return logits[:, :WORDS] - log_norm[:, None], log_norm

    return jax.shard_map(
        local_head,
        mesh=mesh,
        in_specs=(P("dp", "row"), P("row"), P("row", "col")),
        out_specs=(P("dp", ("col", "row")), P("dp")),
        check_vma=False,
    )
```

```python
import functools

import jax
import jax.numpy as jnp
from jax import lax
from jax.experimental import pallas as pl
from jax.experimental.pallas import tpu as pltpu
from jax.sharding import PartitionSpec as P

EPS = 1e-5
MESH = pl.DeviceIdType.MESH
F32 = jnp.float32
BF16 = jnp.bfloat16
LOW = -3.0e38

SEQ, FEAT, WORDS, PAD = 4096, 512, 250, 256
HALF = SEQ // 2
BLOCK, PIECE, WAVE = 128, 32, 16


def kernel(h_hbm, g_ref, w_hbm, z_ref, lse_ref,
           h, hp16, hp, w, wst, wl, wbf, xst, xl, xbf, zs, zp, zr, gl, ssq, rcol, st, st1, st2, st3,
           in_sem, ssq_send, ssq_recv, g_send, g_recv, wp_send, wp_recv, wb_send, wb_recv, wr_send, wr_recv,
           xp_send, xp_recv, xb_send, xf_send, x_recv, z_send, z_recv, zp_send, zp_recv,
           st_send, st1_recv, st2_recv, st3_recv):
    col, row = lax.axis_index("col"), lax.axis_index("row")
    z, y = lax.div(col, 4), lax.rem(col, 4)
    x, c = lax.div(row, 2), lax.rem(row, 2)
    mate = 1 - c
    near = x + 1 - 2 * lax.rem(x, 2)
    far = 3 - x

    def at_row(r):
        return (0, col, r)

    def at_col(yy, zz):
        return (0, zz * 4 + yy, row)

    partner = at_row(x * 2 + mate)
    near_same = at_row(near * 2 + c)
    near_other = at_row(near * 2 + mate)

    def remote(src, dst, send, recv, dev):
        return pltpu.make_async_remote_copy(
            src_ref=src, dst_ref=dst, send_sem=send, recv_sem=recv, device_id=dev, device_id_type=MESH)

    def drain_send(ref, sem):
        remote(ref, ref, sem, sem, partner).wait_send()

    def drain_recv(ref, sem):
        remote(ref, ref, sem, sem, partner).wait_recv()

    firsts, seconds = (y, y, z, z), (z, z, y, y)
    signs = (1, -1, 1, -1)

    def first(f, i):
        return lax.rem(firsts[f] - signs[f] * i + 4, 4)

    def second(f, j):
        return lax.rem(seconds[f] - signs[f] * j + 4, 4)

    def piece_base(f, i, j):
        return f * 512 + first(f, i) * BLOCK + second(f, j) * PIECE

    def piece_rows(f, i, j, offset=0):
        return pl.ds(pl.multiple_of(offset + piece_base(f, i, j), PIECE), PIECE)

    def wave_rows(f, t, offset=0):
        v, i, j = t
        return pl.ds(pl.multiple_of(offset + v * WAVE + piece_base(f, i, j), WAVE), WAVE)

    own_pieces = [(f, core) for f in range(4) for core in range(2)]

    def load_piece(f, core):
        return pltpu.make_async_copy(
            h_hbm.at[piece_rows(f, 0, 0, core * HALF), :], hp16.at[f * 2 + core], in_sem.at[5 + f * 2 + core])

    def load_h(k):
        rows = pl.ds(k * 1024, 1024)
        return pltpu.make_async_copy(h_hbm.at[rows, :], h.at[rows, :], in_sem.at[k])

    for f, core in own_pieces:
        load_piece(f, core).start()
    w_in = pltpu.make_async_copy(w_hbm, w, in_sem.at[4])
    w_in.start()
    for k in range(4):
        load_h(k).start()

    barrier = pltpu.get_barrier_semaphore()
    peers = [at_row(lax.rem(row + d, 8)) for d in range(1, 8)]
    peers += [at_col(lax.rem(y + d, 4), z) for d in range(1, 4)]
    peers += [at_col(y, lax.rem(z + d, 4)) for d in range(1, 4)]
    for dev in peers:
        pl.semaphore_signal(barrier, inc=1, device_id=dev, device_id_type=MESH)

    for f, core in own_pieces:
        load_piece(f, core).wait()
        hp[f * 2 + core] = hp16[f * 2 + core].astype(F32)
    with jax.named_scope("bar"):
        pl.semaphore_wait(barrier, len(peers))

    def send_pieces(v):
        for f, core in own_pieces:
            slot = 1 + (core + c) - 2 * core * c
            remote(hp.at[f * 2 + core, pl.ds(v * WAVE, WAVE), :], xl.at[slot, wave_rows(f, (v, 0, 0)), :],
                   xb_send.at[v], x_recv.at[f, v * 16], at_row(near * 2 + core)).start()

    send_pieces(0)
    for slot, dev in enumerate((partner, near_same, near_other)):
        remote(g_ref, gl.at[slot], g_send, g_recv.at[slot], dev).start()

    w_in.wait()

    def prep(b, rows):
        start = rows // 16 * 16
        for q in range(4):
            lanes = slice(q * 128, (q + 1) * 128)
            wide = w[start:min(start + 272, 8 * WORDS), lanes].astype(F32)
            part = wide[rows - start:rows - start + WORDS, :]
            wst[b, :, lanes] = jnp.concatenate([part, jnp.zeros((PAD - WORDS, 128), F32)], axis=0)

    with jax.named_scope("prep"):
        for b in range(8):
            prep(b, b * WORDS)

    def kind_block(chip, n):
        return ((3 - chip) * 2 + n) if n < 2 else (chip * 2 + n - 2)

    parts = ((0, 0, 128), (0, 128, 128), (1, 0, PAD), (2, 0, PAD), (3, 0, PAD))

    def send_near(p):
        n, w0, size = parts[p]
        rows = pl.ds(w0, size)
        remote(wst.at[kind_block(near, n), rows, :], wl.at[1, n, rows, :], wb_send, wb_recv.at[p], near_same).start()

    for n in range(4):
        remote(wst.at[kind_block(x, n)], wl.at[0, n], wp_send, wp_recv.at[n], partner).start()

    for k in range(4):
        load_h(k).wait()

        def squares(t, _, k=k):
            b = k * 8 + t
            hb = h[pl.ds(pl.multiple_of(b * BLOCK, BLOCK), BLOCK), :].astype(F32)
            sq = hb * hb
            part = (sq[:, 0:128] + sq[:, 128:256]) + (sq[:, 256:384] + sq[:, 384:512])
            ssq[row, pl.ds(b, 1), :] = jnp.sum(part.T, axis=0, keepdims=True)
            return 0

        with jax.named_scope("squares"):
            lax.fori_loop(0, 8, squares, 0)
    for d in range(1, 8):
        remote(ssq.at[row], ssq.at[row], ssq_send, ssq_recv.at[row], at_row(lax.rem(row + d, 8))).start()

    for f in range(4):
        rows = pl.ds(f * 512, 512)
        xst[rows, :] = h[pl.ds(pl.multiple_of(mate * HALF + f * 512, 512), 512), :].astype(F32)
        remote(xst.at[rows, :], xl.at[0, rows, :], xp_send, xp_recv.at[f], partner).start()

    def relay_weights(p):
        n, w0, size = parts[p]
        rows = pl.ds(w0, size)
        with jax.named_scope("wrelay"):
            drain_recv(wl.at[1, n, rows, :], wb_recv.at[p])
        remote(wl.at[1, n, rows, :], wl.at[2, n, rows, :], wr_send, wr_recv.at[p], partner).start()

    def take_weights(p):
        n, w0, size = parts[p]
        rows = pl.ds(w0, size)
        with jax.named_scope("wtake"):
            if w0 == 0:
                drain_recv(wl.at[0, n], wp_recv.at[n])
            drain_recv(wl.at[2, n, rows, :], wr_recv.at[p])
        wbf[n, rows, 0:512] = wst[kind_block(x, n), rows, :].astype(BF16)
        for k in range(3):
            wbf[n, rows, (k + 1) * 512:(k + 2) * 512] = wl[k, n, rows, :].astype(BF16)

    ups = (at_col(lax.rem(y + 1, 4), z), at_col(lax.rem(y + 3, 4), z),
           at_col(y, lax.rem(z + 1, 4)), at_col(y, lax.rem(z + 3, 4)))
    along_first = (ups[0], ups[1], ups[2], ups[3])
    along_second = (ups[2], ups[3], ups[0], ups[1])

    def step_of(n):
        i = 3 - lax.rem(n, 4)
        reach = lax.div(n, 4) - i
        return reach, (lax.div(reach, 4), i, lax.rem(reach, 4))

    def each(lo, hi, body):
        def at(n, _):
            reach, t = step_of(n)

            @pl.when((reach >= 0) & (reach < 8))
            def _():
                body(t)
            return 0

        lax.fori_loop(lo, hi, at, 0)

    def serve(t, flows=(0, 1, 2, 3)):
        v, i, j = t
        with jax.named_scope("serve"):
            for f in flows:
                ref = xl.at[pl.ds(1, 2), wave_rows(f, t), :]
                step = v * 16 + i * 4 + j
                drain_recv(ref, x_recv.at[f, step])

                @pl.when((j == 0) & (i < 3))
                def _():
                    remote(ref, ref, xf_send.at[f], x_recv.at[f, step + 4], along_first[f]).start()

                @pl.when(j < 3)
                def _():
                    remote(ref, ref, xf_send.at[f], x_recv.at[f, step + 1], along_second[f]).start()

    def scales():
        with jax.named_scope("wssq"):
            for d in range(1, 8):
                r = lax.rem(row + d, 8)
                drain_recv(ssq.at[r], ssq_recv.at[r])
            for slot in range(3):
                drain_recv(gl.at[slot], g_recv.at[slot])
        mine = pl.ds(pl.multiple_of(c * 16, 16), 16)
        total = ssq[0, mine, :]
        for r in range(1, 8):
            total = total + ssq[r, mine, :]
        inv = lax.rsqrt(total / (FEAT * 8) + EPS)
        for b in range(16):
            rcol[b * BLOCK:(b + 1) * BLOCK, :] = jnp.broadcast_to(inv[b:b + 1, :], (BLOCK, BLOCK)).T

    def normalise(f, t):
        rows = wave_rows(f, t)
        scale = rcol[rows, :]
        for k in range(4):
            for q in range(4):
                lanes = slice(q * 128, (q + 1) * 128)
                if k == 0:
                    raw, gain = h[wave_rows(f, t, c * HALF), lanes].astype(F32), g_ref[:, lanes]
                else:
                    raw, gain = xl[k - 1, rows, lanes], gl[k - 1, :, lanes]
                xbf[rows, k * 512 + q * 128:k * 512 + (q + 1) * 128] = (raw * scale * gain).astype(BF16)

    def share(left, n, rows=slice(0, PAD)):
        return lax.dot_general(left, wbf[n, rows, :], (((1,), (1,)), ((), ())), preferred_element_type=F32)

    def far_group(t, words):
        with jax.named_scope("group"):
            left = jnp.concatenate([xbf[wave_rows(f, t), :] for f in range(4)], axis=0)
            value = share(left, 0, words)
            lanes = pl.ds(words.start, words.stop - words.start)
            for f in range(4):
                rows = wave_rows(f, t)
                zs[0, rows, words] = value[f * WAVE:(f + 1) * WAVE, :]
                remote(zs.at[0, rows, lanes], zr.at[c, rows, lanes], z_send.at[0],
                       z_recv.at[c, f * 4 + first(f, t[1])], at_row(far * 2)).start()

    def normalise_group(t):
        with jax.named_scope("norm"):
            for f in range(4):
                normalise(f, t)

    low, high, full = slice(0, 128), slice(128, PAD), slice(0, PAD)
    origin = tuple(jnp.int32(0) for _ in range(3))
    serve(origin, (0, 1))
    drain_send(xl.at[0, pl.ds(0, 128), :], xb_send.at[0])
    send_near(0)
    send_near(1)
    serve(origin, (2, 3))
    each(4, 8, serve)
    scales()
    for f in range(4):
        drain_recv(xl.at[0, pl.ds(f * 512, 512), :], xp_recv.at[f])
    relay_weights(0)
    each(0, 8, normalise_group)
    each(8, 10, serve)
    take_weights(0)
    each(0, 8, lambda t: far_group(t, low))

    def low_step(t):
        normalise_group(t)
        far_group(t, low)

    each(8, 10, low_step)
    each(10, 12, lambda t: (serve(t), low_step(t)))
    relay_weights(1)
    send_pieces(1)
    for p in (2, 3, 4):
        send_near(p)
    each(12, 13, serve)
    take_weights(1)
    each(0, 12, lambda t: far_group(t, high))

    def full_step(t):
        normalise_group(t)
        far_group(t, full)

    each(12, 13, full_step)

    def ring_step(t):
        serve(t)
        full_step(t)

    each(13, 26, ring_step)
    relay_weights(2)
    each(26, 38, ring_step)
    relay_weights(3)
    each(38, 44, ring_step)
    take_weights(2)

    def block_rows(blk):
        return pl.ds(pl.multiple_of(blk * BLOCK, BLOCK), BLOCK)

    def step_far(blk, _):
        with jax.named_scope("far"):
            rows = block_rows(blk)
            zs[1, rows, :] = share(xbf[rows, :], 1)
            remote(zs.at[1, rows, :], zr.at[c, rows, :], z_send.at[1], z_recv.at[c, blk], at_row(far * 2 + 1)).start()
        return 0

    lax.fori_loop(0, 8, step_far, 0)
    relay_weights(4)
    lax.fori_loop(8, 16, step_far, 0)
    take_weights(3)
    take_weights(4)

    def pair_rows(pair):
        return pl.ds(pl.multiple_of(pair * 256, 256), 256)

    def step_own(pair, _):
        with jax.named_scope("own"):
            rows = pair_rows(pair)
            xl[0, rows, 256:512] = share(xbf[rows, :], 2 + mate)
            remote(xl.at[0, rows, pl.ds(256, 256)], zp.at[rows, :], zp_send, zp_recv.at[pair], partner).start()
            xl[0, rows, 0:256] = share(xbf[rows, :], 2 + c)
        return 0

    lax.fori_loop(0, 8, step_own, 0)

    def finish(half, blk, mine):
        rows = block_rows(blk)
        with jax.named_scope("wz"):
            drain_recv(zr.at[half, rows, :], z_recv.at[half, blk])
        value = zr[half, rows, :] + mine
        z_ref[pl.ds(pl.multiple_of(half * HALF + blk * BLOCK, BLOCK), BLOCK), :] = value
        lane = lax.broadcasted_iota(jnp.int32, (BLOCK, 128), 1)
        left, right = value[:, 0:128], jnp.where(lane < WORDS - 128, value[:, 128:256], LOW)
        top = jnp.max(jnp.maximum(left, right).T, axis=0, keepdims=True)
        shift = jnp.broadcast_to(top, (BLOCK, BLOCK)).T
        mass = jnp.exp(left - shift) + jnp.exp(right - shift)
        st[0, pl.ds(half * 16 + blk, 1), :] = top
        st[1, pl.ds(half * 16 + blk, 1), :] = jnp.sum(mass.T, axis=0, keepdims=True)

    def step_out(blk, _):
        rows = block_rows(blk)
        finish(c, blk, xl[0, rows, 0:256])

        @pl.when(lax.rem(blk, 2) == 0)
        def _():
            pair = lax.div(blk, 2)
            drain_recv(zp.at[pair_rows(pair), :], zp_recv.at[pair])

        finish(mate, blk, zp[rows, :])
        return 0

    with jax.named_scope("finish"):
        lax.fori_loop(0, 16, step_out, 0)

    def exchange(buf, me, count, send, recv, dev):
        with jax.named_scope("exch"):
            for d in range(1, count):
                remote(buf.at[me], buf.at[me], send, recv.at[me], dev(lax.rem(me + d, count))).start()
            for d in range(1, count):
                other = lax.rem(me + d, count)
                drain_recv(buf.at[other], recv.at[other])
        top = buf[0]
        for k in range(1, count):
            top = jnp.maximum(top, buf[k])
        mass = jnp.exp(buf[0] - top)
        for k in range(1, count):
            mass = mass + jnp.exp(buf[k] - top)
        return top + jnp.log(mass)

    st1[row] = st[0] + jnp.log(st[1])
    st2[z] = exchange(st1, row, 8, st_send.at[0], st1_recv, at_row)
    st3[y] = exchange(st2, z, 4, st_send.at[1], st2_recv, lambda k: at_col(y, k))
    lse_ref[...] = exchange(st3, y, 4, st_send.at[2], st3_recv, lambda k: at_col(k, z))

    drain_send(ssq.at[pl.ds(0, 7)], ssq_send)
    drain_send(gl, g_send)
    drain_send(wl.at[0], wp_send)
    drain_send(wl.at[0], wb_send)
    drain_send(wl.at[0], wr_send)
    drain_send(xl.at[0], xp_send)
    drain_send(xl.at[0, pl.ds(0, 128), :], xb_send.at[1])
    for f in range(4):
        drain_send(xl.at[pl.ds(1, 2), pl.ds(0, 15 * PIECE), :], xf_send.at[f])
    for n in range(2):
        drain_send(zs.at[n], z_send.at[n])
    drain_send(zp, zp_send)
    drain_send(st1.at[pl.ds(0, 7)], st_send.at[0])
    drain_send(st2.at[pl.ds(0, 3)], st_send.at[1])
    drain_send(st3.at[pl.ds(0, 3)], st_send.at[2])


def solution(mesh):
    dma = pltpu.SemaphoreType.DMA

    def local_head(hidden, norm_gain, w_head):
        logits, log_norm = pl.pallas_call(
            kernel,
            out_shape=(pltpu.VMEM((SEQ, PAD), F32), jax.ShapeDtypeStruct((32, 128), F32)),
            in_specs=[pl.BlockSpec(memory_space=pl.ANY), pl.BlockSpec(memory_space=pltpu.VMEM),
                      pl.BlockSpec(memory_space=pl.ANY)],
            out_specs=(pl.BlockSpec(memory_space=pltpu.VMEM), pl.BlockSpec(memory_space=pltpu.VMEM)),
            scratch_shapes=[
                pltpu.VMEM((SEQ, FEAT), BF16),
                pltpu.VMEM((8, PIECE, FEAT), BF16),
                pltpu.VMEM((8, PIECE, FEAT), F32),
                pltpu.VMEM((8 * WORDS, FEAT), BF16),
                pltpu.VMEM((8, PAD, FEAT), F32),
                pltpu.VMEM((3, 4, PAD, FEAT), F32),
                pltpu.VMEM((4, PAD, 4 * FEAT), BF16),
                pltpu.VMEM((HALF, FEAT), F32),
                pltpu.VMEM((3, HALF, FEAT), F32),
                pltpu.VMEM((HALF, 4 * FEAT), BF16),
                pltpu.VMEM((2, HALF, PAD), F32),
                pltpu.VMEM((HALF, PAD), F32),
                pltpu.VMEM((2, HALF, PAD), F32),
                pltpu.VMEM((3, 1, FEAT), F32),
                pltpu.VMEM((8, 32, 128), F32),
                pltpu.VMEM((HALF, 128), F32),
                pltpu.VMEM((2, 32, 128), F32),
                pltpu.VMEM((8, 32, 128), F32),
                pltpu.VMEM((4, 32, 128), F32),
                pltpu.VMEM((4, 32, 128), F32),
                dma((13,)),
                dma, dma((8,)),
                dma, dma((3,)),
                dma, dma((4,)),
                dma, dma((5,)),
                dma, dma((5,)),
                dma, dma((4,)),
                dma((2,)), dma((4,)), dma((4, 32)),
                dma((2,)), dma((2, 16)),
                dma, dma((8,)),
                dma((3,)), dma((8,)), dma((4,)), dma((4,)),
            ],
            compiler_params=pltpu.CompilerParams(
                collective_id=0, has_side_effects=True, vmem_limit_bytes=59 * 1048576),
        )(hidden, norm_gain.reshape(1, FEAT), w_head.T)
        log_norm = log_norm.reshape(SEQ)
        return logits[:, :WORDS] - log_norm[:, None], log_norm

    return jax.shard_map(
        local_head,
        mesh=mesh,
        in_specs=(P("dp", "row"), P("row"), P("row", "col")),
        out_specs=(P("dp", ("col", "row")), P("dp")),
        check_vma=False,
    )
```

```python
import functools

import jax
import jax.numpy as jnp
from jax import lax
from jax.experimental import pallas as pl
from jax.experimental.pallas import tpu as pltpu
from jax.sharding import PartitionSpec as P

EPS = 1e-5
MESH = pl.DeviceIdType.MESH
F32 = jnp.float32
BF16 = jnp.bfloat16
LOW = -3.0e38

SEQ, FEAT, WORDS, PAD = 4096, 512, 250, 256
HALF = SEQ // 2
BLOCK, PIECE, WAVE, GROUP = 128, 32, 16, 64


def kernel(h_hbm, g_ref, w_hbm, z_ref, lse_ref,
           h, hp16, hp, w, wst, wl, wbf, xst, xl, xbf, zs, zp, zr, gl, ssq, rcol, st, st1, st2, st3,
           in_sem, ssq_send, ssq_recv, g_send, g_recv, wp_send, wp_recv, wb_send, wb_recv, wr_send, wr_recv,
           xp_send, xp_recv, xb_send, xf_send, x_recv, z_send, z_recv, zq_recv, zp_send, zp_recv,
           st_send, st1_recv, st2_recv, st3_recv):
    col, row = lax.axis_index("col"), lax.axis_index("row")
    z, y = lax.div(col, 4), lax.rem(col, 4)
    x, c = lax.div(row, 2), lax.rem(row, 2)
    mate = 1 - c
    near = x + 1 - 2 * lax.rem(x, 2)
    far = 3 - x

    def at_row(r):
        return (0, col, r)

    def at_col(yy, zz):
        return (0, zz * 4 + yy, row)

    partner = at_row(x * 2 + mate)
    near_same = at_row(near * 2 + c)
    near_other = at_row(near * 2 + mate)

    def remote(src, dst, send, recv, dev):
        return pltpu.make_async_remote_copy(
            src_ref=src, dst_ref=dst, send_sem=send, recv_sem=recv, device_id=dev, device_id_type=MESH)

    def drain_send(ref, sem):
        remote(ref, ref, sem, sem, partner).wait_send()

    def drain_recv(ref, sem):
        remote(ref, ref, sem, sem, partner).wait_recv()

    firsts, seconds = (y, y, z, z), (z, z, y, y)
    signs = (1, -1, 1, -1)

    def first(f, i):
        return lax.rem(firsts[f] - signs[f] * i + 4, 4)

    def second(f, j):
        return lax.rem(seconds[f] - signs[f] * j + 4, 4)

    def piece_base(f, i, j):
        return f * 512 + first(f, i) * BLOCK + second(f, j) * PIECE

    def piece_rows(f, i, j, offset=0):
        return pl.ds(pl.multiple_of(offset + piece_base(f, i, j), PIECE), PIECE)

    def wave_rows(f, t, offset=0):
        v, i, j = t
        return pl.ds(pl.multiple_of(offset + v * WAVE + piece_base(f, i, j), WAVE), WAVE)

    own_pieces = [(f, core) for f in range(4) for core in range(2)]

    def load_piece(f, core):
        return pltpu.make_async_copy(
            h_hbm.at[piece_rows(f, 0, 0, core * HALF), :], hp16.at[f * 2 + core], in_sem.at[5 + f * 2 + core])

    def load_h(k):
        rows = pl.ds(k * 1024, 1024)
        return pltpu.make_async_copy(h_hbm.at[rows, :], h.at[rows, :], in_sem.at[k])

    for f, core in own_pieces:
        load_piece(f, core).start()
    w_in = pltpu.make_async_copy(w_hbm, w, in_sem.at[4])
    w_in.start()
    for k in range(4):
        load_h(k).start()

    barrier = pltpu.get_barrier_semaphore()
    peers = [at_row(lax.rem(row + d, 8)) for d in range(1, 8)]
    peers += [at_col(lax.rem(y + d, 4), z) for d in range(1, 4)]
    peers += [at_col(y, lax.rem(z + d, 4)) for d in range(1, 4)]
    for dev in peers:
        pl.semaphore_signal(barrier, inc=1, device_id=dev, device_id_type=MESH)

    for f, core in own_pieces:
        load_piece(f, core).wait()
        hp[f * 2 + core] = hp16[f * 2 + core].astype(F32)
    with jax.named_scope("bar"):
        pl.semaphore_wait(barrier, len(peers))

    def send_pieces(v):
        for f, core in own_pieces:
            slot = 1 + (core + c) - 2 * core * c
            remote(hp.at[f * 2 + core, pl.ds(v * WAVE, WAVE), :], xl.at[slot, wave_rows(f, (v, 0, 0)), :],
                   xb_send.at[v], x_recv.at[f, v * 16], at_row(near * 2 + core)).start()

    send_pieces(0)
    for slot, dev in enumerate((partner, near_same, near_other)):
        remote(g_ref, gl.at[slot], g_send, g_recv.at[slot], dev).start()

    w_in.wait()

    def prep(b, rows):
        start = rows // 16 * 16
        for q in range(4):
            lanes = slice(q * 128, (q + 1) * 128)
            wide = w[start:min(start + 272, 8 * WORDS), lanes].astype(F32)
            part = wide[rows - start:rows - start + WORDS, :]
            wst[b, :, lanes] = jnp.concatenate([part, jnp.zeros((PAD - WORDS, 128), F32)], axis=0)

    with jax.named_scope("prep"):
        for b in range(8):
            prep(b, b * WORDS)

    def kind_block(chip, n):
        return ((3 - chip) * 2 + n) if n < 2 else (chip * 2 + n - 2)

    parts = ((0, 0, 128), (0, 128, 128), (1, 0, PAD), (2, 0, PAD), (3, 0, PAD))

    def send_near(p):
        n, w0, size = parts[p]
        rows = pl.ds(w0, size)
        remote(wst.at[kind_block(near, n), rows, :], wl.at[1, n, rows, :], wb_send, wb_recv.at[p], near_same).start()

    for n in range(4):
        remote(wst.at[kind_block(x, n)], wl.at[0, n], wp_send, wp_recv.at[n], partner).start()

    for k in range(4):
        load_h(k).wait()

        def squares(t, _, k=k):
            b = k * 8 + t
            hb = h[pl.ds(pl.multiple_of(b * BLOCK, BLOCK), BLOCK), :].astype(F32)
            sq = hb * hb
            part = (sq[:, 0:128] + sq[:, 128:256]) + (sq[:, 256:384] + sq[:, 384:512])
            ssq[row, pl.ds(b, 1), :] = jnp.sum(part.T, axis=0, keepdims=True)
            return 0

        with jax.named_scope("squares"):
            lax.fori_loop(0, 8, squares, 0)
    for d in range(1, 8):
        remote(ssq.at[row], ssq.at[row], ssq_send, ssq_recv.at[row], at_row(lax.rem(row + d, 8))).start()

    for f in range(4):
        rows = pl.ds(f * 512, 512)
        xst[rows, :] = h[pl.ds(pl.multiple_of(mate * HALF + f * 512, 512), 512), :].astype(F32)
        remote(xst.at[rows, :], xl.at[0, rows, :], xp_send, xp_recv.at[f], partner).start()

    def relay_weights(p):
        n, w0, size = parts[p]
        rows = pl.ds(w0, size)
        with jax.named_scope("wrelay"):
            drain_recv(wl.at[1, n, rows, :], wb_recv.at[p])
        remote(wl.at[1, n, rows, :], wl.at[2, n, rows, :], wr_send, wr_recv.at[p], partner).start()

    def take_weights(p):
        n, w0, size = parts[p]
        rows = pl.ds(w0, size)
        with jax.named_scope("wtake"):
            if w0 == 0:
                drain_recv(wl.at[0, n], wp_recv.at[n])
            drain_recv(wl.at[2, n, rows, :], wr_recv.at[p])
        wbf[n, rows, 0:512] = wst[kind_block(x, n), rows, :].astype(BF16)
        for k in range(3):
            wbf[n, rows, (k + 1) * 512:(k + 2) * 512] = wl[k, n, rows, :].astype(BF16)

    ups = (at_col(lax.rem(y + 1, 4), z), at_col(lax.rem(y + 3, 4), z),
           at_col(y, lax.rem(z + 1, 4)), at_col(y, lax.rem(z + 3, 4)))
    along_first = (ups[0], ups[1], ups[2], ups[3])
    along_second = (ups[2], ups[3], ups[0], ups[1])

    def step_of(n):
        i = 3 - lax.rem(n, 4)
        reach = lax.div(n, 4) - i
        return reach, (lax.div(reach, 4), i, lax.rem(reach, 4))

    def each(lo, hi, body):
        def at(n, _):
            reach, t = step_of(n)

            @pl.when((reach >= 0) & (reach < 8))
            def _():
                body(t)
            return 0

        lax.fori_loop(lo, hi, at, 0)

    def serve(t, flows=(0, 1, 2, 3)):
        v, i, j = t
        with jax.named_scope("serve"):
            for f in flows:
                ref = xl.at[pl.ds(1, 2), wave_rows(f, t), :]
                step = v * 16 + i * 4 + j
                drain_recv(ref, x_recv.at[f, step])

                @pl.when((j == 0) & (i < 3))
                def _():
                    remote(ref, ref, xf_send.at[f], x_recv.at[f, step + 4], along_first[f]).start()

                @pl.when(j < 3)
                def _():
                    remote(ref, ref, xf_send.at[f], x_recv.at[f, step + 1], along_second[f]).start()

    def scales():
        with jax.named_scope("wssq"):
            for d in range(1, 8):
                r = lax.rem(row + d, 8)
                drain_recv(ssq.at[r], ssq_recv.at[r])
            for slot in range(3):
                drain_recv(gl.at[slot], g_recv.at[slot])
        mine = pl.ds(pl.multiple_of(c * 16, 16), 16)
        total = ssq[0, mine, :]
        for r in range(1, 8):
            total = total + ssq[r, mine, :]
        inv = lax.rsqrt(total / (FEAT * 8) + EPS)
        for b in range(16):
            rcol[b * BLOCK:(b + 1) * BLOCK, :] = jnp.broadcast_to(inv[b:b + 1, :], (BLOCK, BLOCK)).T

    def normalise(f, t):
        rows = wave_rows(f, t)
        scale = rcol[rows, :]
        for k in range(4):
            for q in range(4):
                lanes = slice(q * 128, (q + 1) * 128)
                if k == 0:
                    raw, gain = h[wave_rows(f, t, c * HALF), lanes].astype(F32), g_ref[:, lanes]
                else:
                    raw, gain = xl[k - 1, rows, lanes], gl[k - 1, :, lanes]
                xbf[rows, k * 512 + q * 128:k * 512 + (q + 1) * 128] = (raw * scale * gain).astype(BF16)

    def share(left, n, rows=slice(0, PAD)):
        return lax.dot_general(left, wbf[n, rows, :], (((1,), (1,)), ((), ())), preferred_element_type=F32)

    def far_group(t, words):
        with jax.named_scope("group"):
            left = jnp.concatenate([xbf[wave_rows(f, t), :] for f in range(4)], axis=0)
            value = share(left, 0, words)
            lanes = pl.ds(words.start, words.stop - words.start)
            rows = pl.ds(pl.multiple_of(((t[0] * 4 + t[1]) * 4 + t[2]) * GROUP, GROUP), GROUP)
            zs[0, rows, words] = value
            remote(zs.at[0, rows, lanes], zr.at[c, rows, lanes], z_send.at[0], zq_recv.at[c, t[1]],
                   at_row(far * 2)).start()

    def normalise_group(t):
        with jax.named_scope("norm"):
            for f in range(4):
                normalise(f, t)

    low, high, full = slice(0, 128), slice(128, PAD), slice(0, PAD)
    origin = tuple(jnp.int32(0) for _ in range(3))
    serve(origin, (0, 1))
    drain_send(xl.at[0, pl.ds(0, 128), :], xb_send.at[0])
    send_near(0)
    send_near(1)
    serve(origin, (2, 3))
    each(4, 8, serve)
    scales()
    for f in range(4):
        drain_recv(xl.at[0, pl.ds(f * 512, 512), :], xp_recv.at[f])
    relay_weights(0)
    each(0, 8, normalise_group)
    each(8, 10, serve)
    take_weights(0)
    each(0, 8, lambda t: far_group(t, low))

    def low_step(t):
        normalise_group(t)
        far_group(t, low)

    each(8, 10, low_step)
    each(10, 12, lambda t: (serve(t), low_step(t)))
    relay_weights(1)
    send_pieces(1)
    for p in (2, 3, 4):
        send_near(p)
    each(12, 13, serve)
    take_weights(1)
    each(0, 12, lambda t: far_group(t, high))

    def full_step(t):
        normalise_group(t)
        far_group(t, full)

    each(12, 13, full_step)

    def ring_step(t):
        serve(t)
        full_step(t)

    each(13, 26, ring_step)
    relay_weights(2)
    each(26, 38, ring_step)
    relay_weights(3)
    each(38, 44, ring_step)
    take_weights(2)

    def block_rows(blk):
        return pl.ds(pl.multiple_of(blk * BLOCK, BLOCK), BLOCK)

    def step_far(blk, _):
        with jax.named_scope("far"):
            rows = block_rows(blk)
            zs[1, rows, :] = share(xbf[rows, :], 1)
            remote(zs.at[1, rows, :], zr.at[c, rows, :], z_send.at[1], z_recv.at[c, blk], at_row(far * 2 + 1)).start()
        return 0

    lax.fori_loop(0, 8, step_far, 0)
    relay_weights(4)
    lax.fori_loop(8, 16, step_far, 0)
    take_weights(3)
    take_weights(4)

    def pair_rows(pair):
        return pl.ds(pl.multiple_of(pair * 256, 256), 256)

    def step_own(pair, _):
        with jax.named_scope("own"):
            rows = pair_rows(pair)
            xl[0, rows, 256:512] = share(xbf[rows, :], 2 + mate)
            remote(xl.at[0, rows, pl.ds(256, 256)], zp.at[rows, :], zp_send, zp_recv.at[pair], partner).start()
            xl[0, rows, 0:256] = share(xbf[rows, :], 2 + c)
        return 0

    lax.fori_loop(0, 8, step_own, 0)

    for pair in range(8):
        drain_recv(zp.at[pair_rows(pair), :], zp_recv.at[pair])

    def arrived(half, n, i, f, c2, s):
        pieces = []
        for b in range(4):
            for v in range(2):
                group = (v * 4 + i) * 4 + lax.rem(s * (c2 - b) + 4, 4)
                start = c * (n * BLOCK + b * PIECE + v * WAVE) + mate * (group * GROUP + f * WAVE)
                pieces.append(zr[half, pl.ds(pl.multiple_of(start, WAVE), WAVE), :])
        return jnp.concatenate(pieces, axis=0)

    def finish(half, blk, value):
        z_ref[pl.ds(pl.multiple_of(half * HALF + blk * BLOCK, BLOCK), BLOCK), :] = value
        lane = lax.broadcasted_iota(jnp.int32, (BLOCK, 128), 1)
        left, right = value[:, 0:128], jnp.where(lane < WORDS - 128, value[:, 128:256], LOW)
        top = jnp.max(jnp.maximum(left, right).T, axis=0, keepdims=True)
        shift = jnp.broadcast_to(top, (BLOCK, BLOCK)).T
        mass = jnp.exp(left - shift) + jnp.exp(right - shift)
        st[0, pl.ds(half * 16 + blk, 1), :] = top
        st[1, pl.ds(half * 16 + blk, 1), :] = jnp.sum(mass.T, axis=0, keepdims=True)

    def step_out(n, _):
        i, f = lax.div(n, 4), lax.rem(n, 4)
        q, s = lax.div(f, 2), 1 - 2 * lax.rem(f, 2)
        c1, c2 = y * (1 - q) + z * q, z * (1 - q) + y * q
        blk = c * n + mate * (f * 4 + lax.rem(c1 - s * i + 4, 4))
        with jax.named_scope("wz"):
            @pl.when((c == 0) & (f == 0))
            def _():
                for half in range(2):
                    drain_recv(zr.at[half, pl.ds(0, 512), :], zq_recv.at[half, i])

            @pl.when(c == 1)
            def _():
                for half in range(2):
                    drain_recv(zr.at[half, block_rows(n), :], z_recv.at[half, n])
        rows = block_rows(blk)
        finish(c, blk, arrived(c, n, i, f, c2, s) + xl[0, rows, 0:256])
        finish(mate, blk, arrived(mate, n, i, f, c2, s) + zp[rows, :])
        return 0

    with jax.named_scope("finish"):
        lax.fori_loop(0, 16, step_out, 0)

    def exchange(buf, me, count, send, recv, dev):
        with jax.named_scope("exch"):
            for d in range(1, count):
                remote(buf.at[me], buf.at[me], send, recv.at[me], dev(lax.rem(me + d, count))).start()
            for d in range(1, count):
                other = lax.rem(me + d, count)
                drain_recv(buf.at[other], recv.at[other])
        top = buf[0]
        for k in range(1, count):
            top = jnp.maximum(top, buf[k])
        mass = jnp.exp(buf[0] - top)
        for k in range(1, count):
            mass = mass + jnp.exp(buf[k] - top)
        return top + jnp.log(mass)

    st1[row] = st[0] + jnp.log(st[1])
    st2[z] = exchange(st1, row, 8, st_send.at[0], st1_recv, at_row)
    st3[y] = exchange(st2, z, 4, st_send.at[1], st2_recv, lambda k: at_col(y, k))
    lse_ref[...] = exchange(st3, y, 4, st_send.at[2], st3_recv, lambda k: at_col(k, z))

    drain_send(ssq.at[pl.ds(0, 7)], ssq_send)
    drain_send(gl, g_send)
    drain_send(wl.at[0], wp_send)
    drain_send(wl.at[0], wb_send)
    drain_send(wl.at[0], wr_send)
    drain_send(xl.at[0], xp_send)
    drain_send(xl.at[0, pl.ds(0, 128), :], xb_send.at[1])
    for f in range(4):
        drain_send(xl.at[pl.ds(1, 2), pl.ds(0, 15 * PIECE), :], xf_send.at[f])
    for n in range(2):
        drain_send(zs.at[n], z_send.at[n])
    drain_send(zp, zp_send)
    drain_send(st1.at[pl.ds(0, 7)], st_send.at[0])
    drain_send(st2.at[pl.ds(0, 3)], st_send.at[1])
    drain_send(st3.at[pl.ds(0, 3)], st_send.at[2])


def solution(mesh):
    dma = pltpu.SemaphoreType.DMA

    def local_head(hidden, norm_gain, w_head):
        logits, log_norm = pl.pallas_call(
            kernel,
            out_shape=(pltpu.VMEM((SEQ, PAD), F32), pltpu.VMEM((32, 128), F32)),
            in_specs=[pl.BlockSpec(memory_space=pl.ANY), pl.BlockSpec(memory_space=pltpu.VMEM),
                      pl.BlockSpec(memory_space=pl.ANY)],
            out_specs=(pl.BlockSpec(memory_space=pltpu.VMEM), pl.BlockSpec(memory_space=pltpu.VMEM)),
            scratch_shapes=[
                pltpu.VMEM((SEQ, FEAT), BF16),
                pltpu.VMEM((8, PIECE, FEAT), BF16),
                pltpu.VMEM((8, PIECE, FEAT), F32),
                pltpu.VMEM((8 * WORDS, FEAT), BF16),
                pltpu.VMEM((8, PAD, FEAT), F32),
                pltpu.VMEM((3, 4, PAD, FEAT), F32),
                pltpu.VMEM((4, PAD, 4 * FEAT), BF16),
                pltpu.VMEM((HALF, FEAT), F32),
                pltpu.VMEM((3, HALF, FEAT), F32),
                pltpu.VMEM((HALF, 4 * FEAT), BF16),
                pltpu.VMEM((2, HALF, PAD), F32),
                pltpu.VMEM((HALF, PAD), F32),
                pltpu.VMEM((2, HALF, PAD), F32),
                pltpu.VMEM((3, 1, FEAT), F32),
                pltpu.VMEM((8, 32, 128), F32),
                pltpu.VMEM((HALF, 128), F32),
                pltpu.VMEM((2, 32, 128), F32),
                pltpu.VMEM((8, 32, 128), F32),
                pltpu.VMEM((4, 32, 128), F32),
                pltpu.VMEM((4, 32, 128), F32),
                dma((13,)),
                dma, dma((8,)),
                dma, dma((3,)),
                dma, dma((4,)),
                dma, dma((5,)),
                dma, dma((5,)),
                dma, dma((4,)),
                dma((2,)), dma((4,)), dma((4, 32)),
                dma((2,)), dma((2, 16)), dma((2, 4)),
                dma, dma((8,)),
                dma((3,)), dma((8,)), dma((4,)), dma((4,)),
            ],
            compiler_params=pltpu.CompilerParams(
                collective_id=0, has_side_effects=True, vmem_limit_bytes=59 * 1048576),
        )(hidden, norm_gain.reshape(1, FEAT), w_head.T)
        log_norm = log_norm.reshape(SEQ)
        return logits[:, :WORDS] - log_norm[:, None], log_norm

    return jax.shard_map(
        local_head,
        mesh=mesh,
        in_specs=(P("dp", "row"), P("row"), P("row", "col")),
        out_specs=(P("dp", ("col", "row")), P("dp")),
        check_vma=False,
    )
```

```python
import functools

import jax
import jax.numpy as jnp
from jax import lax
from jax.experimental import pallas as pl
from jax.experimental.pallas import tpu as pltpu
from jax.sharding import PartitionSpec as P

EPS = 1e-5
MESH = pl.DeviceIdType.MESH
F32 = jnp.float32
BF16 = jnp.bfloat16
LOW = -3.0e38

SEQ, FEAT, WORDS, PAD = 4096, 512, 250, 256
HALF = SEQ // 2
BLOCK, PIECE, WAVE, GROUP = 128, 32, 16, 64


def kernel(h_hbm, g_ref, w_hbm, z_ref, lse_ref,
           h, hp16, hp, w, wst, wl, wbf, xst, xl, xbf, zs, zp, zr, gl, ssq, rcol, st, st1, st2, st3,
           in_sem, ssq_send, ssq_recv, g_send, g_recv, wp_send, wp_recv, wb_send, wb_recv, wr_send, wr_recv,
           xp_send, xp_recv, xb_send, xf_send, x_recv, z_send, z_recv, zq_recv, zp_send, zp_recv,
           st_send, st1_recv, st2_recv, st3_recv):
    col, row = lax.axis_index("col"), lax.axis_index("row")
    z, y = lax.div(col, 4), lax.rem(col, 4)
    x, c = lax.div(row, 2), lax.rem(row, 2)
    mate = 1 - c
    near = x + 1 - 2 * lax.rem(x, 2)
    far = 3 - x

    def at_row(r):
        return (0, col, r)

    def at_col(yy, zz):
        return (0, zz * 4 + yy, row)

    partner = at_row(x * 2 + mate)
    near_same = at_row(near * 2 + c)
    near_other = at_row(near * 2 + mate)

    def remote(src, dst, send, recv, dev):
        return pltpu.make_async_remote_copy(
            src_ref=src, dst_ref=dst, send_sem=send, recv_sem=recv, device_id=dev, device_id_type=MESH)

    def drain_send(ref, sem):
        remote(ref, ref, sem, sem, partner).wait_send()

    def drain_recv(ref, sem):
        remote(ref, ref, sem, sem, partner).wait_recv()

    firsts, seconds = (y, y, z, z), (z, z, y, y)
    signs = (1, -1, 1, -1)

    def first(f, i):
        return lax.rem(firsts[f] - signs[f] * i + 4, 4)

    def second(f, j):
        return lax.rem(seconds[f] - signs[f] * j + 4, 4)

    def piece_base(f, i, j):
        return f * 512 + first(f, i) * BLOCK + second(f, j) * PIECE

    def piece_rows(f, i, j, offset=0):
        return pl.ds(pl.multiple_of(offset + piece_base(f, i, j), PIECE), PIECE)

    def wave_rows(f, t, offset=0):
        v, i, j = t
        return pl.ds(pl.multiple_of(offset + v * WAVE + piece_base(f, i, j), WAVE), WAVE)

    own_pieces = [(f, core) for f in range(4) for core in range(2)]

    def load_piece(f, core):
        return pltpu.make_async_copy(
            h_hbm.at[piece_rows(f, 0, 0, core * HALF), :], hp16.at[f * 2 + core], in_sem.at[5 + f * 2 + core])

    def load_h(k):
        rows = pl.ds(k * 1024, 1024)
        return pltpu.make_async_copy(h_hbm.at[rows, :], h.at[rows, :], in_sem.at[k])

    for f, core in own_pieces:
        load_piece(f, core).start()
    w_in = pltpu.make_async_copy(w_hbm, w, in_sem.at[4])
    w_in.start()
    for k in range(4):
        load_h(k).start()

    barrier = pltpu.get_barrier_semaphore()
    peers = [at_row(lax.rem(row + d, 8)) for d in range(1, 8)]
    peers += [at_col(lax.rem(y + d, 4), z) for d in range(1, 4)]
    peers += [at_col(y, lax.rem(z + d, 4)) for d in range(1, 4)]
    for dev in peers:
        pl.semaphore_signal(barrier, inc=1, device_id=dev, device_id_type=MESH)

    for f, core in own_pieces:
        load_piece(f, core).wait()
        hp[f * 2 + core] = hp16[f * 2 + core].astype(F32)
    with jax.named_scope("bar"):
        pl.semaphore_wait(barrier, len(peers))

    def send_pieces(v):
        for f, core in own_pieces:
            slot = 1 + (core + c) - 2 * core * c
            remote(hp.at[f * 2 + core, pl.ds(v * WAVE, WAVE), :], xl.at[slot, wave_rows(f, (v, 0, 0)), :],
                   xb_send.at[v], x_recv.at[f, v * 16], at_row(near * 2 + core)).start()

    send_pieces(0)
    for slot, dev in enumerate((partner, near_same, near_other)):
        remote(g_ref, gl.at[slot], g_send, g_recv.at[slot], dev).start()

    w_in.wait()

    def prep(b, rows):
        start = rows // 16 * 16
        for q in range(4):
            lanes = slice(q * 128, (q + 1) * 128)
            wide = w[start:min(start + 272, 8 * WORDS), lanes].astype(F32)
            part = wide[rows - start:rows - start + WORDS, :]
            wst[b, :, lanes] = jnp.concatenate([part, jnp.zeros((PAD - WORDS, 128), F32)], axis=0)

    with jax.named_scope("prep"):
        for b in range(8):
            prep(b, b * WORDS)

    def kind_block(chip, n):
        return ((3 - chip) * 2 + n) if n < 2 else (chip * 2 + n - 2)

    parts = ((0, 0, 128), (0, 128, 128), (1, 0, PAD), (2, 0, PAD), (3, 0, PAD))

    def send_near(p):
        n, w0, size = parts[p]
        rows = pl.ds(w0, size)
        remote(wst.at[kind_block(near, n), rows, :], wl.at[1, n, rows, :], wb_send, wb_recv.at[p], near_same).start()

    for n in range(4):
        remote(wst.at[kind_block(x, n)], wl.at[0, n], wp_send, wp_recv.at[n], partner).start()

    for k in range(4):
        load_h(k).wait()

        def squares(t, _, k=k):
            b = k * 8 + t
            hb = h[pl.ds(pl.multiple_of(b * BLOCK, BLOCK), BLOCK), :].astype(F32)
            sq = hb * hb
            part = (sq[:, 0:128] + sq[:, 128:256]) + (sq[:, 256:384] + sq[:, 384:512])
            ssq[row, pl.ds(b, 1), :] = jnp.sum(part.T, axis=0, keepdims=True)
            return 0

        with jax.named_scope("squares"):
            lax.fori_loop(0, 8, squares, 0)
    for d in range(1, 8):
        peer = lax.rem(row + d, 8)
        theirs = ssq.at[row, pl.ds(pl.multiple_of(lax.rem(peer, 2) * 16, 16), 16), :]
        remote(theirs, theirs, ssq_send, ssq_recv.at[row], at_row(peer)).start()

    for f in range(4):
        rows = pl.ds(f * 512, 512)
        xst[rows, :] = h[pl.ds(pl.multiple_of(mate * HALF + f * 512, 512), 512), :].astype(F32)
        remote(xst.at[rows, :], xl.at[0, rows, :], xp_send, xp_recv.at[f], partner).start()

    def relay_weights(p):
        n, w0, size = parts[p]
        rows = pl.ds(w0, size)
        with jax.named_scope("wrelay"):
            drain_recv(wl.at[1, n, rows, :], wb_recv.at[p])
        remote(wl.at[1, n, rows, :], wl.at[2, n, rows, :], wr_send, wr_recv.at[p], partner).start()

    def take_weights(p):
        n, w0, size = parts[p]
        rows = pl.ds(w0, size)
        with jax.named_scope("wtake"):
            if w0 == 0:
                drain_recv(wl.at[0, n], wp_recv.at[n])
            drain_recv(wl.at[2, n, rows, :], wr_recv.at[p])
        wbf[n, rows, 0:512] = wst[kind_block(x, n), rows, :].astype(BF16)
        for k in range(3):
            wbf[n, rows, (k + 1) * 512:(k + 2) * 512] = wl[k, n, rows, :].astype(BF16)

    ups = (at_col(lax.rem(y + 1, 4), z), at_col(lax.rem(y + 3, 4), z),
           at_col(y, lax.rem(z + 1, 4)), at_col(y, lax.rem(z + 3, 4)))
    along_first = (ups[0], ups[1], ups[2], ups[3])
    along_second = (ups[2], ups[3], ups[0], ups[1])

    def step_of(n):
        i = 3 - lax.rem(n, 4)
        reach = lax.div(n, 4) - i
        return reach, (lax.div(reach, 4), i, lax.rem(reach, 4))

    def each(lo, hi, body):
        def at(n, _):
            reach, t = step_of(n)

            @pl.when((reach >= 0) & (reach < 8))
            def _():
                body(t)
            return 0

        lax.fori_loop(lo, hi, at, 0)

    def serve(t, flows=(0, 1, 2, 3)):
        v, i, j = t
        with jax.named_scope("serve"):
            for f in flows:
                ref = xl.at[pl.ds(1, 2), wave_rows(f, t), :]
                step = v * 16 + i * 4 + j
                drain_recv(ref, x_recv.at[f, step])

                @pl.when((j == 0) & (i < 3))
                def _():
                    remote(ref, ref, xf_send.at[f], x_recv.at[f, step + 4], along_first[f]).start()

                @pl.when(j < 3)
                def _():
                    remote(ref, ref, xf_send.at[f], x_recv.at[f, step + 1], along_second[f]).start()

    def scales():
        with jax.named_scope("wssq"):
            for d in range(1, 8):
                r = lax.rem(row + d, 8)
                drain_recv(ssq.at[r, pl.ds(0, 16), :], ssq_recv.at[r])
            for slot in range(3):
                drain_recv(gl.at[slot], g_recv.at[slot])
        mine = pl.ds(pl.multiple_of(c * 16, 16), 16)
        total = ssq[0, mine, :]
        for r in range(1, 8):
            total = total + ssq[r, mine, :]
        inv = lax.rsqrt(total / (FEAT * 8) + EPS)
        for b in range(16):
            rcol[b * BLOCK:(b + 1) * BLOCK, :] = jnp.broadcast_to(inv[b:b + 1, :], (BLOCK, BLOCK)).T

    def normalise(f, t):
        rows = wave_rows(f, t)
        scale = rcol[rows, :]
        for k in range(4):
            for q in range(4):
                lanes = slice(q * 128, (q + 1) * 128)
                if k == 0:
                    raw, gain = h[wave_rows(f, t, c * HALF), lanes].astype(F32), g_ref[:, lanes]
                else:
                    raw, gain = xl[k - 1, rows, lanes], gl[k - 1, :, lanes]
                xbf[rows, k * 512 + q * 128:k * 512 + (q + 1) * 128] = (raw * scale * gain).astype(BF16)

    def share(left, n, rows=slice(0, PAD)):
        return lax.dot_general(left, wbf[n, rows, :], (((1,), (1,)), ((), ())), preferred_element_type=F32)

    def far_group(t, words):
        with jax.named_scope("group"):
            left = jnp.concatenate([xbf[wave_rows(f, t), :] for f in range(4)], axis=0)
            value = share(left, 0, words)
            lanes = pl.ds(words.start, words.stop - words.start)
            rows = pl.ds(pl.multiple_of(((t[0] * 4 + t[1]) * 4 + t[2]) * GROUP, GROUP), GROUP)
            zs[0, rows, words] = value
            remote(zs.at[0, rows, lanes], zr.at[c, rows, lanes], z_send.at[0], zq_recv.at[c, t[1]],
                   at_row(far * 2)).start()

    def normalise_group(t):
        with jax.named_scope("norm"):
            for f in range(4):
                normalise(f, t)

    low, high, full = slice(0, 128), slice(128, PAD), slice(0, PAD)
    origin = tuple(jnp.int32(0) for _ in range(3))
    drain_send(xl.at[0, pl.ds(0, 128), :], xb_send.at[0])
    send_near(0)
    send_near(1)
    serve(origin)
    each(4, 8, serve)
    scales()
    for f in range(4):
        drain_recv(xl.at[0, pl.ds(f * 512, 512), :], xp_recv.at[f])
    relay_weights(0)
    each(0, 8, normalise_group)
    each(8, 10, serve)
    take_weights(0)
    each(0, 8, lambda t: far_group(t, low))

    def low_step(t):
        normalise_group(t)
        far_group(t, low)

    each(8, 10, low_step)
    each(10, 12, lambda t: (serve(t), low_step(t)))
    relay_weights(1)
    send_pieces(1)
    for p in (2, 3, 4):
        send_near(p)
    each(12, 13, serve)
    take_weights(1)
    each(0, 12, lambda t: far_group(t, high))

    def full_step(t):
        normalise_group(t)
        far_group(t, full)

    each(12, 13, full_step)

    def ring_step(t):
        serve(t)
        full_step(t)

    each(13, 26, ring_step)
    relay_weights(2)
    each(26, 38, ring_step)
    relay_weights(3)
    each(38, 44, ring_step)
    take_weights(2)

    def block_rows(blk):
        return pl.ds(pl.multiple_of(blk * BLOCK, BLOCK), BLOCK)

    def step_far(blk, _):
        with jax.named_scope("far"):
            rows = block_rows(blk)
            zs[1, rows, :] = share(xbf[rows, :], 1)
            remote(zs.at[1, rows, :], zr.at[c, rows, :], z_send.at[1], z_recv.at[c, blk], at_row(far * 2 + 1)).start()
        return 0

    lax.fori_loop(0, 8, step_far, 0)
    relay_weights(4)
    lax.fori_loop(8, 16, step_far, 0)
    take_weights(3)
    take_weights(4)

    def pair_rows(pair):
        return pl.ds(pl.multiple_of(pair * 256, 256), 256)

    def step_own(pair, _):
        with jax.named_scope("own"):
            rows = pair_rows(pair)
            xl[0, rows, 256:512] = share(xbf[rows, :], 2 + mate)
            remote(xl.at[0, rows, pl.ds(256, 256)], zp.at[rows, :], zp_send, zp_recv.at[pair], partner).start()
            xl[0, rows, 0:256] = share(xbf[rows, :], 2 + c)
        return 0

    lax.fori_loop(0, 8, step_own, 0)

    for pair in range(8):
        drain_recv(zp.at[pair_rows(pair), :], zp_recv.at[pair])

    def arrived(half, n, i, f, c2, s):
        pieces = []
        for b in range(4):
            for v in range(2):
                group = (v * 4 + i) * 4 + lax.rem(s * (c2 - b) + 4, 4)
                start = c * (n * BLOCK + b * PIECE + v * WAVE) + mate * (group * GROUP + f * WAVE)
                pieces.append(zr[half, pl.ds(pl.multiple_of(start, WAVE), WAVE), :])
        return jnp.concatenate(pieces, axis=0)

    def finish(half, blk, value):
        z_ref[pl.ds(pl.multiple_of(half * HALF + blk * BLOCK, BLOCK), BLOCK), :] = value
        lane = lax.broadcasted_iota(jnp.int32, (BLOCK, 128), 1)
        left, right = value[:, 0:128], jnp.where(lane < WORDS - 128, value[:, 128:256], LOW)
        top = jnp.max(jnp.maximum(left, right).T, axis=0, keepdims=True)
        shift = jnp.broadcast_to(top, (BLOCK, BLOCK)).T
        mass = jnp.exp(left - shift) + jnp.exp(right - shift)
        st[0, pl.ds(half * 16 + blk, 1), :] = top
        st[1, pl.ds(half * 16 + blk, 1), :] = jnp.sum(mass.T, axis=0, keepdims=True)

    def step_out(n, _):
        i, f = lax.div(n, 4), lax.rem(n, 4)
        q, s = lax.div(f, 2), 1 - 2 * lax.rem(f, 2)
        c1, c2 = y * (1 - q) + z * q, z * (1 - q) + y * q
        blk = c * n + mate * (f * 4 + lax.rem(c1 - s * i + 4, 4))
        with jax.named_scope("wz"):
            @pl.when((c == 0) & (f == 0))
            def _():
                for half in range(2):
                    drain_recv(zr.at[half, pl.ds(0, 512), :], zq_recv.at[half, i])

            @pl.when(c == 1)
            def _():
                for half in range(2):
                    drain_recv(zr.at[half, block_rows(n), :], z_recv.at[half, n])
        rows = block_rows(blk)
        finish(c, blk, arrived(c, n, i, f, c2, s) + xl[0, rows, 0:256])
        finish(mate, blk, arrived(mate, n, i, f, c2, s) + zp[rows, :])
        return 0

    with jax.named_scope("finish"):
        lax.fori_loop(0, 16, step_out, 0)

    def exchange(buf, me, count, send, recv, dev):
        with jax.named_scope("exch"):
            for d in sorted(range(1, count), key=lambda d: abs(d - count // 2)):
                remote(buf.at[me], buf.at[me], send, recv.at[me], dev(lax.rem(me + d, count))).start()
            for d in range(1, count):
                other = lax.rem(me + d, count)
                drain_recv(buf.at[other], recv.at[other])
        top = buf[0]
        for k in range(1, count):
            top = jnp.maximum(top, buf[k])
        mass = jnp.exp(buf[0] - top)
        for k in range(1, count):
            mass = mass + jnp.exp(buf[k] - top)
        return top + jnp.log(mass)

    st1[row] = st[0] + jnp.log(st[1])
    st2[z] = exchange(st1, row, 8, st_send.at[0], st1_recv, at_row)
    st3[y] = exchange(st2, z, 4, st_send.at[1], st2_recv, lambda k: at_col(y, k))
    lse_ref[...] = exchange(st3, y, 4, st_send.at[2], st3_recv, lambda k: at_col(k, z))

    drain_send(ssq.at[pl.ds(0, 7), pl.ds(0, 16), :], ssq_send)
    drain_send(gl, g_send)
    drain_send(wl.at[0], wp_send)
    drain_send(wl.at[0], wb_send)
    drain_send(wl.at[0], wr_send)
    drain_send(xl.at[0], xp_send)
    drain_send(xl.at[0, pl.ds(0, 128), :], xb_send.at[1])
    for f in range(4):
        drain_send(xl.at[pl.ds(1, 2), pl.ds(0, 15 * PIECE), :], xf_send.at[f])
    for n in range(2):
        drain_send(zs.at[n], z_send.at[n])
    drain_send(zp, zp_send)
    drain_send(st1.at[pl.ds(0, 7)], st_send.at[0])
    drain_send(st2.at[pl.ds(0, 3)], st_send.at[1])
    drain_send(st3.at[pl.ds(0, 3)], st_send.at[2])


def solution(mesh):
    dma = pltpu.SemaphoreType.DMA

    def local_head(hidden, norm_gain, w_head):
        logits, log_norm = pl.pallas_call(
            kernel,
            out_shape=(pltpu.VMEM((SEQ, PAD), F32), pltpu.VMEM((32, 128), F32)),
            in_specs=[pl.BlockSpec(memory_space=pl.ANY), pl.BlockSpec(memory_space=pltpu.VMEM),
                      pl.BlockSpec(memory_space=pl.ANY)],
            out_specs=(pl.BlockSpec(memory_space=pltpu.VMEM), pl.BlockSpec(memory_space=pltpu.VMEM)),
            scratch_shapes=[
                pltpu.VMEM((SEQ, FEAT), BF16),
                pltpu.VMEM((8, PIECE, FEAT), BF16),
                pltpu.VMEM((8, PIECE, FEAT), F32),
                pltpu.VMEM((8 * WORDS, FEAT), BF16),
                pltpu.VMEM((8, PAD, FEAT), F32),
                pltpu.VMEM((3, 4, PAD, FEAT), F32),
                pltpu.VMEM((4, PAD, 4 * FEAT), BF16),
                pltpu.VMEM((HALF, FEAT), F32),
                pltpu.VMEM((3, HALF, FEAT), F32),
                pltpu.VMEM((HALF, 4 * FEAT), BF16),
                pltpu.VMEM((2, HALF, PAD), F32),
                pltpu.VMEM((HALF, PAD), F32),
                pltpu.VMEM((2, HALF, PAD), F32),
                pltpu.VMEM((3, 1, FEAT), F32),
                pltpu.VMEM((8, 32, 128), F32),
                pltpu.VMEM((HALF, 128), F32),
                pltpu.VMEM((2, 32, 128), F32),
                pltpu.VMEM((8, 32, 128), F32),
                pltpu.VMEM((4, 32, 128), F32),
                pltpu.VMEM((4, 32, 128), F32),
                dma((13,)),
                dma, dma((8,)),
                dma, dma((3,)),
                dma, dma((4,)),
                dma, dma((5,)),
                dma, dma((5,)),
                dma, dma((4,)),
                dma((2,)), dma((4,)), dma((4, 32)),
                dma((2,)), dma((2, 16)), dma((2, 4)),
                dma, dma((8,)),
                dma((3,)), dma((8,)), dma((4,)), dma((4,)),
            ],
            compiler_params=pltpu.CompilerParams(
                collective_id=0, has_side_effects=True, vmem_limit_bytes=59 * 1048576),
        )(hidden, norm_gain.reshape(1, FEAT), w_head.T)
        log_norm = log_norm.reshape(SEQ)
        return logits[:, :WORDS] - log_norm[:, None], log_norm

    return jax.shard_map(
        local_head,
        mesh=mesh,
        in_specs=(P("dp", "row"), P("row"), P("row", "col")),
        out_specs=(P("dp", ("col", "row")), P("dp")),
        check_vma=False,
    )
```

```python
import functools

import jax
import jax.numpy as jnp
from jax import lax
from jax.experimental import pallas as pl
from jax.experimental.pallas import tpu as pltpu
from jax.sharding import PartitionSpec as P

EPS = 1e-5
MESH = pl.DeviceIdType.MESH
F32 = jnp.float32
BF16 = jnp.bfloat16
LOW = -3.0e38

SEQ, FEAT, WORDS, PAD = 4096, 512, 250, 256
HALF = SEQ // 2
BLOCK, PIECE, WAVE, GROUP = 128, 32, 16, 64


def kernel(h_hbm, g_ref, w_hbm, z_ref, lse_ref,
           h, hp16, hp, w, wst, wl, wbf, xst, xl, xbf, zs, zp, zr, gl, ssq, rcol, st, st1, st2, st3,
           in_sem, ssq_send, ssq_recv, g_send, g_recv, wp_send, wp_recv, wb_send, wb_recv, wr_send, wr_recv,
           xp_send, xp_recv, xb_send, xf_send, x_recv, z_send, z_recv, zq_recv, zp_send, zp_recv,
           st_send, st1_recv, st2_recv, st3_recv):
    col, row = lax.axis_index("col"), lax.axis_index("row")
    z, y = lax.div(col, 4), lax.rem(col, 4)
    x, c = lax.div(row, 2), lax.rem(row, 2)
    mate = 1 - c
    near = x + 1 - 2 * lax.rem(x, 2)
    far = 3 - x

    def at_row(r):
        return (0, col, r)

    def at_col(yy, zz):
        return (0, zz * 4 + yy, row)

    partner = at_row(x * 2 + mate)
    near_same = at_row(near * 2 + c)
    near_other = at_row(near * 2 + mate)

    def remote(src, dst, send, recv, dev):
        return pltpu.make_async_remote_copy(
            src_ref=src, dst_ref=dst, send_sem=send, recv_sem=recv, device_id=dev, device_id_type=MESH)

    def drain_send(ref, sem):
        remote(ref, ref, sem, sem, partner).wait_send()

    def drain_recv(ref, sem):
        remote(ref, ref, sem, sem, partner).wait_recv()

    firsts, seconds = (y, y, z, z), (z, z, y, y)
    signs = (1, -1, 1, -1)

    def first(f, i):
        return lax.rem(firsts[f] - signs[f] * i + 4, 4)

    def second(f, j):
        return lax.rem(seconds[f] - signs[f] * j + 4, 4)

    def piece_base(f, i, j):
        return f * 512 + first(f, i) * BLOCK + second(f, j) * PIECE

    def piece_rows(f, i, j, offset=0):
        return pl.ds(pl.multiple_of(offset + piece_base(f, i, j), PIECE), PIECE)

    def wave_rows(f, t, offset=0):
        v, i, j = t
        return pl.ds(pl.multiple_of(offset + v * WAVE + piece_base(f, i, j), WAVE), WAVE)

    own_pieces = [(f, core) for f in range(4) for core in range(2)]

    def load_piece(f, core):
        return pltpu.make_async_copy(
            h_hbm.at[piece_rows(f, 0, 0, core * HALF), :], hp16.at[f * 2 + core], in_sem.at[5 + f * 2 + core])

    def load_h(k):
        rows = pl.ds(k * 1024, 1024)
        return pltpu.make_async_copy(h_hbm.at[rows, :], h.at[rows, :], in_sem.at[k])

    for f, core in own_pieces:
        load_piece(f, core).start()
    w_in = pltpu.make_async_copy(w_hbm, w, in_sem.at[4])
    w_in.start()
    for k in range(4):
        load_h(k).start()

    barrier = pltpu.get_barrier_semaphore()
    peers = [at_row(lax.rem(row + d, 8)) for d in range(1, 8)]
    peers += [at_col(lax.rem(y + d, 4), z) for d in range(1, 4)]
    peers += [at_col(y, lax.rem(z + d, 4)) for d in range(1, 4)]
    for dev in peers:
        pl.semaphore_signal(barrier, inc=1, device_id=dev, device_id_type=MESH)

    for f, core in own_pieces:
        load_piece(f, core).wait()
        hp[f * 2 + core] = hp16[f * 2 + core].astype(F32)
    with jax.named_scope("bar"):
        pl.semaphore_wait(barrier, len(peers))

    def send_pieces(v):
        for f, core in own_pieces:
            slot = 1 + (core + c) - 2 * core * c
            remote(hp.at[f * 2 + core, pl.ds(v * WAVE, WAVE), :], xl.at[slot, wave_rows(f, (v, 0, 0)), :],
                   xb_send.at[v], x_recv.at[f, v * 16], at_row(near * 2 + core)).start()

    send_pieces(0)
    for slot, dev in enumerate((partner, near_same, near_other)):
        remote(g_ref, gl.at[slot], g_send, g_recv.at[slot], dev).start()

    w_in.wait()

    def prep(b, rows):
        start = rows // 16 * 16
        for q in range(4):
            lanes = slice(q * 128, (q + 1) * 128)
            wide = w[start:min(start + 272, 8 * WORDS), lanes].astype(F32)
            part = wide[rows - start:rows - start + WORDS, :]
            wst[b, :, lanes] = jnp.concatenate([part, jnp.zeros((PAD - WORDS, 128), F32)], axis=0)

    with jax.named_scope("prep"):
        for b in range(8):
            prep(b, b * WORDS)

    def kind_block(chip, n):
        return ((3 - chip) * 2 + n) if n < 2 else (chip * 2 + n - 2)

    parts = ((0, 0, 128), (0, 128, 128), (1, 0, PAD), (2, 0, PAD), (3, 0, PAD))

    def send_near(p):
        n, w0, size = parts[p]
        rows = pl.ds(w0, size)
        remote(wst.at[kind_block(near, n), rows, :], wl.at[1, n, rows, :], wb_send, wb_recv.at[p], near_same).start()

    for n in range(4):
        remote(wst.at[kind_block(x, n)], wl.at[0, n], wp_send, wp_recv.at[n], partner).start()

    for k in range(4):
        load_h(k).wait()

        def squares(t, _, k=k):
            b = k * 8 + t
            hb = h[pl.ds(pl.multiple_of(b * BLOCK, BLOCK), BLOCK), :].astype(F32)
            sq = hb * hb
            part = (sq[:, 0:128] + sq[:, 128:256]) + (sq[:, 256:384] + sq[:, 384:512])
            ssq[row, pl.ds(b, 1), :] = jnp.sum(part.T, axis=0, keepdims=True)
            return 0

        with jax.named_scope("squares"):
            lax.fori_loop(0, 8, squares, 0)
    for d in range(1, 8):
        peer = lax.rem(row + d, 8)
        theirs = ssq.at[row, pl.ds(pl.multiple_of(lax.rem(peer, 2) * 16, 16), 16), :]
        remote(theirs, theirs, ssq_send, ssq_recv.at[row], at_row(peer)).start()

    for f in range(4):
        rows = pl.ds(f * 512, 512)
        xst[rows, :] = h[pl.ds(pl.multiple_of(mate * HALF + f * 512, 512), 512), :].astype(F32)
        remote(xst.at[rows, :], xl.at[0, rows, :], xp_send, xp_recv.at[f], partner).start()

    def relay_weights(p):
        n, w0, size = parts[p]
        rows = pl.ds(w0, size)
        with jax.named_scope("wrelay"):
            drain_recv(wl.at[1, n, rows, :], wb_recv.at[p])
        remote(wl.at[1, n, rows, :], wl.at[2, n, rows, :], wr_send, wr_recv.at[p], partner).start()

    def take_weights(p):
        n, w0, size = parts[p]
        rows = pl.ds(w0, size)
        with jax.named_scope("wtake"):
            if w0 == 0:
                drain_recv(wl.at[0, n], wp_recv.at[n])
            drain_recv(wl.at[2, n, rows, :], wr_recv.at[p])
        wbf[n, rows, 0:512] = wst[kind_block(x, n), rows, :].astype(BF16)
        for k in range(3):
            wbf[n, rows, (k + 1) * 512:(k + 2) * 512] = wl[k, n, rows, :].astype(BF16)

    ups = (at_col(lax.rem(y + 1, 4), z), at_col(lax.rem(y + 3, 4), z),
           at_col(y, lax.rem(z + 1, 4)), at_col(y, lax.rem(z + 3, 4)))
    along_first = (ups[0], ups[1], ups[2], ups[3])
    along_second = (ups[2], ups[3], ups[0], ups[1])

    def step_of(n):
        i = 3 - lax.rem(n, 4)
        reach = lax.div(n, 4) - i
        return reach, (lax.div(reach, 4), i, lax.rem(reach, 4))

    def each(lo, hi, body):
        def at(n, _):
            reach, t = step_of(n)

            @pl.when((reach >= 0) & (reach < 8))
            def _():
                body(t)
            return 0

        lax.fori_loop(lo, hi, at, 0)

    def serve(t):
        v, i, j = t
        step = v * 16 + i * 4 + j
        with jax.named_scope("serve"):
            refs = [xl.at[pl.ds(1, 2), wave_rows(f, t), :] for f in range(4)]
            for f, ref in enumerate(refs):
                drain_recv(ref, x_recv.at[f, step])

                @pl.when((j == 0) & (i < 3))
                def _():
                    remote(ref, ref, xf_send.at[f], x_recv.at[f, step + 4], along_first[f]).start()

            @pl.when(j < 3)
            def _():
                for f, ref in enumerate(refs):
                    remote(ref, ref, xf_send.at[f], x_recv.at[f, step + 1], along_second[f]).start()

    def scales():
        with jax.named_scope("wssq"):
            for d in range(1, 8):
                r = lax.rem(row + d, 8)
                drain_recv(ssq.at[r, pl.ds(0, 16), :], ssq_recv.at[r])
            for slot in range(3):
                drain_recv(gl.at[slot], g_recv.at[slot])
        mine = pl.ds(pl.multiple_of(c * 16, 16), 16)
        total = ssq[0, mine, :]
        for r in range(1, 8):
            total = total + ssq[r, mine, :]
        inv = lax.rsqrt(total / (FEAT * 8) + EPS)
        for b in range(16):
            rcol[b * BLOCK:(b + 1) * BLOCK, :] = jnp.broadcast_to(inv[b:b + 1, :], (BLOCK, BLOCK)).T

    def normalise(f, t):
        rows = wave_rows(f, t)
        scale = rcol[rows, :]
        for k in range(4):
            for q in range(4):
                lanes = slice(q * 128, (q + 1) * 128)
                if k == 0:
                    raw, gain = h[wave_rows(f, t, c * HALF), lanes].astype(F32), g_ref[:, lanes]
                else:
                    raw, gain = xl[k - 1, rows, lanes], gl[k - 1, :, lanes]
                xbf[rows, k * 512 + q * 128:k * 512 + (q + 1) * 128] = (raw * scale * gain).astype(BF16)

    def share(left, n, rows=slice(0, PAD)):
        return lax.dot_general(left, wbf[n, rows, :], (((1,), (1,)), ((), ())), preferred_element_type=F32)

    def far_group(t, words):
        with jax.named_scope("group"):
            left = jnp.concatenate([xbf[wave_rows(f, t), :] for f in range(4)], axis=0)
            value = share(left, 0, words)
            lanes = pl.ds(words.start, words.stop - words.start)
            rows = pl.ds(pl.multiple_of(((t[0] * 4 + t[1]) * 4 + t[2]) * GROUP, GROUP), GROUP)
            zs[0, rows, words] = value
            remote(zs.at[0, rows, lanes], zr.at[c, rows, lanes], z_send.at[0], zq_recv.at[c, t[1]],
                   at_row(far * 2)).start()

    def normalise_group(t):
        with jax.named_scope("norm"):
            for f in range(4):
                normalise(f, t)

    low, high, full = slice(0, 128), slice(128, PAD), slice(0, PAD)
    origin = tuple(jnp.int32(0) for _ in range(3))
    drain_send(xl.at[0, pl.ds(0, 128), :], xb_send.at[0])
    send_near(0)
    send_near(1)
    serve(origin)
    each(4, 8, serve)
    scales()
    for f in range(4):
        drain_recv(xl.at[0, pl.ds(f * 512, 512), :], xp_recv.at[f])
    relay_weights(0)
    each(0, 8, normalise_group)
    take_weights(0)
    each(0, 8, lambda t: far_group(t, low))

    def low_step(t):
        normalise_group(t)
        far_group(t, low)

    each(8, 11, lambda t: (serve(t), low_step(t)))
    relay_weights(1)
    send_pieces(1)
    for p in (2, 3, 4):
        send_near(p)
    each(11, 12, lambda t: (serve(t), low_step(t)))
    take_weights(1)
    each(0, 12, lambda t: far_group(t, high))

    def full_step(t):
        normalise_group(t)
        far_group(t, full)

    def ring_step(t):
        serve(t)
        full_step(t)

    each(12, 26, ring_step)
    relay_weights(2)
    each(26, 38, ring_step)
    relay_weights(3)
    each(38, 44, ring_step)
    take_weights(2)

    def block_rows(blk):
        return pl.ds(pl.multiple_of(blk * BLOCK, BLOCK), BLOCK)

    def step_far(blk, _):
        with jax.named_scope("far"):
            rows = block_rows(blk)
            zs[1, rows, :] = share(xbf[rows, :], 1)
            remote(zs.at[1, rows, :], zr.at[c, rows, :], z_send.at[1], z_recv.at[c, blk], at_row(far * 2 + 1)).start()
        return 0

    lax.fori_loop(0, 8, step_far, 0)
    relay_weights(4)
    lax.fori_loop(8, 16, step_far, 0)
    take_weights(3)
    take_weights(4)

    def pair_rows(pair):
        return pl.ds(pl.multiple_of(pair * 256, 256), 256)

    def step_own(pair, _):
        with jax.named_scope("own"):
            rows = pair_rows(pair)
            xl[0, rows, 256:512] = share(xbf[rows, :], 2 + mate)
            remote(xl.at[0, rows, pl.ds(256, 256)], zp.at[rows, :], zp_send, zp_recv.at[pair], partner).start()
            xl[0, rows, 0:256] = share(xbf[rows, :], 2 + c)
        return 0

    lax.fori_loop(0, 8, step_own, 0)

    for pair in range(8):
        drain_recv(zp.at[pair_rows(pair), :], zp_recv.at[pair])

    def arrived(half, n, i, f, c2, s):
        pieces = []
        for b in range(4):
            for v in range(2):
                group = (v * 4 + i) * 4 + lax.rem(s * (c2 - b) + 4, 4)
                start = c * (n * BLOCK + b * PIECE + v * WAVE) + mate * (group * GROUP + f * WAVE)
                pieces.append(zr[half, pl.ds(pl.multiple_of(start, WAVE), WAVE), :])
        return jnp.concatenate(pieces, axis=0)

    def finish(half, blk, value):
        z_ref[pl.ds(pl.multiple_of(half * HALF + blk * BLOCK, BLOCK), BLOCK), :] = value
        lane = lax.broadcasted_iota(jnp.int32, (BLOCK, 128), 1)
        left, right = value[:, 0:128], jnp.where(lane < WORDS - 128, value[:, 128:256], LOW)
        top = jnp.max(jnp.maximum(left, right).T, axis=0, keepdims=True)
        shift = jnp.broadcast_to(top, (BLOCK, BLOCK)).T
        mass = jnp.exp(left - shift) + jnp.exp(right - shift)
        st[0, pl.ds(half * 16 + blk, 1), :] = top
        st[1, pl.ds(half * 16 + blk, 1), :] = jnp.sum(mass.T, axis=0, keepdims=True)

    def step_out(n, _):
        i, f = lax.div(n, 4), lax.rem(n, 4)
        q, s = lax.div(f, 2), 1 - 2 * lax.rem(f, 2)
        c1, c2 = y * (1 - q) + z * q, z * (1 - q) + y * q
        blk = c * n + mate * (f * 4 + lax.rem(c1 - s * i + 4, 4))
        with jax.named_scope("wz"):
            @pl.when((c == 0) & (f == 0))
            def _():
                for half in range(2):
                    drain_recv(zr.at[half, pl.ds(0, 512), :], zq_recv.at[half, i])

            @pl.when(c == 1)
            def _():
                for half in range(2):
                    drain_recv(zr.at[half, block_rows(n), :], z_recv.at[half, n])
        rows = block_rows(blk)
        finish(c, blk, arrived(c, n, i, f, c2, s) + xl[0, rows, 0:256])
        finish(mate, blk, arrived(mate, n, i, f, c2, s) + zp[rows, :])
        return 0

    with jax.named_scope("finish"):
        lax.fori_loop(0, 16, step_out, 0)

    def exchange(buf, me, count, send, recv, dev):
        with jax.named_scope("exch"):
            for d in sorted(range(1, count), key=lambda d: abs(d - count // 2)):
                remote(buf.at[me], buf.at[me], send, recv.at[me], dev(lax.rem(me + d, count))).start()
            for d in range(1, count):
                other = lax.rem(me + d, count)
                drain_recv(buf.at[other], recv.at[other])
        top = buf[0]
        for k in range(1, count):
            top = jnp.maximum(top, buf[k])
        mass = jnp.exp(buf[0] - top)
        for k in range(1, count):
            mass = mass + jnp.exp(buf[k] - top)
        return top + jnp.log(mass)

    st1[row] = st[0] + jnp.log(st[1])
    st2[z] = exchange(st1, row, 8, st_send.at[0], st1_recv, at_row)
    st3[y] = exchange(st2, z, 4, st_send.at[1], st2_recv, lambda k: at_col(y, k))
    lse_ref[...] = exchange(st3, y, 4, st_send.at[2], st3_recv, lambda k: at_col(k, z))

    drain_send(ssq.at[pl.ds(0, 7), pl.ds(0, 16), :], ssq_send)
    drain_send(gl, g_send)
    drain_send(wl.at[0], wp_send)
    drain_send(wl.at[0], wb_send)
    drain_send(wl.at[0], wr_send)
    drain_send(xl.at[0], xp_send)
    drain_send(xl.at[0, pl.ds(0, 128), :], xb_send.at[1])
    for f in range(4):
        drain_send(xl.at[pl.ds(1, 2), pl.ds(0, 15 * PIECE), :], xf_send.at[f])
    for n in range(2):
        drain_send(zs.at[n], z_send.at[n])
    drain_send(zp, zp_send)
    drain_send(st1.at[pl.ds(0, 7)], st_send.at[0])
    drain_send(st2.at[pl.ds(0, 3)], st_send.at[1])
    drain_send(st3.at[pl.ds(0, 3)], st_send.at[2])


def solution(mesh):
    dma = pltpu.SemaphoreType.DMA

    def local_head(hidden, norm_gain, w_head):
        logits, log_norm = pl.pallas_call(
            kernel,
            out_shape=(pltpu.VMEM((SEQ, PAD), F32), pltpu.VMEM((32, 128), F32)),
            in_specs=[pl.BlockSpec(memory_space=pl.ANY), pl.BlockSpec(memory_space=pltpu.VMEM),
                      pl.BlockSpec(memory_space=pl.ANY)],
            out_specs=(pl.BlockSpec(memory_space=pltpu.VMEM), pl.BlockSpec(memory_space=pltpu.VMEM)),
            scratch_shapes=[
                pltpu.VMEM((SEQ, FEAT), BF16),
                pltpu.VMEM((8, PIECE, FEAT), BF16),
                pltpu.VMEM((8, PIECE, FEAT), F32),
                pltpu.VMEM((8 * WORDS, FEAT), BF16),
                pltpu.VMEM((8, PAD, FEAT), F32),
                pltpu.VMEM((3, 4, PAD, FEAT), F32),
                pltpu.VMEM((4, PAD, 4 * FEAT), BF16),
                pltpu.VMEM((HALF, FEAT), F32),
                pltpu.VMEM((3, HALF, FEAT), F32),
                pltpu.VMEM((HALF, 4 * FEAT), BF16),
                pltpu.VMEM((2, HALF, PAD), F32),
                pltpu.VMEM((HALF, PAD), F32),
                pltpu.VMEM((2, HALF, PAD), F32),
                pltpu.VMEM((3, 1, FEAT), F32),
                pltpu.VMEM((8, 32, 128), F32),
                pltpu.VMEM((HALF, 128), F32),
                pltpu.VMEM((2, 32, 128), F32),
                pltpu.VMEM((8, 32, 128), F32),
                pltpu.VMEM((4, 32, 128), F32),
                pltpu.VMEM((4, 32, 128), F32),
                dma((13,)),
                dma, dma((8,)),
                dma, dma((3,)),
                dma, dma((4,)),
                dma, dma((5,)),
                dma, dma((5,)),
                dma, dma((4,)),
                dma((2,)), dma((4,)), dma((4, 32)),
                dma((2,)), dma((2, 16)), dma((2, 4)),
                dma, dma((8,)),
                dma((3,)), dma((8,)), dma((4,)), dma((4,)),
            ],
            compiler_params=pltpu.CompilerParams(
                collective_id=0, has_side_effects=True, vmem_limit_bytes=59 * 1048576),
        )(hidden, norm_gain.reshape(1, FEAT), w_head.T)
        log_norm = log_norm.reshape(SEQ)
        return logits[:, :WORDS] - log_norm[:, None], log_norm

    return jax.shard_map(
        local_head,
        mesh=mesh,
        in_specs=(P("dp", "row"), P("row"), P("row", "col")),
        out_specs=(P("dp", ("col", "row")), P("dp")),
        check_vma=False,
    )
```

```python
import functools

import jax
import jax.numpy as jnp
from jax import lax
from jax.experimental import pallas as pl
from jax.experimental.pallas import tpu as pltpu
from jax.sharding import PartitionSpec as P

EPS = 1e-5
MESH = pl.DeviceIdType.MESH
F32 = jnp.float32
BF16 = jnp.bfloat16
LOW = -3.0e38

SEQ, FEAT, WORDS, PAD = 4096, 512, 250, 256
HALF = SEQ // 2
BLOCK, PIECE, WAVE, GROUP = 128, 32, 16, 64


def kernel(h_hbm, g_ref, w_hbm, z_ref, lse_ref,
           h, hp16, hp, w, wst, wl, wbf, xst, xl, xbf, zs, zp, zr, gl, ssq, rcol, st, st1, st2, st3,
           in_sem, ssq_send, ssq_recv, g_send, g_recv, wp_send, wp_recv, wb_send, wb_recv, wr_send, wr_recv,
           xp_send, xp_recv, xb_send, xf_send, x_recv, z_send, z_recv, zq_recv, zp_send, zp_recv,
           st_send, st1_recv, st2_recv, st3_recv):
    col, row = lax.axis_index("col"), lax.axis_index("row")
    z, y = lax.div(col, 4), lax.rem(col, 4)
    x, c = lax.div(row, 2), lax.rem(row, 2)
    mate = 1 - c
    near = x + 1 - 2 * lax.rem(x, 2)
    far = 3 - x

    def at_row(r):
        return (0, col, r)

    def at_col(yy, zz):
        return (0, zz * 4 + yy, row)

    partner = at_row(x * 2 + mate)
    near_same = at_row(near * 2 + c)
    near_other = at_row(near * 2 + mate)

    def remote(src, dst, send, recv, dev):
        return pltpu.make_async_remote_copy(
            src_ref=src, dst_ref=dst, send_sem=send, recv_sem=recv, device_id=dev, device_id_type=MESH)

    def drain_send(ref, sem):
        remote(ref, ref, sem, sem, partner).wait_send()

    def drain_recv(ref, sem):
        remote(ref, ref, sem, sem, partner).wait_recv()

    firsts, seconds = (y, y, z, z), (z, z, y, y)
    signs = (1, -1, 1, -1)

    def first(f, i):
        return lax.rem(firsts[f] - signs[f] * i + 4, 4)

    def second(f, j):
        return lax.rem(seconds[f] - signs[f] * j + 4, 4)

    def piece_base(f, i, j):
        return f * 512 + first(f, i) * BLOCK + second(f, j) * PIECE

    def piece_rows(f, i, j, offset=0):
        return pl.ds(pl.multiple_of(offset + piece_base(f, i, j), PIECE), PIECE)

    def wave_rows(f, t, offset=0):
        v, i, j = t
        return pl.ds(pl.multiple_of(offset + v * WAVE + piece_base(f, i, j), WAVE), WAVE)

    own_pieces = [(f, core) for f in range(4) for core in range(2)]

    def load_piece(f, core):
        return pltpu.make_async_copy(
            h_hbm.at[piece_rows(f, 0, 0, core * HALF), :], hp16.at[f * 2 + core], in_sem.at[5 + f * 2 + core])

    def load_h(k):
        rows = pl.ds(k * 1024, 1024)
        return pltpu.make_async_copy(h_hbm.at[rows, :], h.at[rows, :], in_sem.at[k])

    for f, core in own_pieces:
        load_piece(f, core).start()
    w_in = pltpu.make_async_copy(w_hbm, w, in_sem.at[4])
    w_in.start()
    for k in range(4):
        load_h(k).start()

    barrier = pltpu.get_barrier_semaphore()
    peers = [at_row(lax.rem(row + d, 8)) for d in range(1, 8)]
    peers += [at_col(lax.rem(y + d, 4), z) for d in range(1, 4)]
    peers += [at_col(y, lax.rem(z + d, 4)) for d in range(1, 4)]
    for dev in peers:
        pl.semaphore_signal(barrier, inc=1, device_id=dev, device_id_type=MESH)

    for f, core in own_pieces:
        load_piece(f, core).wait()
        hp[f * 2 + core] = hp16[f * 2 + core].astype(F32)
    with jax.named_scope("bar"):
        pl.semaphore_wait(barrier, len(peers))

    def send_pieces(v):
        for f, core in own_pieces:
            slot = 1 + (core + c) - 2 * core * c
            remote(hp.at[f * 2 + core, pl.ds(v * WAVE, WAVE), :], xl.at[slot, wave_rows(f, (v, 0, 0)), :],
                   xb_send.at[v], x_recv.at[f, v * 16], at_row(near * 2 + core)).start()

    send_pieces(0)
    for slot, dev in enumerate((partner, near_same, near_other)):
        remote(g_ref, gl.at[slot], g_send, g_recv.at[slot], dev).start()

    w_in.wait()

    def prep(b, rows):
        start = rows // 16 * 16
        for q in range(4):
            lanes = slice(q * 128, (q + 1) * 128)
            wide = w[start:min(start + 272, 8 * WORDS), lanes].astype(F32)
            part = wide[rows - start:rows - start + WORDS, :]
            wst[b, :, lanes] = jnp.concatenate([part, jnp.zeros((PAD - WORDS, 128), F32)], axis=0)

    with jax.named_scope("prep"):
        for b in range(8):
            prep(b, b * WORDS)

    def kind_block(chip, n):
        return ((3 - chip) * 2 + n) if n < 2 else (chip * 2 + n - 2)

    parts = ((0, 0, 128), (0, 128, 128), (1, 0, PAD), (2, 0, PAD), (3, 0, PAD))

    def send_near(p):
        n, w0, size = parts[p]
        rows = pl.ds(w0, size)
        remote(wst.at[kind_block(near, n), rows, :], wl.at[1, n, rows, :], wb_send, wb_recv.at[p], near_same).start()

    for n in range(4):
        remote(wst.at[kind_block(x, n)], wl.at[0, n], wp_send, wp_recv.at[n], partner).start()

    for k in range(4):
        load_h(k).wait()

        def squares(t, _, k=k):
            b = k * 8 + t
            hb = h[pl.ds(pl.multiple_of(b * BLOCK, BLOCK), BLOCK), :].astype(F32)
            sq = hb * hb
            part = (sq[:, 0:128] + sq[:, 128:256]) + (sq[:, 256:384] + sq[:, 384:512])
            ssq[row, pl.ds(b, 1), :] = jnp.sum(part.T, axis=0, keepdims=True)
            return 0

        with jax.named_scope("squares"):
            lax.fori_loop(0, 8, squares, 0)
    for d in range(1, 8):
        peer = lax.rem(row + d, 8)
        theirs = ssq.at[row, pl.ds(pl.multiple_of(lax.rem(peer, 2) * 16, 16), 16), :]
        remote(theirs, theirs, ssq_send, ssq_recv.at[row], at_row(peer)).start()

    for f in range(4):
        rows = pl.ds(f * 512, 512)
        xst[rows, :] = h[pl.ds(pl.multiple_of(mate * HALF + f * 512, 512), 512), :].astype(F32)
        remote(xst.at[rows, :], xl.at[0, rows, :], xp_send, xp_recv.at[f], partner).start()

    def relay_weights(p):
        n, w0, size = parts[p]
        rows = pl.ds(w0, size)
        with jax.named_scope("wrelay"):
            drain_recv(wl.at[1, n, rows, :], wb_recv.at[p])
        remote(wl.at[1, n, rows, :], wl.at[2, n, rows, :], wr_send, wr_recv.at[p], partner).start()

    def take_weights(p):
        n, w0, size = parts[p]
        rows = pl.ds(w0, size)
        with jax.named_scope("wtake"):
            if w0 == 0:
                drain_recv(wl.at[0, n], wp_recv.at[n])
            drain_recv(wl.at[2, n, rows, :], wr_recv.at[p])
        wbf[n, rows, 0:512] = wst[kind_block(x, n), rows, :].astype(BF16)
        for k in range(3):
            wbf[n, rows, (k + 1) * 512:(k + 2) * 512] = wl[k, n, rows, :].astype(BF16)

    ups = (at_col(lax.rem(y + 1, 4), z), at_col(lax.rem(y + 3, 4), z),
           at_col(y, lax.rem(z + 1, 4)), at_col(y, lax.rem(z + 3, 4)))
    along_first = (ups[0], ups[1], ups[2], ups[3])
    along_second = (ups[2], ups[3], ups[0], ups[1])

    def step_of(n):
        i = 3 - lax.rem(n, 4)
        reach = lax.div(n, 4) - i
        return reach, (lax.div(reach, 4), i, lax.rem(reach, 4))

    def each(lo, hi, body):
        def at(n, _):
            reach, t = step_of(n)

            @pl.when((reach >= 0) & (reach < 8))
            def _():
                body(t)
            return 0

        lax.fori_loop(lo, hi, at, 0)

    def serve(t):
        v, i, j = t
        step = v * 16 + i * 4 + j
        with jax.named_scope("serve"):
            refs = [xl.at[pl.ds(1, 2), wave_rows(f, t), :] for f in range(4)]
            for f, ref in enumerate(refs):
                drain_recv(ref, x_recv.at[f, step])

                @pl.when((j == 0) & (i < 3))
                def _():
                    remote(ref, ref, xf_send.at[f], x_recv.at[f, step + 4], along_first[f]).start()

            @pl.when(j < 3)
            def _():
                for f, ref in enumerate(refs):
                    remote(ref, ref, xf_send.at[f], x_recv.at[f, step + 1], along_second[f]).start()

    def scales():
        with jax.named_scope("wssq"):
            for d in range(1, 8):
                r = lax.rem(row + d, 8)
                drain_recv(ssq.at[r, pl.ds(0, 16), :], ssq_recv.at[r])
            for slot in range(3):
                drain_recv(gl.at[slot], g_recv.at[slot])
        mine = pl.ds(pl.multiple_of(c * 16, 16), 16)
        total = ssq[0, mine, :]
        for r in range(1, 8):
            total = total + ssq[r, mine, :]
        inv = lax.rsqrt(total / (FEAT * 8) + EPS)
        for b in range(16):
            rcol[b * BLOCK:(b + 1) * BLOCK, :] = jnp.broadcast_to(inv[b:b + 1, :], (BLOCK, BLOCK)).T

    def normalise(f, t):
        rows = wave_rows(f, t)
        scale = rcol[rows, :]
        for k in range(4):
            for q in range(4):
                lanes = slice(q * 128, (q + 1) * 128)
                if k == 0:
                    raw, gain = h[wave_rows(f, t, c * HALF), lanes].astype(F32), g_ref[:, lanes]
                else:
                    raw, gain = xl[k - 1, rows, lanes], gl[k - 1, :, lanes]
                xbf[rows, k * 512 + q * 128:k * 512 + (q + 1) * 128] = (raw * scale * gain).astype(BF16)

    def share(left, n, rows=slice(0, PAD)):
        return lax.dot_general(left, wbf[n, rows, :], (((1,), (1,)), ((), ())), preferred_element_type=F32)

    def far_group(t, words):
        with jax.named_scope("group"):
            left = jnp.concatenate([xbf[wave_rows(f, t), :] for f in range(4)], axis=0)
            value = share(left, 0, words)
            lanes = pl.ds(words.start, words.stop - words.start)
            rows = pl.ds(pl.multiple_of(((t[0] * 4 + t[1]) * 4 + t[2]) * GROUP, GROUP), GROUP)
            zs[0, rows, words] = value
            remote(zs.at[0, rows, lanes], zr.at[c, rows, lanes], z_send.at[0], zq_recv.at[c, t[1]],
                   at_row(far * 2)).start()

    def normalise_group(t):
        with jax.named_scope("norm"):
            for f in range(4):
                normalise(f, t)

    def block_rows(blk):
        return pl.ds(pl.multiple_of(blk * BLOCK, BLOCK), BLOCK)

    def block_of(n):
        i, f = lax.div(n, 4), lax.rem(n, 4)
        q, s = lax.div(f, 2), 1 - 2 * lax.rem(f, 2)
        c1, c2 = y * (1 - q) + z * q, z * (1 - q) + y * q
        return i, f, f * 4 + lax.rem(c1 - s * i + 4, 4), c2, s

    def step_far(n, _):
        with jax.named_scope("far"):
            blk = block_of(n)[2]
            rows = block_rows(blk)
            zs[1, rows, :] = share(xbf[rows, :], 1)
            remote(zs.at[1, rows, :], zr.at[c, rows, :], z_send.at[1], z_recv.at[c, blk], at_row(far * 2 + 1)).start()
        return 0

    low, high, full = slice(0, 128), slice(128, PAD), slice(0, PAD)
    origin = tuple(jnp.int32(0) for _ in range(3))
    drain_send(xl.at[0, pl.ds(0, 128), :], xb_send.at[0])
    send_near(0)
    send_near(1)
    serve(origin)
    each(4, 8, serve)
    scales()
    for f in range(4):
        drain_recv(xl.at[0, pl.ds(f * 512, 512), :], xp_recv.at[f])
    relay_weights(0)
    each(0, 8, normalise_group)
    take_weights(0)
    each(0, 8, lambda t: far_group(t, low))

    def low_step(t):
        normalise_group(t)
        far_group(t, low)

    each(8, 11, lambda t: (serve(t), low_step(t)))
    relay_weights(1)
    send_pieces(1)
    for p in (2, 3, 4):
        send_near(p)
    each(11, 12, lambda t: (serve(t), low_step(t)))
    take_weights(1)
    each(0, 12, lambda t: far_group(t, high))

    def full_step(t):
        normalise_group(t)
        far_group(t, full)

    def ring_step(t):
        serve(t)
        full_step(t)

    each(12, 26, ring_step)
    relay_weights(2)
    each(26, 32, ring_step)
    take_weights(2)

    def mixed_step(n, _):
        each(n, n + 1, ring_step)
        return step_far(n - 32, 0)

    lax.fori_loop(32, 36, mixed_step, 0)
    each(36, 38, ring_step)
    relay_weights(3)
    each(38, 44, ring_step)

    lax.fori_loop(4, 10, step_far, 0)
    relay_weights(4)
    lax.fori_loop(10, 16, step_far, 0)
    take_weights(3)
    take_weights(4)

    def pair_rows(pair):
        return pl.ds(pl.multiple_of(pair * 256, 256), 256)

    def step_own(pair, _):
        with jax.named_scope("own"):
            rows = pair_rows(pair)
            xl[0, rows, 256:512] = share(xbf[rows, :], 2 + mate)
            remote(xl.at[0, rows, pl.ds(256, 256)], zp.at[rows, :], zp_send, zp_recv.at[pair], partner).start()
            xl[0, rows, 0:256] = share(xbf[rows, :], 2 + c)
        return 0

    lax.fori_loop(0, 8, step_own, 0)

    for pair in range(8):
        drain_recv(zp.at[pair_rows(pair), :], zp_recv.at[pair])

    def arrived(half, i, f, blk, c2, s):
        pieces = []
        for b in range(4):
            for v in range(2):
                group = (v * 4 + i) * 4 + lax.rem(s * (c2 - b) + 4, 4)
                start = c * (blk * BLOCK + b * PIECE + v * WAVE) + mate * (group * GROUP + f * WAVE)
                pieces.append(zr[half, pl.ds(pl.multiple_of(start, WAVE), WAVE), :])
        return jnp.concatenate(pieces, axis=0)

    def finish(half, blk, value):
        z_ref[pl.ds(pl.multiple_of(half * HALF + blk * BLOCK, BLOCK), BLOCK), :] = value
        lane = lax.broadcasted_iota(jnp.int32, (BLOCK, 128), 1)
        left, right = value[:, 0:128], jnp.where(lane < WORDS - 128, value[:, 128:256], LOW)
        top = jnp.max(jnp.maximum(left, right).T, axis=0, keepdims=True)
        shift = jnp.broadcast_to(top, (BLOCK, BLOCK)).T
        mass = jnp.exp(left - shift) + jnp.exp(right - shift)
        st[0, pl.ds(half * 16 + blk, 1), :] = top
        st[1, pl.ds(half * 16 + blk, 1), :] = jnp.sum(mass.T, axis=0, keepdims=True)

    def step_out(n, _):
        i, f, blk, c2, s = block_of(n)
        with jax.named_scope("wz"):
            @pl.when((c == 0) & (f == 0))
            def _():
                for half in range(2):
                    drain_recv(zr.at[half, pl.ds(0, 512), :], zq_recv.at[half, i])

            @pl.when(c == 1)
            def _():
                for half in range(2):
                    drain_recv(zr.at[half, block_rows(blk), :], z_recv.at[half, blk])
        rows = block_rows(blk)
        finish(c, blk, arrived(c, i, f, blk, c2, s) + xl[0, rows, 0:256])
        finish(mate, blk, arrived(mate, i, f, blk, c2, s) + zp[rows, :])
        return 0

    drain_send(ssq.at[pl.ds(0, 7), pl.ds(0, 16), :], ssq_send)
    drain_send(gl, g_send)
    drain_send(wl.at[0], wp_send)
    drain_send(wl.at[0], wb_send)
    drain_send(wl.at[0], wr_send)
    drain_send(xl.at[0], xp_send)
    drain_send(xl.at[0, pl.ds(0, 128), :], xb_send.at[1])
    for f in range(4):
        drain_send(xl.at[pl.ds(1, 2), pl.ds(0, 15 * PIECE), :], xf_send.at[f])
    drain_send(zp, zp_send)

    with jax.named_scope("finish"):
        lax.fori_loop(0, 16, step_out, 0)

    def exchange(buf, me, count, send, recv, dev):
        with jax.named_scope("exch"):
            for d in sorted(range(1, count), key=lambda d: abs(d - count // 2)):
                remote(buf.at[me], buf.at[me], send, recv.at[me], dev(lax.rem(me + d, count))).start()
            for d in range(1, count):
                other = lax.rem(me + d, count)
                drain_recv(buf.at[other], recv.at[other])
        top = buf[0]
        for k in range(1, count):
            top = jnp.maximum(top, buf[k])
        mass = jnp.exp(buf[0] - top)
        for k in range(1, count):
            mass = mass + jnp.exp(buf[k] - top)
        return top + jnp.log(mass)

    st1[row] = st[0] + jnp.log(st[1])
    st2[z] = exchange(st1, row, 8, st_send.at[0], st1_recv, at_row)
    for n in range(2):
        drain_send(zs.at[n], z_send.at[n])
    st3[y] = exchange(st2, z, 4, st_send.at[1], st2_recv, lambda k: at_col(y, k))
    lse_ref[...] = exchange(st3, y, 4, st_send.at[2], st3_recv, lambda k: at_col(k, z))

    drain_send(st1.at[pl.ds(0, 7)], st_send.at[0])
    drain_send(st2.at[pl.ds(0, 3)], st_send.at[1])
    drain_send(st3.at[pl.ds(0, 3)], st_send.at[2])


def solution(mesh):
    dma = pltpu.SemaphoreType.DMA

    def local_head(hidden, norm_gain, w_head):
        logits, log_norm = pl.pallas_call(
            kernel,
            out_shape=(pltpu.VMEM((SEQ, PAD), F32), pltpu.VMEM((32, 128), F32)),
            in_specs=[pl.BlockSpec(memory_space=pl.ANY), pl.BlockSpec(memory_space=pltpu.VMEM),
                      pl.BlockSpec(memory_space=pl.ANY)],
            out_specs=(pl.BlockSpec(memory_space=pltpu.VMEM), pl.BlockSpec(memory_space=pltpu.VMEM)),
            scratch_shapes=[
                pltpu.VMEM((SEQ, FEAT), BF16),
                pltpu.VMEM((8, PIECE, FEAT), BF16),
                pltpu.VMEM((8, PIECE, FEAT), F32),
                pltpu.VMEM((8 * WORDS, FEAT), BF16),
                pltpu.VMEM((8, PAD, FEAT), F32),
                pltpu.VMEM((3, 4, PAD, FEAT), F32),
                pltpu.VMEM((4, PAD, 4 * FEAT), BF16),
                pltpu.VMEM((HALF, FEAT), F32),
                pltpu.VMEM((3, HALF, FEAT), F32),
                pltpu.VMEM((HALF, 4 * FEAT), BF16),
                pltpu.VMEM((2, HALF, PAD), F32),
                pltpu.VMEM((HALF, PAD), F32),
                pltpu.VMEM((2, HALF, PAD), F32),
                pltpu.VMEM((3, 1, FEAT), F32),
                pltpu.VMEM((8, 32, 128), F32),
                pltpu.VMEM((HALF, 128), F32),
                pltpu.VMEM((2, 32, 128), F32),
                pltpu.VMEM((8, 32, 128), F32),
                pltpu.VMEM((4, 32, 128), F32),
                pltpu.VMEM((4, 32, 128), F32),
                dma((13,)),
                dma, dma((8,)),
                dma, dma((3,)),
                dma, dma((4,)),
                dma, dma((5,)),
                dma, dma((5,)),
                dma, dma((4,)),
                dma((2,)), dma((4,)), dma((4, 32)),
                dma((2,)), dma((2, 16)), dma((2, 4)),
                dma, dma((8,)),
                dma((3,)), dma((8,)), dma((4,)), dma((4,)),
            ],
            compiler_params=pltpu.CompilerParams(
                collective_id=0, has_side_effects=True, vmem_limit_bytes=59 * 1048576),
        )(hidden, norm_gain.reshape(1, FEAT), w_head.T)
        log_norm = log_norm.reshape(SEQ)
        return logits[:, :WORDS] - log_norm[:, None], log_norm

    return jax.shard_map(
        local_head,
        mesh=mesh,
        in_specs=(P("dp", "row"), P("row"), P("row", "col")),
        out_specs=(P("dp", ("col", "row")), P("dp")),
        check_vma=False,
    )
```

```python
import functools

import jax
import jax.numpy as jnp
from jax import lax
from jax.experimental import pallas as pl
from jax.experimental.pallas import tpu as pltpu
from jax.sharding import PartitionSpec as P

EPS = 1e-5
MESH = pl.DeviceIdType.MESH
F32 = jnp.float32
BF16 = jnp.bfloat16
LOW = -3.0e38

SEQ, FEAT, WORDS, PAD = 4096, 512, 250, 256
HALF = SEQ // 2
BLOCK, PIECE, WAVE, GROUP = 128, 32, 16, 64


def kernel(h_hbm, g_ref, w_hbm, z_ref, lse_ref,
           h, hp16, hp, w, wst, wl, wbf, xst, xl, xbf, zs, zp, zr, gl, ssq, rcol, st, st1, st2, st3,
           in_sem, ssq_send, ssq_recv, g_send, g_recv, wp_send, wp_recv, wb_send, wb_recv, wr_send, wr_recv,
           xp_send, xp_recv, xb_send, xf_send, x_recv, z_send, z_recv, zq_recv, zp_send, zp_recv,
           st_send, st1_recv, st2_recv, st3_recv):
    col, row = lax.axis_index("col"), lax.axis_index("row")
    z, y = lax.div(col, 4), lax.rem(col, 4)
    x, c = lax.div(row, 2), lax.rem(row, 2)
    mate = 1 - c
    near = x + 1 - 2 * lax.rem(x, 2)
    far = 3 - x

    def at_row(r):
        return (0, col, r)

    def at_col(yy, zz):
        return (0, zz * 4 + yy, row)

    partner = at_row(x * 2 + mate)
    near_same = at_row(near * 2 + c)
    near_other = at_row(near * 2 + mate)

    def remote(src, dst, send, recv, dev):
        return pltpu.make_async_remote_copy(
            src_ref=src, dst_ref=dst, send_sem=send, recv_sem=recv, device_id=dev, device_id_type=MESH)

    def drain_send(ref, sem):
        remote(ref, ref, sem, sem, partner).wait_send()

    def drain_recv(ref, sem):
        remote(ref, ref, sem, sem, partner).wait_recv()

    firsts, seconds = (y, y, z, z), (z, z, y, y)
    signs = (1, -1, 1, -1)

    def first(f, i):
        return lax.rem(firsts[f] - signs[f] * i + 4, 4)

    def second(f, j):
        return lax.rem(seconds[f] - signs[f] * j + 4, 4)

    def piece_base(f, i, j):
        return f * 512 + first(f, i) * BLOCK + second(f, j) * PIECE

    def piece_rows(f, i, j, offset=0):
        return pl.ds(pl.multiple_of(offset + piece_base(f, i, j), PIECE), PIECE)

    def wave_rows(f, t, offset=0):
        v, i, j = t
        return pl.ds(pl.multiple_of(offset + v * WAVE + piece_base(f, i, j), WAVE), WAVE)

    own_pieces = [(f, core) for f in range(4) for core in range(2)]

    def load_piece(f, core):
        return pltpu.make_async_copy(
            h_hbm.at[piece_rows(f, 0, 0, core * HALF), :], hp16.at[f * 2 + core], in_sem.at[5 + f * 2 + core])

    def load_h(k):
        rows = pl.ds(k * 1024, 1024)
        return pltpu.make_async_copy(h_hbm.at[rows, :], h.at[rows, :], in_sem.at[k])

    for f, core in own_pieces:
        load_piece(f, core).start()
    w_in = pltpu.make_async_copy(w_hbm, w, in_sem.at[4])
    w_in.start()
    for k in range(4):
        load_h(k).start()

    barrier = pltpu.get_barrier_semaphore()
    peers = [at_row(lax.rem(row + d, 8)) for d in range(1, 8)]
    peers += [at_col(lax.rem(y + d, 4), z) for d in range(1, 4)]
    peers += [at_col(y, lax.rem(z + d, 4)) for d in range(1, 4)]
    for dev in peers:
        pl.semaphore_signal(barrier, inc=1, device_id=dev, device_id_type=MESH)

    for f, core in own_pieces:
        load_piece(f, core).wait()
        hp[f * 2 + core] = hp16[f * 2 + core].astype(F32)
    with jax.named_scope("bar"):
        pl.semaphore_wait(barrier, len(peers))

    def send_pieces(v):
        for f, core in own_pieces:
            slot = 1 + (core + c) - 2 * core * c
            remote(hp.at[f * 2 + core, pl.ds(v * WAVE, WAVE), :], xl.at[slot, wave_rows(f, (v, 0, 0)), :],
                   xb_send.at[v], x_recv.at[f, v * 16], at_row(near * 2 + core)).start()

    send_pieces(0)
    for slot, dev in enumerate((partner, near_same, near_other)):
        remote(g_ref, gl.at[slot], g_send, g_recv.at[slot], dev).start()

    w_in.wait()

    def prep(b, rows):
        start = rows // 16 * 16
        for q in range(4):
            lanes = slice(q * 128, (q + 1) * 128)
            wide = w[start:min(start + 272, 8 * WORDS), lanes].astype(F32)
            part = wide[rows - start:rows - start + WORDS, :]
            wst[b, :, lanes] = jnp.concatenate([part, jnp.zeros((PAD - WORDS, 128), F32)], axis=0)

    with jax.named_scope("prep"):
        for b in range(8):
            prep(b, b * WORDS)

    def kind_block(chip, n):
        return ((3 - chip) * 2 + n) if n < 2 else (chip * 2 + n - 2)

    parts = ((0, 0, 128), (0, 128, 128), (1, 0, PAD), (2, 0, PAD), (3, 0, PAD))

    def send_near(p):
        n, w0, size = parts[p]
        rows = pl.ds(w0, size)
        remote(wst.at[kind_block(near, n), rows, :], wl.at[1, n, rows, :], wb_send, wb_recv.at[p], near_same).start()

    def send_partner(n):
        remote(wst.at[kind_block(x, n)], wl.at[0, n], wp_send, wp_recv.at[n], partner).start()

    send_partner(0)

    for k in range(4):
        load_h(k).wait()

        def squares(t, _, k=k):
            b = k * 8 + t
            hb = h[pl.ds(pl.multiple_of(b * BLOCK, BLOCK), BLOCK), :].astype(F32)
            sq = hb * hb
            part = (sq[:, 0:128] + sq[:, 128:256]) + (sq[:, 256:384] + sq[:, 384:512])
            ssq[row, pl.ds(b, 1), :] = jnp.sum(part.T, axis=0, keepdims=True)
            return 0

        with jax.named_scope("squares"):
            lax.fori_loop(0, 8, squares, 0)
    for d in range(1, 8):
        peer = lax.rem(row + d, 8)
        theirs = ssq.at[row, pl.ds(pl.multiple_of(lax.rem(peer, 2) * 16, 16), 16), :]
        remote(theirs, theirs, ssq_send, ssq_recv.at[row], at_row(peer)).start()

    for f in range(4):
        rows = pl.ds(f * 512, 512)
        xst[rows, :] = h[pl.ds(pl.multiple_of(mate * HALF + f * 512, 512), 512), :].astype(F32)
        remote(xst.at[rows, :], xl.at[0, rows, :], xp_send, xp_recv.at[f], partner).start()

    def relay_weights(p):
        n, w0, size = parts[p]
        rows = pl.ds(w0, size)
        with jax.named_scope("wrelay"):
            drain_recv(wl.at[1, n, rows, :], wb_recv.at[p])
        remote(wl.at[1, n, rows, :], wl.at[2, n, rows, :], wr_send, wr_recv.at[p], partner).start()

    def take_weights(p):
        n, w0, size = parts[p]
        rows = pl.ds(w0, size)
        with jax.named_scope("wtake"):
            if w0 == 0:
                drain_recv(wl.at[0, n], wp_recv.at[n])
            drain_recv(wl.at[2, n, rows, :], wr_recv.at[p])
        wbf[n, rows, 0:512] = wst[kind_block(x, n), rows, :].astype(BF16)
        for k in range(3):
            wbf[n, rows, (k + 1) * 512:(k + 2) * 512] = wl[k, n, rows, :].astype(BF16)

    ups = (at_col(lax.rem(y + 1, 4), z), at_col(lax.rem(y + 3, 4), z),
           at_col(y, lax.rem(z + 1, 4)), at_col(y, lax.rem(z + 3, 4)))
    along_first = (ups[0], ups[1], ups[2], ups[3])
    along_second = (ups[2], ups[3], ups[0], ups[1])

    def step_of(n):
        i = 3 - lax.rem(n, 4)
        reach = lax.div(n, 4) - i
        return reach, (lax.div(reach, 4), i, lax.rem(reach, 4))

    def each(lo, hi, body):
        def at(n, _):
            reach, t = step_of(n)

            @pl.when((reach >= 0) & (reach < 8))
            def _():
                body(t)
            return 0

        lax.fori_loop(lo, hi, at, 0)

    def serve(t):
        v, i, j = t
        step = v * 16 + i * 4 + j
        with jax.named_scope("serve"):
            refs = [xl.at[pl.ds(1, 2), wave_rows(f, t), :] for f in range(4)]
            for f, ref in enumerate(refs):
                drain_recv(ref, x_recv.at[f, step])

                @pl.when((j == 0) & (i < 3))
                def _():
                    remote(ref, ref, xf_send.at[f], x_recv.at[f, step + 4], along_first[f]).start()

            @pl.when(j < 3)
            def _():
                for f, ref in enumerate(refs):
                    remote(ref, ref, xf_send.at[f], x_recv.at[f, step + 1], along_second[f]).start()

    def scales():
        with jax.named_scope("wssq"):
            for d in range(1, 8):
                r = lax.rem(row + d, 8)
                drain_recv(ssq.at[r, pl.ds(0, 16), :], ssq_recv.at[r])
            for slot in range(3):
                drain_recv(gl.at[slot], g_recv.at[slot])
        mine = pl.ds(pl.multiple_of(c * 16, 16), 16)
        total = ssq[0, mine, :]
        for r in range(1, 8):
            total = total + ssq[r, mine, :]
        inv = lax.rsqrt(total / (FEAT * 8) + EPS)
        for b in range(16):
            rcol[b * BLOCK:(b + 1) * BLOCK, :] = jnp.broadcast_to(inv[b:b + 1, :], (BLOCK, BLOCK)).T

    def normalise(f, t):
        rows = wave_rows(f, t)
        scale = rcol[rows, :]
        for k in range(4):
            for q in range(4):
                lanes = slice(q * 128, (q + 1) * 128)
                if k == 0:
                    raw, gain = h[wave_rows(f, t, c * HALF), lanes].astype(F32), g_ref[:, lanes]
                else:
                    raw, gain = xl[k - 1, rows, lanes], gl[k - 1, :, lanes]
                xbf[rows, k * 512 + q * 128:k * 512 + (q + 1) * 128] = (raw * scale * gain).astype(BF16)

    def share(left, n, rows=slice(0, PAD)):
        return lax.dot_general(left, wbf[n, rows, :], (((1,), (1,)), ((), ())), preferred_element_type=F32)

    def far_group(t, words):
        with jax.named_scope("group"):
            left = jnp.concatenate([xbf[wave_rows(f, t), :] for f in range(4)], axis=0)
            value = share(left, 0, words)
            lanes = pl.ds(words.start, words.stop - words.start)
            rows = pl.ds(pl.multiple_of(((t[0] * 4 + t[1]) * 4 + t[2]) * GROUP, GROUP), GROUP)
            zs[0, rows, words] = value
            remote(zs.at[0, rows, lanes], zr.at[c, rows, lanes], z_send.at[0], zq_recv.at[c, t[1]],
                   at_row(far * 2)).start()

    def normalise_group(t):
        with jax.named_scope("norm"):
            for f in range(4):
                normalise(f, t)

    def block_rows(blk):
        return pl.ds(pl.multiple_of(blk * BLOCK, BLOCK), BLOCK)

    def block_of(n):
        i, f = lax.div(n, 4), lax.rem(n, 4)
        q, s = lax.div(f, 2), 1 - 2 * lax.rem(f, 2)
        c1, c2 = y * (1 - q) + z * q, z * (1 - q) + y * q
        return i, f, f * 4 + lax.rem(c1 - s * i + 4, 4), c2, s

    def step_far(n, _):
        with jax.named_scope("far"):
            blk = block_of(n)[2]
            rows = block_rows(blk)
            zs[1, rows, :] = share(xbf[rows, :], 1)
            remote(zs.at[1, rows, :], zr.at[c, rows, :], z_send.at[1], z_recv.at[c, blk], at_row(far * 2 + 1)).start()
        return 0

    low, high, full = slice(0, 128), slice(128, PAD), slice(0, PAD)
    origin = tuple(jnp.int32(0) for _ in range(3))
    drain_send(xl.at[0, pl.ds(0, 128), :], xb_send.at[0])
    send_near(0)
    send_near(1)
    serve(origin)
    each(4, 8, serve)
    scales()
    for f in range(4):
        drain_recv(xl.at[0, pl.ds(f * 512, 512), :], xp_recv.at[f])
    relay_weights(0)
    each(0, 8, normalise_group)
    take_weights(0)
    each(0, 8, lambda t: far_group(t, low))

    def low_step(t):
        normalise_group(t)
        far_group(t, low)

    each(8, 11, lambda t: (serve(t), low_step(t)))
    relay_weights(1)
    send_pieces(1)
    for p in (2, 3, 4):
        send_near(p)
    for n in range(1, 4):
        send_partner(n)
    each(11, 12, lambda t: (serve(t), low_step(t)))
    take_weights(1)
    each(0, 12, lambda t: far_group(t, high))

    def full_step(t):
        normalise_group(t)
        far_group(t, full)

    def ring_step(t):
        serve(t)
        full_step(t)

    each(12, 26, ring_step)
    relay_weights(2)
    each(26, 32, ring_step)
    take_weights(2)

    def mixed_step(n, _):
        each(n, n + 1, ring_step)
        return step_far(n - 32, 0)

    lax.fori_loop(32, 36, mixed_step, 0)
    each(36, 38, ring_step)
    relay_weights(3)
    each(38, 44, ring_step)

    lax.fori_loop(4, 10, step_far, 0)
    relay_weights(4)
    lax.fori_loop(10, 16, step_far, 0)
    take_weights(3)
    take_weights(4)

    def pair_rows(pair):
        return pl.ds(pl.multiple_of(pair * 256, 256), 256)

    def step_own(pair, _):
        with jax.named_scope("own"):
            rows = pair_rows(pair)
            xl[0, rows, 256:512] = share(xbf[rows, :], 2 + mate)
            remote(xl.at[0, rows, pl.ds(256, 256)], zp.at[rows, :], zp_send, zp_recv.at[pair], partner).start()
            xl[0, rows, 0:256] = share(xbf[rows, :], 2 + c)
        return 0

    lax.fori_loop(0, 8, step_own, 0)

    for pair in range(8):
        drain_recv(zp.at[pair_rows(pair), :], zp_recv.at[pair])

    def arrived(half, i, f, blk, c2, s):
        pieces = []
        for b in range(4):
            for v in range(2):
                group = (v * 4 + i) * 4 + lax.rem(s * (c2 - b) + 4, 4)
                start = c * (blk * BLOCK + b * PIECE + v * WAVE) + mate * (group * GROUP + f * WAVE)
                pieces.append(zr[half, pl.ds(pl.multiple_of(start, WAVE), WAVE), :])
        return jnp.concatenate(pieces, axis=0)

    def finish(half, blk, value):
        z_ref[pl.ds(pl.multiple_of(half * HALF + blk * BLOCK, BLOCK), BLOCK), :] = value
        lane = lax.broadcasted_iota(jnp.int32, (BLOCK, 128), 1)
        left, right = value[:, 0:128], jnp.where(lane < WORDS - 128, value[:, 128:256], LOW)
        top = jnp.max(jnp.maximum(left, right).T, axis=0, keepdims=True)
        shift = jnp.broadcast_to(top, (BLOCK, BLOCK)).T
        mass = jnp.exp(left - shift) + jnp.exp(right - shift)
        st[0, pl.ds(half * 16 + blk, 1), :] = top
        st[1, pl.ds(half * 16 + blk, 1), :] = jnp.sum(mass.T, axis=0, keepdims=True)

    def step_out(n, _):
        i, f, blk, c2, s = block_of(n)
        with jax.named_scope("wz"):
            @pl.when((c == 0) & (f == 0))
            def _():
                for half in range(2):
                    drain_recv(zr.at[half, pl.ds(0, 512), :], zq_recv.at[half, i])

            @pl.when(c == 1)
            def _():
                for half in range(2):
                    drain_recv(zr.at[half, block_rows(blk), :], z_recv.at[half, blk])
        rows = block_rows(blk)
        finish(c, blk, arrived(c, i, f, blk, c2, s) + xl[0, rows, 0:256])
        finish(mate, blk, arrived(mate, i, f, blk, c2, s) + zp[rows, :])
        return 0

    drain_send(ssq.at[pl.ds(0, 7), pl.ds(0, 16), :], ssq_send)
    drain_send(gl, g_send)
    drain_send(wl.at[0], wp_send)
    drain_send(wl.at[0], wb_send)
    drain_send(wl.at[0], wr_send)
    drain_send(xl.at[0], xp_send)
    drain_send(xl.at[0, pl.ds(0, 128), :], xb_send.at[1])
    for f in range(4):
        drain_send(xl.at[pl.ds(1, 2), pl.ds(0, 15 * PIECE), :], xf_send.at[f])
    drain_send(zp, zp_send)

    with jax.named_scope("finish"):
        lax.fori_loop(0, 16, step_out, 0)

    def exchange(buf, me, count, send, recv, dev):
        with jax.named_scope("exch"):
            for d in sorted(range(1, count), key=lambda d: abs(d - count // 2)):
                remote(buf.at[me], buf.at[me], send, recv.at[me], dev(lax.rem(me + d, count))).start()
            for d in range(1, count):
                other = lax.rem(me + d, count)
                drain_recv(buf.at[other], recv.at[other])
        top = buf[0]
        for k in range(1, count):
            top = jnp.maximum(top, buf[k])
        mass = jnp.exp(buf[0] - top)
        for k in range(1, count):
            mass = mass + jnp.exp(buf[k] - top)
        return top + jnp.log(mass)

    st1[row] = st[0] + jnp.log(st[1])
    st3[y] = exchange(st1, row, 8, st_send.at[0], st1_recv, at_row)
    for n in range(2):
        drain_send(zs.at[n], z_send.at[n])
    st2[z] = exchange(st3, y, 4, st_send.at[2], st3_recv, lambda k: at_col(k, z))
    lse_ref[...] = exchange(st2, z, 4, st_send.at[1], st2_recv, lambda k: at_col(y, k))

    drain_send(st1.at[pl.ds(0, 7)], st_send.at[0])
    drain_send(st2.at[pl.ds(0, 3)], st_send.at[1])
    drain_send(st3.at[pl.ds(0, 3)], st_send.at[2])


def solution(mesh):
    dma = pltpu.SemaphoreType.DMA

    def local_head(hidden, norm_gain, w_head):
        logits, log_norm = pl.pallas_call(
            kernel,
            out_shape=(pltpu.VMEM((SEQ, PAD), F32), pltpu.VMEM((32, 128), F32)),
            in_specs=[pl.BlockSpec(memory_space=pl.ANY), pl.BlockSpec(memory_space=pltpu.VMEM),
                      pl.BlockSpec(memory_space=pl.ANY)],
            out_specs=(pl.BlockSpec(memory_space=pltpu.VMEM), pl.BlockSpec(memory_space=pltpu.VMEM)),
            scratch_shapes=[
                pltpu.VMEM((SEQ, FEAT), BF16),
                pltpu.VMEM((8, PIECE, FEAT), BF16),
                pltpu.VMEM((8, PIECE, FEAT), F32),
                pltpu.VMEM((8 * WORDS, FEAT), BF16),
                pltpu.VMEM((8, PAD, FEAT), F32),
                pltpu.VMEM((3, 4, PAD, FEAT), F32),
                pltpu.VMEM((4, PAD, 4 * FEAT), BF16),
                pltpu.VMEM((HALF, FEAT), F32),
                pltpu.VMEM((3, HALF, FEAT), F32),
                pltpu.VMEM((HALF, 4 * FEAT), BF16),
                pltpu.VMEM((2, HALF, PAD), F32),
                pltpu.VMEM((HALF, PAD), F32),
                pltpu.VMEM((2, HALF, PAD), F32),
                pltpu.VMEM((3, 1, FEAT), F32),
                pltpu.VMEM((8, 32, 128), F32),
                pltpu.VMEM((HALF, 128), F32),
                pltpu.VMEM((2, 32, 128), F32),
                pltpu.VMEM((8, 32, 128), F32),
                pltpu.VMEM((4, 32, 128), F32),
                pltpu.VMEM((4, 32, 128), F32),
                dma((13,)),
                dma, dma((8,)),
                dma, dma((3,)),
                dma, dma((4,)),
                dma, dma((5,)),
                dma, dma((5,)),
                dma, dma((4,)),
                dma((2,)), dma((4,)), dma((4, 32)),
                dma((2,)), dma((2, 16)), dma((2, 4)),
                dma, dma((8,)),
                dma((3,)), dma((8,)), dma((4,)), dma((4,)),
            ],
            compiler_params=pltpu.CompilerParams(
                collective_id=0, has_side_effects=True, vmem_limit_bytes=59 * 1048576),
        )(hidden, norm_gain.reshape(1, FEAT), w_head.T)
        log_norm = log_norm.reshape(SEQ)
        return logits[:, :WORDS] - log_norm[:, None], log_norm

    return jax.shard_map(
        local_head,
        mesh=mesh,
        in_specs=(P("dp", "row"), P("row"), P("row", "col")),
        out_specs=(P("dp", ("col", "row")), P("dp")),
        check_vma=False,
    )
```
